32 devices in a mesh: fsdp: 2 (over x), ctx: 4 (over z), tp: 4 (over y, core).
Axes of the slice: x: 2, y: 2, z: 4, core: 2. Of those that a mesh axis runs over, the one named last changes fastest.
Arguments:
- tokens: bfloat16 [2, 2048, 3072], P('fsdp', 'ctx'), may hold values from -6 to 6
- segments: int32 [2, 2048], P('fsdp'), may hold values from 0 to 5, never falling along the last dimension, each value on 1 to 1024 neighbouring positions
- w_qkv: bfloat16 [3, 3072, 3072], P(None, ('fsdp', 'ctx'), 'tp'), may hold values from -1 to 1
- w_out: bfloat16 [3072, 3072], P('tp', ('fsdp', 'ctx')), may hold values from -1.75 to 1.75
- w_gate_up: bfloat16 [2, 3072, 8192], P(None, ('fsdp', 'ctx'), 'tp'), may hold values from -0.109375 to 0.109375
- w_down: bfloat16 [8192, 3072], P('tp', ('fsdp', 'ctx')), may hold values from -0.0625 to 0.0625
- norm_attn: bfloat16 [3072], P(('fsdp', 'ctx')), may hold values from 0.099609375 to 1.8984375
- norm_mlp: bfloat16 [3072], P(('fsdp', 'ctx')), may hold values from 0.099609375 to 1.8984375
- cotangent: bfloat16 [2, 2048, 3072], P('fsdp', 'ctx'), may hold values from -6 to 6
Outputs:
- output: bfloat16 [2, 2048, 3072], P('fsdp', 'ctx')
- grad_tokens: bfloat16 [2, 2048, 3072], P('fsdp', 'ctx')
- grad_qkv: float32 [3, 3072, 3072], P(None, ('fsdp', 'ctx'), 'tp')
- grad_out: float32 [3072, 3072], P('tp', ('fsdp', 'ctx'))
- grad_gate_up: float32 [2, 3072, 8192], P(None, ('fsdp', 'ctx'), 'tp')
- grad_down: float32 [8192, 3072], P('tp', ('fsdp', 'ctx'))
- grad_norm_attn: float32 [3072], P(('fsdp', 'ctx'))
- grad_norm_mlp: float32 [3072], P(('fsdp', 'ctx'))
The draws below stay inside these ranges and needn't reach their ends.
Inputs may be any that keep to these rules, and one draw needn't show every extreme that they name: `segments`: document numbers never fall along a sequence and begin at 0; every one of the 6 numbers is used, each document has 1 to 1024 tokens and one has exactly 1024.
All inputs are finite; a program needn't handle non-finite values.
Results may differ from the reference program's by a relative error of at most 0.014.
Values may be sent and summed in bfloat16 or wider, within the bound.
A program may use at most 384 MiB of HBM per device.

```python
import math
import jax
import jax.numpy as jnp
import numpy as np
from jax import lax

D = 3072
HD = 96
FF = 8192
L = 2048
DOCS = 6
DOC_MOST = 1024
SEQS = 2


def draw_tokens(key, part):
    values_out = jnp.clip(jax.random.normal(jax.random.fold_in(key, 25), (SEQS, L, D), jnp.float32), -6.0, 6.0)
    return values_out.astype(jnp.bfloat16)


def draw_w_qkv(key, part):
    noise_part = jnp.clip(jax.random.normal(jax.random.fold_in(key, 11), (3, D, D), jnp.float32), -6.0, 6.0)
    noise_part = noise_part * float(D) ** (-0.5)
    return noise_part.astype(jnp.bfloat16)


def steps_of(key, dims, pieces, least, top_value):
    def one(dim, shards_of):
        draws = jax.random.uniform(jax.random.fold_in(jax.random.fold_in(key, 6), dim), (shards_of,), jnp.float32, least / len(pieces), top_value / len(pieces))
        return jnp.repeat(jnp.exp(draws), dims[dim] // shards_of).reshape((-1,) + (1,) * (len(dims) - dim - 1))

    level = one(*pieces[0])
    for cut in pieces[1:]:
        level = level * one(*cut)
    return level


def split_up(amount, total, reach, lean):
    loads = [(1 << 20) // math.isqrt(standing ** lean) + 1 for standing in range(2, amount + 1)]
    rest, holding = total - reach - (amount - 1), [1] * (amount - 1)
    while rest > 0:
        candidates = [i for i in range(amount - 1) if holding[i] < reach]
        mass, budget = sum([loads[i] for i in candidates]), rest
        for i in candidates:
            more = min(reach - holding[i], max(1, budget * loads[i] // mass), rest)
            holding[i] = holding[i] + more
            rest = rest - more
    return np.array([reach] + holding)


def ragged(key, count, total, bound, skew):
    if count == 2:
        one = jax.random.randint(key, (), max(1, total - bound), min(bound, total - 1) + 1)
        return jnp.stack([one, total - one])
    sizes = jnp.asarray(split_up(count, total, bound, skew), jnp.int32)
    couples = (count - 1) // 2
    giver, sink = sizes[1:1 + 2 * couples:2], sizes[2:2 + 2 * couples:2]
    slack = jnp.minimum(giver - 1, bound - sink)
    shifted = jax.random.randint(jax.random.fold_in(key, 1), (couples,), 0, 1 << 20) % (slack + 1)
    sizes = sizes.at[1:1 + 2 * couples:2].set(giver - shifted).at[2:2 + 2 * couples:2].set(sink + shifted)
    return sizes[jax.random.permutation(jax.random.fold_in(key, 2), count)]


def noise(own_key, extent, deviation, most, cuts=(), held_as=jnp.bfloat16):
    drawn = jax.random.normal(own_key, extent, jnp.float32) * deviation
    if len(cuts) > 0:
        drawn = steps_of(own_key, extent, cuts, -0.22, 0.18) * drawn
    return jnp.clip(drawn, min=-most, max=most).astype(held_as)


def setup_inputs(seed: int = 0) -> dict:
    seeds = jax.random.split(jax.random.key(seed), 10)
    tokens = draw_tokens(jax.random.fold_in(seeds[9], 71), 0)
    segments = jax.vmap(lambda own: jnp.searchsorted(jnp.cumsum(ragged(own, DOCS, L, DOC_MOST, 1)), jnp.arange(L), side="right"))(jax.random.split(seeds[1], SEQS)).reshape((SEQS, L)).astype(jnp.int32)
    w_qkv = draw_w_qkv(jax.random.fold_in(seeds[9], 71), 0)
    w_out = noise(seeds[3], (D, D), (max(D // 256, 1)) ** -0.5, 1.75, ((0, 4), (1, 8)))
    w_gate_up = noise(seeds[4], (2, D, FF), D ** -0.5, 0.109375, ((1, 8), (2, 4)))
    w_down = noise(seeds[5], (FF, D), FF ** -0.5, 0.0625, ((0, 4), (1, 8)))
    norm_attn = jnp.clip(1.0 + 0.18 * jax.random.normal(seeds[6], (D,), jnp.float32), 0.099609375, 1.8984375).astype(jnp.bfloat16)
    norm_mlp = jnp.clip(1.0 + 0.18 * jax.random.normal(seeds[7], (D,), jnp.float32), 0.099609375, 1.8984375).astype(jnp.bfloat16)
    cotangent = noise(seeds[8], (SEQS, L, D), 1.0, 6.0, ((0, 2), (1, 4)))
    return {"tokens": tokens, "segments": segments, "w_qkv": w_qkv, "w_out": w_out, "w_gate_up": w_gate_up, "w_down": w_down, "norm_attn": norm_attn, "norm_mlp": norm_mlp, "cotangent": cotangent}


@jax.custom_vjp
def low(v):
    return lax.optimization_barrier(v.astype(jnp.bfloat16)).astype(jnp.float32)

@jax.custom_vjp
def low_back(v):
    return v

def low_keep(v):
    return (low(v), None)

def low_pass(kept, grad):
    return (grad,)

def back_keep(v):
    return (v, None)

def back_low(kept, grad):
    return (low(grad),)
low.defvjp(low_keep, low_pass)
low_back.defvjp(back_keep, back_low)
EPSILON = 1e-05
MASK_FILL = -1e+30
ROPE_BASE = 10000.0
HIGHEST = lax.Precision.HIGHEST

def doc_positions(segment_row):
    places = jnp.arange(segment_row.shape[0], dtype=jnp.int32)
    starts = jnp.concatenate([jnp.ones((1,), dtype=jnp.bool_), segment_row[1:] != segment_row[:-1]])
    first = lax.cummax(jnp.where(starts, places, jnp.zeros_like(places)), axis=0)
    return places - first

def rope_tables(positions, head_dim):
    half = head_dim // 2
    freqs = ROPE_BASE ** (-(jnp.arange(half, dtype=jnp.float32) * 2.0 / head_dim))
    angles = positions.astype(jnp.float32)[..., None] * freqs
    cosine = jnp.cos(angles)
    sine = jnp.sin(angles)
    return (jnp.concatenate([cosine, cosine], axis=-1), jnp.concatenate([sine, sine], axis=-1))

def rotate(values_in, cosine, sine):
    half = values_in.shape[-1] // 2
    turned = jnp.concatenate([-values_in[..., half:], values_in[..., :half]], axis=-1)
    return values_in * cosine[..., None, :] + turned * sine[..., None, :]

def rms_scale(values_in):
    return lax.rsqrt(lax.optimization_barrier(jnp.mean(values_in * values_in, axis=-1, keepdims=True)) + EPSILON)

def head_attend(query_h, keys_h, values_h, allowed):
    scale = 1.0 / math.sqrt(query_h.shape[-1])
    scores = low_back(jnp.dot(query_h, keys_h.T, precision=HIGHEST) * scale)
    scores = jnp.where(allowed, scores, MASK_FILL)
    peak = lax.optimization_barrier(jnp.max(scores, axis=1, keepdims=True))
    expo = jnp.exp(scores - peak)
    probs = expo / lax.optimization_barrier(jnp.sum(expo, axis=1, keepdims=True))
    return jnp.dot(low(probs), values_h, precision=HIGHEST)

def forward(tokens_row, segment_row, w_qkv, w_out, w_gate_up, w_down, norm_attn, norm_mlp):
    length, width = tokens_row.shape
    heads = width // HD
    normed1 = low(tokens_row * rms_scale(tokens_row) * norm_attn)
    projected = low_back(jnp.einsum('ld,cde->cle', normed1, w_qkv, precision=HIGHEST))
    cosine, sine = rope_tables(doc_positions(segment_row), HD)
    query = low_back(low(rotate(projected[0].reshape(length, heads, HD), cosine, sine)))
    keys = low_back(low(rotate(projected[1].reshape(length, heads, HD), cosine, sine)))
    values_v = low_back(low(projected[2].reshape(length, heads, HD)))
    places = jnp.arange(length, dtype=jnp.int32)
    allowed = (places[None, :] <= places[:, None]) & (segment_row[None, :] == segment_row[:, None])
    attend = jax.checkpoint(head_attend)
    mixed = lax.map(lambda triple: attend(triple[0], triple[1], triple[2], allowed), (query.transpose(1, 0, 2), keys.transpose(1, 0, 2), values_v.transpose(1, 0, 2)))
    attn = low_back(low(mixed.transpose(1, 0, 2).reshape(length, width)))
    hidden1 = tokens_row + low_back(jnp.dot(attn, w_out, precision=HIGHEST))
    normed2 = low(hidden1 * rms_scale(hidden1) * norm_mlp)
    gate_up = low_back(jnp.einsum('ld,cdf->clf', normed2, w_gate_up, precision=HIGHEST))
    act = low(jax.nn.silu(gate_up[0]) * gate_up[1])
    return hidden1 + low_back(jnp.dot(act, w_down, precision=HIGHEST))

def reference(tokens, segments, w_qkv, w_out, w_gate_up, w_down, norm_attn, norm_mlp, cotangent):
    weights = tuple((weight.astype(jnp.float32) for weight in (w_qkv, w_out, w_gate_up, w_down, norm_attn, norm_mlp)))

    def one_sequence(totals, item):
        tokens_row, segment_row, grad_row = item

        def block_fn(tokens_in, *params):
            return forward(tokens_in, segment_row, *params)
        result, pull = jax.vjp(block_fn, tokens_row.astype(jnp.float32), *weights)
        grads = pull(grad_row.astype(jnp.float32))
        totals = tuple((total + grad for total, grad in zip(totals, grads[1:])))
        return (totals, (result.astype(jnp.bfloat16), grads[0].astype(jnp.bfloat16)))
    zero_totals = tuple((jnp.zeros(weight.shape, jnp.float32) for weight in weights))
    totals, (output, grad_tokens) = lax.scan(one_sequence, zero_totals, (tokens, segments, cotangent))
    return (output, grad_tokens, totals[0], totals[1], totals[2], totals[3], totals[4], totals[5])
```

```python
import functools
import math

import jax
import jax.numpy as jnp
from jax import lax
from jax.experimental import pallas as pl
from jax.experimental.pallas import tpu as pltpu
from jax.sharding import PartitionSpec as P

HD = 96
HALF = HD // 2
LANES = 128
EPSILON = 1e-05
MASK_FILL = -1e30
ROPE_BASE = 10000.0
GROUP = ("ctx", "tp")
BLK = 256
MESH = pl.DeviceIdType.MESH
SUBS = 2
VLIM = 64 * 1024 * 1024 - 65536


def near_order(c, j, size):
    low = c < size // 2
    base = jnp.where(low, c, size - 1 - c)
    zig = jnp.where(j % 2 == 1, base - (j + 1) // 2, base + j // 2)
    place = jnp.where(j <= 2 * base, zig, j)
    return jnp.where(low, place, size - 1 - place)


def places():
    c, t = lax.axis_index("ctx"), lax.axis_index("tp")
    return c, t // 2, t % 2


def greet(c, y, k, size):
    barrier = pltpu.get_barrier_semaphore()

    @pl.when(c < size - 1)
    def _():
        pl.semaphore_signal(barrier, inc=1, device_id={"ctx": c + 1}, device_id_type=MESH)

    @pl.when(c > 0)
    def _():
        pl.semaphore_signal(barrier, inc=1, device_id={"ctx": c - 1}, device_id_type=MESH)

    pl.semaphore_signal(barrier, inc=1, device_id={"tp": (1 - y) * 2 + k}, device_id_type=MESH)
    pl.semaphore_signal(barrier, inc=1, device_id={"tp": y * 2 + 1 - k}, device_id_type=MESH)
    pl.semaphore_wait(barrier, jnp.where((c > 0) & (c < size - 1), 4, 3))


def gather_kernel(size, part, n_in, n_out, compute, *refs):
    x_ref = refs[0]
    hbm_ins = refs[1 : 1 + n_in]
    full_ref = refs[1 + n_in]
    outs = refs[2 + n_in : 2 + n_in + n_out]
    ins = refs[2 + n_in + n_out : 2 + 2 * n_in + n_out]
    buf, recv, zs, ys, ks, local, load, in_sems = refs[2 + 2 * n_in + n_out :]
    c, y, k = places()
    sub = part // SUBS

    def slot(cc, yy, kk, s):
        return buf.at[cc * 2 + yy, pl.ds(pl.multiple_of(kk * part + s * sub, sub), sub)]

    def copy(cc, yy, kk, s, sem, dev):
        return pltpu.make_async_remote_copy(
            src_ref=slot(cc, yy, kk, s),
            dst_ref=slot(cc, yy, kk, s),
            send_sem=sem,
            recv_sem=recv.at[cc * 2 + yy, kk, s],
            device_id=dev,
            device_id_type=MESH,
        )

    up, down = {"ctx": c + 1}, {"ctx": c - 1}
    ydev, kdev = {"tp": (1 - y) * 2 + k}, {"tp": y * 2 + 1 - k}

    def z_up(cc, s):
        return copy(cc, y, k, s, zs.at[0, cc, s], up)

    def z_down(cc, s):
        return copy(cc, y, k, s, zs.at[1, cc, s], down)

    def y_send(cc, s):
        return copy(cc, y, k, s, ys.at[cc, s], ydev)

    def k_send(cc, yy, s):
        return copy(cc, yy, k, s, ks.at[cc * 2 + yy, s], kdev)

    def pair_out(cc, yy):
        pair = cc * 2 + yy
        return pltpu.make_async_copy(
            buf.at[pair],
            full_ref.at[pl.ds(pl.multiple_of(pair * 2 * part, 2 * part), 2 * part)],
            local.at[pair],
        )

    def got(cc, yy, kk, s):
        copy(cc, yy, kk, s, ys.at[0, 0], ydev).wait_recv()

    mine = buf.at[c * 2 + y, pl.ds(pl.multiple_of(k * part, part), part)]
    first = pltpu.make_async_copy(x_ref, mine, load)
    first.start()
    for i in range(n_in):
        pltpu.make_async_copy(hbm_ins[i], ins[i], in_sems.at[i]).start()
    greet(c, y, k, size)
    first.wait()

    def z_stage(cc, s):
        @pl.when((cc <= c) & (c < size - 1))
        def _():
            z_up(cc, s).start()

        @pl.when((cc >= c) & (c > 0))
        def _():
            z_down(cc, s).start()

        y_send(cc, s).start()
        k_send(cc, y, s).start()

    for s in range(SUBS):
        z_stage(c, s)
    for i in range(n_in):
        pltpu.make_async_copy(hbm_ins[i], ins[i], in_sems.at[i]).wait()

    def finish(cc, yy):
        for s in range(SUBS):
            got(cc, yy, 1 - k, s)
        pair_out(cc, yy).start()
        compute(cc * 2 + yy, buf, ins, outs)

    def step(r, carry):
        for s in range(SUBS):
            for sign in (-1, 1):
                nxt = c + sign * (r + 1)

                @pl.when((nxt >= 0) & (nxt < size))
                def _():
                    got(nxt, y, k, s)
                    z_stage(nxt, s)

            for sign in (-1, 1):
                cc = c + sign * r

                @pl.when((cc >= 0) & (cc < size) & ((r > 0) | (sign > 0)))
                def _():
                    if s == SUBS - 1:
                        finish(cc, y)
                    got(cc, 1 - y, k, s)
                    k_send(cc, 1 - y, s).start()
                    if s == SUBS - 1:
                        finish(cc, 1 - y)

        return carry

    lax.fori_loop(0, size, step, 0)

    def drain(cc, carry):
        for s in range(SUBS):
            @pl.when((cc <= c) & (c < size - 1))
            def _():
                z_up(cc, s).wait_send()

            @pl.when((cc >= c) & (c > 0))
            def _():
                z_down(cc, s).wait_send()

            y_send(cc, s).wait_send()
            for yy in range(2):
                k_send(cc, yy, s).wait_send()
        for yy in range(2):
            pair_out(cc, yy).wait()
        return carry

    lax.fori_loop(0, size, drain, 0)


def gather_call(x, ins, out_shapes, compute, name, cid, size):
    part, width = x.shape
    any_spec = pl.BlockSpec(memory_space=pl.ANY)
    vmem = pl.BlockSpec(memory_space=pltpu.VMEM)
    full = jax.ShapeDtypeStruct((size * 4 * part, width), x.dtype)
    return pl.pallas_call(
        functools.partial(gather_kernel, size, part, len(ins), len(out_shapes), compute),
        out_shape=(full, *out_shapes),
        in_specs=[any_spec] * (1 + len(ins)),
        out_specs=(any_spec, *([vmem] * len(out_shapes))),
        scratch_shapes=[
            *(pltpu.VMEM(one.shape, one.dtype) for one in ins),
            pltpu.VMEM((size * 2, 2 * part, width), x.dtype),
            pltpu.SemaphoreType.DMA((size * 2, 2, SUBS)),
            pltpu.SemaphoreType.DMA((2, size, SUBS)),
            pltpu.SemaphoreType.DMA((size, SUBS)),
            pltpu.SemaphoreType.DMA((size * 2, SUBS)),
            pltpu.SemaphoreType.DMA((size * 2,)),
            pltpu.SemaphoreType.DMA,
            pltpu.SemaphoreType.DMA((max(len(ins), 1),)),
        ],
        compiler_params=pltpu.CompilerParams(
            collective_id=cid, has_side_effects=True, vmem_limit_bytes=VLIM
        ),
        name=name,
    )(x, *ins)


def reduce_kernel(size, part, n_in, n_out, final, *refs):
    a_ref, w_ref = refs[:2]
    ins = refs[2 : 2 + n_in]
    outs = refs[2 + n_in : 2 + n_in + n_out]
    (
        own,
        ksend,
        krecv,
        ysend,
        yrecv,
        qown,
        zsend,
        zrecv,
        total,
        k_sems,
        y_sems,
        z_sems,
    ) = refs[2 + n_in + n_out :]
    c, y, k = places()
    chunk = 16
    tile = 512
    width = total.shape[1]

    sub = part // SUBS

    def remote(src, dst, sems, dev):
        return pltpu.make_async_remote_copy(
            src_ref=src,
            dst_ref=dst,
            send_sem=sems.at[0],
            recv_sem=sems.at[1],
            device_id=dev,
            device_id_type=MESH,
        )

    ydev, kdev = {"tp": (1 - y) * 2 + k}, {"tp": y * 2 + 1 - k}

    def k_copy(cc, yy):
        pair = cc * 2 + yy
        return remote(ksend.at[pair], krecv.at[pair], k_sems.at[pair], kdev)

    def y_copy(cc, s):
        r = pl.ds(s * sub, sub)
        return remote(ysend.at[cc, r], yrecv.at[cc, r], y_sems.at[cc, s], ydev)

    def z_up(cc, s):
        r = pl.ds(s * sub, sub)
        return remote(zsend.at[cc, r], zrecv.at[0, cc, r], z_sems.at[0, cc, s], {"ctx": c + 1})

    def z_down(cc, s):
        r = pl.ds(s * sub, sub)
        return remote(zsend.at[cc, r], zrecv.at[1, cc, r], z_sems.at[1, cc, s], {"ctx": c - 1})

    greet(c, y, k, size)

    def rows(i):
        return pl.ds(pl.multiple_of(i * chunk, chunk), chunk)

    def sweep(body, s=None):
        steps = part // chunk
        lo, hi = (0, steps) if s is None else (s * steps // SUBS, (s + 1) * steps // SUBS)

        def one(i, carry):
            body(rows(i))
            return carry

        lax.fori_loop(lo, hi, one, 0)

    def produce(cc, yy, keep):
        pair = cc * 2 + yy
        mine = pl.ds(pl.multiple_of(pair * 2 * part + k * part, part), part)
        other = pl.ds(pl.multiple_of(pair * 2 * part + (1 - k) * part, part), part)

        def one(i, carry):
            lanes = pl.ds(pl.multiple_of(i * tile, tile), tile)
            w = w_ref[:, lanes]
            ksend[pair, :, lanes] = jnp.dot(
                a_ref[other, :], w, preferred_element_type=jnp.float32
            ).astype(jnp.bfloat16)
            own[keep, :, lanes] = jnp.dot(a_ref[mine, :], w, preferred_element_type=jnp.float32)
            return carry

        lax.fori_loop(0, width // tile, one, 0)
        k_copy(cc, yy).start()

    def first(j, carry):
        cc = near_order(c, size - 1 - j, size)
        produce(cc, 1 - y, 0)
        produce(cc, y, 1)
        k_copy(cc, 1 - y).wait_recv()

        def add_y(r):
            got = krecv[cc * 2 + 1 - y, r, :].astype(jnp.float32)
            ysend[cc, r, :] = (own[0, r, :] + got).astype(jnp.bfloat16)

        for s in range(SUBS):
            sweep(add_y, s)
            y_copy(cc, s).start()
        k_copy(cc, y).wait_recv()

        def add_k(r):
            qown[cc, r, :] = own[1, r, :] + krecv[cc * 2 + y, r, :].astype(jnp.float32)

        sweep(add_k)
        return carry

    lax.fori_loop(0, size, first, 0)

    def pass_on(cc, s, into, edge, send):
        @pl.when(jnp.logical_not(edge))
        def _():
            send(cc, s).wait_recv()

            def add(r):
                part_sum = qown[cc, r, :] + yrecv[cc, r, :].astype(jnp.float32)
                zsend[cc, r, :] = (part_sum + zrecv[into, cc, r, :].astype(jnp.float32)).astype(
                    jnp.bfloat16
                )

            sweep(add, s)

        @pl.when(edge)
        def _():
            def add(r):
                part_sum = qown[cc, r, :] + yrecv[cc, r, :].astype(jnp.float32)
                zsend[cc, r, :] = part_sum.astype(jnp.bfloat16)

            sweep(add, s)

        send(cc, s).start()

    def second(j, carry):
        cc = near_order(c, size - 1 - j, size)
        for s in range(SUBS):
            y_copy(cc, s).wait_recv()

            @pl.when(cc > c)
            def _():
                pass_on(cc, s, 0, c == 0, z_up)

            @pl.when(cc < c)
            def _():
                pass_on(cc, s, 1, c == size - 1, z_down)

        return carry

    lax.fori_loop(0, size, second, 0)

    def add_own(r):
        total[r, :] = qown[c, r, :] + yrecv[c, r, :].astype(jnp.float32)

    sweep(add_own)

    @pl.when(c > 0)
    def _():
        for s in range(SUBS):
            z_up(c, s).wait_recv()

        def add(r):
            total[r, :] += zrecv[0, c, r, :].astype(jnp.float32)

        sweep(add)

    @pl.when(c < size - 1)
    def _():
        for s in range(SUBS):
            z_down(c, s).wait_recv()

        def add(r):
            total[r, :] += zrecv[1, c, r, :].astype(jnp.float32)

        sweep(add)

    final(total, sweep, ins, outs)

    def drain(cc, carry):
        for yy in range(2):
            k_copy(cc, yy).wait_send()
        for s in range(SUBS):
            y_copy(cc, s).wait_send()

            @pl.when(cc > c)
            def _():
                z_up(cc, s).wait_send()

            @pl.when(cc < c)
            def _():
                z_down(cc, s).wait_send()

        return carry

    lax.fori_loop(0, size, drain, 0)


def reduce_call(a, w, ins, out_shapes, final, name, cid, size):
    width = w.shape[1]
    part = a.shape[0] // (size * 4)
    vmem = pl.BlockSpec(memory_space=pltpu.VMEM)
    low, full = jnp.bfloat16, jnp.float32
    return pl.pallas_call(
        functools.partial(reduce_kernel, size, part, len(ins), len(out_shapes), final),
        out_shape=tuple(out_shapes),
        in_specs=[vmem] * (2 + len(ins)),
        out_specs=tuple([vmem] * len(out_shapes)),
        scratch_shapes=[
            pltpu.VMEM((2, part, width), full),
            pltpu.VMEM((size * 2, part, width), low),
            pltpu.VMEM((size * 2, part, width), low),
            pltpu.VMEM((size, part, width), low),
            pltpu.VMEM((size, part, width), low),
            pltpu.VMEM((size, part, width), full),
            pltpu.VMEM((size, part, width), low),
            pltpu.VMEM((2, size, part, width), low),
            pltpu.VMEM((part, width), full),
            pltpu.SemaphoreType.DMA((size * 2, 2)),
            pltpu.SemaphoreType.DMA((size, SUBS, 2)),
            pltpu.SemaphoreType.DMA((2, size, SUBS, 2)),
        ],
        compiler_params=pltpu.CompilerParams(
            collective_id=cid, has_side_effects=True, vmem_limit_bytes=VLIM
        ),
        name=name,
    )(a, w, *ins)


def doc_positions(segment_row):
    places_in = jnp.arange(segment_row.shape[0], dtype=jnp.int32)
    starts = jnp.concatenate([jnp.ones((1,), dtype=jnp.bool_), segment_row[1:] != segment_row[:-1]])
    first = lax.cummax(jnp.where(starts, places_in, jnp.zeros_like(places_in)), axis=0)
    return places_in - first


def rope_tables(positions):
    freqs = ROPE_BASE ** (-(jnp.arange(HALF, dtype=jnp.float32) * 2.0 / HD))
    angles = positions.astype(jnp.float32)[:, None] * freqs
    gap = jnp.zeros((positions.shape[0], LANES // 2 - HALF), jnp.float32)
    cosine, sine = jnp.cos(angles), jnp.sin(angles)
    return (
        jnp.concatenate([cosine, gap, cosine, gap], axis=1),
        jnp.concatenate([-sine, gap, sine, gap], axis=1),
    )


def spread(array, axis):
    shape = array.shape
    halves = array.reshape(*shape[:axis], shape[axis] // HALF, HALF, *shape[axis + 1 :])
    pads = [(0, 0)] * halves.ndim
    pads[axis + 1] = (0, LANES // 2 - HALF)
    wide = jnp.pad(halves, pads)
    return wide.reshape(*shape[:axis], -1, *shape[axis + 1 :])


def unspread(array, axis):
    shape = array.shape
    half = LANES // 2
    halves = array.reshape(*shape[:axis], shape[axis] // half, half, *shape[axis + 1 :])
    kept = lax.slice_in_dim(halves, 0, HALF, axis=axis + 1)
    return kept.reshape(*shape[:axis], -1, *shape[axis + 1 :])


def nt(left, right):
    return lax.dot_general(left, right, (((1,), (1,)), ((), ())), preferred_element_type=jnp.float32)


def nn(left, right):
    return jnp.dot(left, right, preferred_element_type=jnp.float32)


def tn(left, right):
    return lax.dot_general(left, right, (((0,), (0,)), ((), ())), preferred_element_type=jnp.float32)


def qkv_kernel(heads, x_ref, w_ref, cos_ref, sin_ref, out_ref):
    proj = nt(x_ref[...], w_ref[...])
    for i in range(3 * heads):
        cut = slice(i * LANES, (i + 1) * LANES)
        one = proj[:, cut]
        if i < 2 * heads:
            one = one * cos_ref[...] + pltpu.roll(one, LANES // 2, 1) * sin_ref[...]
        out_ref[:, cut] = one.astype(jnp.bfloat16)


def qkv_call(x, w, cosine, sine, heads):
    rows, width = x.shape
    return pl.pallas_call(
        functools.partial(qkv_kernel, heads),
        out_shape=jax.ShapeDtypeStruct((rows, w.shape[0]), jnp.bfloat16),
        grid=(rows // BLK,),
        in_specs=[
            pl.BlockSpec((BLK, width), lambda i: (i, 0)),
            pl.BlockSpec(w.shape, lambda i: (0, 0)),
            pl.BlockSpec((BLK, LANES), lambda i: (i, 0)),
            pl.BlockSpec((BLK, LANES), lambda i: (i, 0)),
        ],
        out_specs=pl.BlockSpec((BLK, w.shape[0]), lambda i: (i, 0)),
        compiler_params=pltpu.CompilerParams(vmem_limit_bytes=VLIM),
        name="qkv",
    )(x, w, cosine, sine)


def block(ref, i, head):
    return ref[pl.ds(pl.multiple_of(i * BLK, BLK), BLK), head * LANES : (head + 1) * LANES]


def masked_scores(keys, query, seg_col, seg_row, kb, qb, scale):
    scores = nt(keys, query) * scale
    key_pos = kb * BLK + lax.broadcasted_iota(jnp.int32, scores.shape, 0)
    query_pos = qb * BLK + lax.broadcasted_iota(jnp.int32, scores.shape, 1)
    return jnp.where((key_pos <= query_pos) & (seg_col == seg_row), scores, MASK_FILL)


def attend_kernel(heads, scale, low_ref, qkv_ref, col_ref, row_ref, out_ref, lse_ref):
    blocks = qkv_ref.shape[0] // BLK

    def one(i, carry):
        cut = pl.ds(pl.multiple_of(i * BLK, BLK), BLK)
        seg_row = row_ref[:, cut]
        for h in range(heads):
            query = block(qkv_ref, i, h)

            def inner(kb, state):
                peak, total, acc = state
                keys = block(qkv_ref, kb, heads + h)
                seg_col = col_ref[pl.ds(pl.multiple_of(kb * BLK, BLK), BLK), :]
                scores = masked_scores(keys, query, seg_col, seg_row, kb, i, scale)
                new = jnp.maximum(peak, jnp.max(scores, axis=0, keepdims=True))
                fade = jnp.exp(peak - new)
                expo = jnp.exp(scores - new)
                total = total * fade + jnp.sum(expo, axis=0, keepdims=True)
                mixed = tn(block(qkv_ref, kb, 2 * heads + h), expo.astype(jnp.bfloat16))
                return new, total, acc * fade + mixed

            peak, total, acc = lax.fori_loop(
                low_ref[i],
                i + 1,
                inner,
                (
                    jnp.full((1, BLK), MASK_FILL, jnp.float32),
                    jnp.zeros((1, BLK), jnp.float32),
                    jnp.zeros((LANES, BLK), jnp.float32),
                ),
            )
            out_ref[cut, h * LANES : (h + 1) * LANES] = (acc / total).T.astype(jnp.bfloat16)
            lse_ref[h : h + 1, cut] = peak + jnp.log(total)
        return carry

    lax.fori_loop(0, blocks, one, 0)


def attend_call(qkv, seg, low, heads, scale):
    rows = qkv.shape[0]
    vmem = pl.BlockSpec(memory_space=pltpu.VMEM)
    return pl.pallas_call(
        functools.partial(attend_kernel, heads, scale),
        out_shape=(
            jax.ShapeDtypeStruct((rows, heads * LANES), jnp.bfloat16),
            jax.ShapeDtypeStruct((heads, rows), jnp.float32),
        ),
        in_specs=[pl.BlockSpec(memory_space=pltpu.SMEM), vmem, vmem, vmem],
        out_specs=(vmem, vmem),
        compiler_params=pltpu.CompilerParams(vmem_limit_bytes=VLIM),
        name="attend",
    )(low, qkv, seg[:, None], seg[None, :])


def attend_back_kernel(
    heads,
    scale,
    high_ref,
    qkv_ref,
    out_ref,
    grad_ref,
    lse_ref,
    col_ref,
    row_ref,
    cos_ref,
    sin_ref,
    res_ref,
    delta_ref,
    gq_ref,
):
    blocks = qkv_ref.shape[0] // BLK
    gq_ref[...] = jnp.zeros_like(gq_ref)

    def dots(i, carry):
        cut = pl.ds(pl.multiple_of(i * BLK, BLK), BLK)
        for h in range(heads):
            prod = block(out_ref, i, h).astype(jnp.float32) * block(grad_ref, i, h).astype(
                jnp.float32
            )
            delta_ref[h : h + 1, cut] = jnp.sum(prod.T, axis=0, keepdims=True)
        return carry

    lax.fori_loop(0, blocks, dots, 0)

    def turn_back(value, cut):
        low = value.astype(jnp.bfloat16).astype(jnp.float32)
        turned = low * cos_ref[cut, :] - pltpu.roll(low, LANES // 2, 1) * sin_ref[cut, :]
        return turned.astype(jnp.bfloat16)

    def one(kb, carry):
        cut = pl.ds(pl.multiple_of(kb * BLK, BLK), BLK)
        seg_col = col_ref[cut, :]
        for h in range(heads):
            keys = block(qkv_ref, kb, heads + h)
            values = block(qkv_ref, kb, 2 * heads + h)

            def inner(i, state):
                gk, gv = state
                at = pl.ds(pl.multiple_of(i * BLK, BLK), BLK)
                query = block(qkv_ref, i, h)
                grad = block(grad_ref, i, h)
                scores = masked_scores(keys, query, seg_col, row_ref[:, at], kb, i, scale)
                probs = jnp.exp(scores - lse_ref[h : h + 1, at])
                gv = gv + nn(probs.astype(jnp.bfloat16), grad)
                g_probs = nt(values, grad)
                g_scores = (probs * (g_probs - delta_ref[h : h + 1, at])).astype(jnp.bfloat16)
                gk = gk + nn(g_scores, query)
                lanes = slice(h * LANES, (h + 1) * LANES)
                gq_ref[at, lanes] += tn(g_scores, keys)
                return gk, gv

            zero = jnp.zeros((BLK, LANES), jnp.float32)
            gk, gv = lax.fori_loop(kb, high_ref[kb] + 1, inner, (zero, zero))
            at_k = slice((heads + h) * LANES, (heads + h + 1) * LANES)
            at_v = slice((2 * heads + h) * LANES, (2 * heads + h + 1) * LANES)
            res_ref[cut, at_k] = turn_back(gk * scale, cut)
            res_ref[cut, at_v] = gv.astype(jnp.bfloat16)
        return carry

    lax.fori_loop(0, blocks, one, 0)

    def close(i, carry):
        cut = pl.ds(pl.multiple_of(i * BLK, BLK), BLK)
        for h in range(heads):
            lanes = slice(h * LANES, (h + 1) * LANES)
            res_ref[cut, lanes] = turn_back(gq_ref[cut, lanes] * scale, cut)
        return carry

    lax.fori_loop(0, blocks, close, 0)


def attend_back_call(qkv, out, grad, lse, seg, high, cosine, sine, heads, scale):
    rows = qkv.shape[0]
    vmem = pl.BlockSpec(memory_space=pltpu.VMEM)
    return pl.pallas_call(
        functools.partial(attend_back_kernel, heads, scale),
        out_shape=jax.ShapeDtypeStruct(qkv.shape, jnp.bfloat16),
        in_specs=[pl.BlockSpec(memory_space=pltpu.SMEM)] + [vmem] * 8,
        out_specs=vmem,
        scratch_shapes=[
            pltpu.VMEM((heads, rows), jnp.float32),
            pltpu.VMEM((rows, heads * LANES), jnp.float32),
        ],
        compiler_params=pltpu.CompilerParams(vmem_limit_bytes=VLIM),
        name="attend_back",
    )(high, qkv, out, grad, lse, seg[:, None], seg[None, :], cosine, sine)


def cross(weight):
    size, groups = lax.axis_size("ctx"), lax.axis_size("fsdp")
    c, f = lax.axis_index("ctx"), lax.axis_index("fsdp")
    n = weight.shape[1] // size
    pieces = []
    for s in range(size):
        piece = lax.dynamic_slice_in_dim(weight, ((c + s) % size) * n, n, 1)
        if s:
            piece = lax.ppermute(piece, "ctx", [(i, (i + s) % size) for i in range(size)])
        pieces.append((piece, f * size + (c - s) % size))
    for g in range(1, groups):
        for s in range(size):
            piece = lax.ppermute(
                pieces[s][0], "fsdp", [(i, (i + g) % groups) for i in range(groups)]
            )
            pieces.append((piece, ((f - g) % groups) * size + (c - s) % size))
    return pieces


def join_kernel(count, cuts, groups, size, *refs):
    pieces, out, sems = refs[:count], refs[count], refs[count + 1]
    c, f = lax.axis_index("ctx"), lax.axis_index("fsdp")
    m, n, d = pieces[0].shape
    tall = out.shape[0] // m

    def copies(go):
        for i in range(count):
            g, s = i // size, i % size
            place = ((f + groups - g) % groups) * size + (c + size - s) % size
            lanes = pl.ds(pl.multiple_of(place * d, d), d)
            for j in range(m):
                for q, (src, dst, rows) in enumerate(cuts):
                    go(
                        pltpu.make_async_copy(
                            pieces[i].at[j, pl.ds(src, rows)],
                            out.at[pl.ds(j * tall + dst, rows), lanes],
                            sems.at[i, j * len(cuts) + q],
                        )
                    )

    copies(lambda one: one.start())
    for j in range(m):
        for k, (_, dst, rows) in enumerate(cuts):
            stop = cuts[k + 1][1] if k + 1 < len(cuts) else tall
            if dst + rows < stop:
                gap = stop - dst - rows
                out[pl.ds(j * tall + dst + rows, gap), :] = jnp.zeros(
                    (gap, out.shape[1]), out.dtype
                )
    copies(lambda one: one.wait())


def join(pieces, spaced, name):
    m, n, d = pieces[0][0].shape
    width = len(pieces) * d
    if d % LANES:
        buf = jnp.zeros((len(pieces), m, n, d), pieces[0][0].dtype)
        for piece, place in pieces:
            buf = lax.dynamic_update_slice(buf, piece[None], (place, 0, 0, 0))
        flat = buf.transpose(1, 2, 0, 3).reshape(m, n, width)
        flat = spread(flat, 1) if spaced else flat
        return flat.reshape(-1, width)
    cuts = [(0, 0, n)]
    if spaced:
        cuts = [(i * HALF, i * LANES // 2, HALF) for i in range(n // HALF)]
    tall = n * LANES // HD if spaced else n
    return pl.pallas_call(
        functools.partial(
            join_kernel,
            len(pieces),
            cuts,
            lax.axis_size("fsdp"),
            lax.axis_size("ctx"),
        ),
        out_shape=jax.ShapeDtypeStruct((m * tall, width), pieces[0][0].dtype),
        in_specs=[pl.BlockSpec(memory_space=pl.ANY)] * len(pieces),
        out_specs=pl.BlockSpec(memory_space=pltpu.VMEM),
        scratch_shapes=[pltpu.SemaphoreType.DMA((len(pieces), m * len(cuts)))],
        compiler_params=pltpu.CompilerParams(vmem_limit_bytes=VLIM),
        name=name,
    )(*[piece for piece, _ in pieces])


def hand_out(grad):
    size, groups = lax.axis_size("ctx"), lax.axis_size("fsdp")
    c, f = lax.axis_index("ctx"), lax.axis_index("fsdp")
    rows = grad.shape[0] // groups
    d = rows // size
    total = lax.dynamic_slice_in_dim(grad, f * rows, rows, 0)
    for g in range(1, groups):
        sent = lax.dynamic_slice_in_dim(grad, ((f + g) % groups) * rows, rows, 0)
        got = lax.ppermute(
            sent.astype(jnp.bfloat16), "fsdp", [(i, (i + g) % groups) for i in range(groups)]
        )
        total = total.astype(jnp.float32) + got.astype(jnp.float32)
    total = total.astype(jnp.bfloat16)
    out = jnp.zeros((size, d, grad.shape[1]), jnp.bfloat16)
    for s in range(size):
        piece = lax.dynamic_slice_in_dim(total, ((c + s) % size) * d, d, 0)
        if s:
            piece = lax.ppermute(piece, "ctx", [(i, (i + s) % size) for i in range(size)])
        out = lax.dynamic_update_slice(out, piece[None], ((c - s) % size, 0, 0))
    return out.astype(jnp.float32)


def wide_gather(part):
    full = lax.all_gather(part, GROUP, axis=0, tiled=True)
    return full


def mlp_block(half, pair, buf, ins, outs):
    w, g_act = ins
    act, g_gate, g_up = outs
    rows = buf.shape[1]
    tile = 256
    at = pl.ds(pl.multiple_of(pair * rows, rows), rows)

    def one(i, carry):
        lanes = pl.ds(pl.multiple_of(i * tile, tile), tile)
        gate = nt(buf[pair], w[lanes, :])
        up = nt(buf[pair], w[pl.ds(pl.multiple_of(half + i * tile, tile), tile), :])
        grad = g_act[at, lanes]
        sigma = 1.0 / (1.0 + jnp.exp(-gate))
        silu = gate * sigma
        act[at, lanes] = (silu * up).astype(jnp.bfloat16)
        g_up[at, lanes] = (grad * silu).astype(jnp.bfloat16)
        g_gate[at, lanes] = (grad * up * sigma * (1.0 + gate * (1.0 - sigma))).astype(jnp.bfloat16)
        return carry

    lax.fori_loop(0, half // tile, one, 0)


def attn_block(pair, buf, ins, outs):
    rows = buf.shape[1]
    at = pl.ds(pl.multiple_of(pair * rows, rows), rows)
    outs[0][at, :] = nt(buf[pair], ins[0][...]).astype(jnp.bfloat16)


def no_block(pair, buf, ins, outs):
    pass


def after_out(total, sweep, ins, outs):
    tokens, gain = ins
    hidden, normed = outs

    def one(r):
        value = tokens[r, :].astype(jnp.float32) + total[r, :]
        scale = lax.rsqrt(jnp.mean(value * value, axis=1, keepdims=True) + EPSILON)
        hidden[r, :] = value
        normed[r, :] = (value * scale * gain[...]).astype(jnp.bfloat16)

    sweep(one)


def norm_back(grad, value, gain, top):
    scale = lax.rsqrt(jnp.mean(value * value, axis=1, keepdims=True) + EPSILON)
    unit = value * scale
    g_unit = grad * gain
    inner = jnp.mean(g_unit * unit, axis=1, keepdims=True)
    return top + scale * (g_unit - unit * inner), grad * unit


def after_mlp(total, sweep, ins, outs):
    hidden, cot, gain = ins
    g_hidden, g_branch, g_gain = outs
    g_gain[...] = jnp.zeros_like(g_gain)

    def one(r):
        grad, part = norm_back(
            total[r, :], hidden[r, :], gain[...], cot[r, :].astype(jnp.float32)
        )
        g_hidden[r, :] = grad
        g_branch[r, :] = grad.astype(jnp.bfloat16)
        g_gain[...] += part

    sweep(one)


def after_qkv(total, sweep, ins, outs):
    tokens, g_hidden, gain = ins
    g_tokens, g_gain = outs
    g_gain[...] = jnp.zeros_like(g_gain)

    def one(r):
        grad, part = norm_back(
            total[r, :], tokens[r, :].astype(jnp.float32), gain[...], g_hidden[r, :]
        )
        g_tokens[r, :] = grad.astype(jnp.bfloat16)
        g_gain[...] += part

    sweep(one)


def shards(tokens, segments, w_qkv, w_out, w_gate_up, w_down, norm_attn, norm_mlp, cotangent):
    seqs, rows, width = tokens.shape
    size, tp_size = lax.axis_size("ctx"), lax.axis_size("tp")
    length = segments.shape[1]
    assert seqs == 1 and tp_size == 4
    part = rows // tp_size
    begin = lax.axis_index("tp") * part
    scale = 1.0 / math.sqrt(HD)
    low, full = jnp.bfloat16, jnp.float32
    heads = w_qkv.shape[2] // HD // size
    seg = segments[0]

    tokens_own = lax.dynamic_slice_in_dim(tokens[0], begin, part, 0)
    cot_own = lax.dynamic_slice_in_dim(cotangent[0], begin, part, 0)

    pieces_q = cross(w_qkv.transpose(0, 2, 1))
    gains = lax.all_gather(
        jnp.stack([norm_attn, norm_mlp]), ("fsdp", "ctx"), axis=1, tiled=True
    ).astype(full)
    gain_attn, gain_mlp = gains[0:1], gains[1:2]
    resid = tokens_own.astype(full)
    scale_one = lax.rsqrt(jnp.mean(resid * resid, axis=1, keepdims=True) + EPSILON)
    normed1_own = (resid * scale_one * gain_attn).astype(low)

    w_out, w_gate_up, w_down, cot_gate, _ = lax.optimization_barrier(
        (w_out, w_gate_up, w_down, cot_own, [p for p, _ in pieces_q[:size]])
    )
    wq = join(pieces_q, True, "join_qkv")
    wo = join(cross(w_out[None]), True, "join_out")
    wd = join(cross(w_down[None]), False, "join_down")
    wg = join(cross(w_gate_up.transpose(0, 2, 1)), False, "join_gate_up")
    half = wg.shape[0] // 2
    cot_full = wide_gather(cot_gate)

    positions = doc_positions(seg)
    cosine, sine = rope_tables(positions)
    starts = (jnp.arange(length, dtype=jnp.int32) - positions)[::BLK] // BLK
    marks = jnp.arange(length // BLK, dtype=jnp.int32)
    ends = jnp.sum((starts[None, :] <= marks[:, None]).astype(jnp.int32), axis=1) - 1

    normed1 = gather_call(normed1_own, [], [], no_block, "gather_normed1", 1, size)[0]
    qkv = qkv_call(normed1, wq, cosine, sine, heads)
    attn, lse = attend_call(qkv, seg, starts, heads, scale)

    row_shape = jax.ShapeDtypeStruct((part, width), full)
    row_low = jax.ShapeDtypeStruct((part, width), low)
    gain_shape = jax.ShapeDtypeStruct((16, width), full)
    hidden1, normed2_own = reduce_call(
        attn, wo, [tokens_own, gain_mlp], [row_shape, row_low], after_out, "reduce_out", 2, size
    )
    g_act = nt(cot_full, wd)
    half_shape = jax.ShapeDtypeStruct((length, half), low)
    normed2, act, g_gate, g_up = gather_call(
        normed2_own,
        [wg, g_act],
        [half_shape] * 3,
        functools.partial(mlp_block, half),
        "gather_mlp",
        3,
        size,
    )
    g_gu = jnp.concatenate([g_gate, g_up], axis=1)
    part_down, part_gu = tn(cot_full, act).astype(low), tn(normed2, g_gu).astype(low)
    g_gu, part_down, part_gu = lax.optimization_barrier((g_gu, part_down, part_gu))
    g_hidden1, g_branch_own, g_gain_mlp = reduce_call(
        g_gu,
        wg,
        [hidden1, cot_own, gain_mlp],
        [row_shape, row_low, gain_shape],
        after_mlp,
        "reduce_mlp",
        4,
        size,
    )
    down = lax.psum_scatter(nn(act, wd).astype(low), GROUP, scatter_dimension=0, tiled=True)
    output = (hidden1 + down.astype(full)).astype(low)
    output = lax.all_gather(output, "tp", axis=0, tiled=True)[None]

    g_branch, g_attn = gather_call(
        g_branch_own,
        [wo],
        [jax.ShapeDtypeStruct((length, heads * LANES), low)],
        attn_block,
        "gather_branch",
        5,
        size,
    )
    out_down = hand_out(part_down)
    out_gu = hand_out(part_gu)
    part_out = unspread(tn(g_branch, attn), 1).astype(low)
    g_attn, part_out = lax.optimization_barrier((g_attn, part_out))
    g_proj = attend_back_call(qkv, attn, g_attn, lse, seg, ends, cosine, sine, heads, scale)
    out_out = hand_out(part_out)
    part_qkv = unspread(tn(normed1, g_proj), 1).astype(low)
    g_proj, part_qkv = lax.optimization_barrier((g_proj, part_qkv))
    out_qkv = hand_out(part_qkv)
    g_tokens, g_gain_attn = reduce_call(
        g_proj,
        wq,
        [tokens_own, g_hidden1, gain_attn],
        [row_low, gain_shape],
        after_qkv,
        "reduce_qkv",
        6,
        size,
    )
    g_tokens = lax.all_gather(g_tokens, "tp", axis=0, tiled=True)[None]

    d = w_qkv.shape[1]
    grad_qkv = out_qkv.reshape(size, d, 3, -1).transpose(2, 1, 0, 3).reshape(3, d, -1)
    grad_gu = out_gu.reshape(size, d, 2, -1).transpose(2, 1, 0, 3).reshape(2, d, -1)
    grad_out = out_out.transpose(0, 2, 1).reshape(-1, d)
    grad_down = out_down.transpose(0, 2, 1).reshape(-1, d)

    gain_sums = lax.psum(
        jnp.stack([jnp.sum(g_gain_attn, axis=0), jnp.sum(g_gain_mlp, axis=0)]),
        ("fsdp", "ctx", "tp"),
    )
    mine = lax.axis_index("fsdp") * size + lax.axis_index("ctx")
    gain_grads = lax.dynamic_slice_in_dim(gain_sums, mine * d, d, 1)
    return (
        output,
        g_tokens,
        grad_qkv,
        grad_out,
        grad_gu,
        grad_down,
        gain_grads[0],
        gain_grads[1],
    )


def solution(mesh):
    in_specs = (
        P("fsdp", "ctx", None),
        P("fsdp", None),
        P(None, ("fsdp", "ctx"), "tp"),
        P("tp", ("fsdp", "ctx")),
        P(None, ("fsdp", "ctx"), "tp"),
        P("tp", ("fsdp", "ctx")),
        P(("fsdp", "ctx")),
        P(("fsdp", "ctx")),
        P("fsdp", "ctx", None),
    )
    out_specs = (
        P("fsdp", "ctx", None),
        P("fsdp", "ctx", None),
        P(None, ("fsdp", "ctx"), "tp"),
        P("tp", ("fsdp", "ctx")),
        P(None, ("fsdp", "ctx"), "tp"),
        P("tp", ("fsdp", "ctx")),
        P(("fsdp", "ctx")),
        P(("fsdp", "ctx")),
    )
    return jax.shard_map(shards, mesh=mesh, in_specs=in_specs, out_specs=out_specs, check_vma=False)
```

```python
import functools
import math

import jax
import jax.numpy as jnp
from jax import lax
from jax.experimental import pallas as pl
from jax.experimental.pallas import tpu as pltpu
from jax.sharding import PartitionSpec as P


HD = 96
HALF = HD // 2
LANES = 128
EPSILON = 1e-05
MASK_FILL = -1e30
ROPE_BASE = 10000.0
GROUP = ("ctx", "tp")
BLK = 256
GAIN_ROWS = 16
MESH = pl.DeviceIdType.MESH
SUBS = 2
VLIM = 64 * 1024 * 1024 - 65536


def cost(us):
    return pl.CostEstimate(flops=0, bytes_accessed=us * 3_000_000, transcendentals=0)


def near_order(c, j, size):
    low = c < size // 2
    base = jnp.where(low, c, size - 1 - c)
    zig = jnp.where(j % 2 == 1, base - (j + 1) // 2, base + j // 2)
    place = jnp.where(j <= 2 * base, zig, j)
    return jnp.where(low, place, size - 1 - place)


def places():
    c, t = lax.axis_index("ctx"), lax.axis_index("tp")
    return c, t // 2, t % 2


def greet(c, y, k, size):
    barrier = pltpu.get_barrier_semaphore()

    @pl.when(c < size - 1)
    def _():
        pl.semaphore_signal(barrier, inc=1, device_id={"ctx": c + 1}, device_id_type=MESH)

    @pl.when(c > 0)
    def _():
        pl.semaphore_signal(barrier, inc=1, device_id={"ctx": c - 1}, device_id_type=MESH)

    pl.semaphore_signal(barrier, inc=1, device_id={"tp": (1 - y) * 2 + k}, device_id_type=MESH)
    pl.semaphore_signal(barrier, inc=1, device_id={"tp": y * 2 + 1 - k}, device_id_type=MESH)
    pl.semaphore_wait(barrier, jnp.where((c > 0) & (c < size - 1), 4, 3))


def greet_all(c, y, k, size, groups):
    barrier = pltpu.get_barrier_semaphore()
    f = lax.axis_index("fsdp")

    def hello(dev):
        pl.semaphore_signal(barrier, inc=1, device_id=dev, device_id_type=MESH)

    for s in range(1, size):
        hello({"ctx": (c + s) % size})
    for g in range(1, groups):
        hello({"fsdp": (f + g) % groups})
    hello({"tp": (1 - y) * 2 + k})
    hello({"tp": y * 2 + 1 - k})
    pl.semaphore_wait(barrier, size + groups)


class Moves:
    def __init__(self, size, groups, sent, pieces, z_sems, x_sems):
        self.size, self.groups, self.sent, self.pieces = size, groups, sent, pieces
        self.z_sems, self.x_sems = z_sems, x_sems
        self.c, self.f = lax.axis_index("ctx"), lax.axis_index("fsdp")

    def z(self, w, s):
        to = (self.c + s) % self.size
        return pltpu.make_async_remote_copy(
            src_ref=self.sent[w].at[to],
            dst_ref=self.pieces[w].at[self.f * self.size + self.c],
            send_sem=self.z_sems.at[w, s - 1, 0],
            recv_sem=self.z_sems.at[w, s - 1, 1],
            device_id={"ctx": to},
            device_id_type=MESH,
        )

    def x(self, w, g, s):
        slot = self.pieces[w].at[self.f * self.size + (self.c + self.size - s) % self.size]
        return pltpu.make_async_remote_copy(
            src_ref=slot if s else self.sent[w].at[self.c],
            dst_ref=slot,
            send_sem=self.x_sems.at[w, g - 1, s, 0],
            recv_sem=self.x_sems.at[w, g - 1, s, 1],
            device_id={"fsdp": (self.f + g) % self.groups},
            device_id_type=MESH,
        )

    def start_z(self, w, s):
        self.z(w, s).start()

    def start_x(self, w, s):
        if s:
            self.z(w, s).wait_recv()
        for g in range(1, self.groups):
            self.x(w, g, s).start()

    def finish(self):
        for w in range(len(self.sent)):
            for s in range(self.size):
                if s:
                    self.z(w, s).wait_send()
                for g in range(1, self.groups):
                    self.x(w, g, s).wait()


class HandOut:
    def __init__(self, size, groups, part, out, got, mine, ready, x_sems, z_sems, l_sems):
        self.size, self.groups, self.part, self.out = size, groups, part, out
        self.got, self.mine, self.ready = got, mine, ready
        self.x_sems, self.z_sems, self.l_sems = x_sems, z_sems, l_sems
        self.c, self.f = lax.axis_index("ctx"), lax.axis_index("fsdp")
        self.d = mine.shape[1]

    def rows(self, f, c):
        return self.part.at[pl.ds(pl.multiple_of((f * self.size + c) * self.d, self.d), self.d)]

    def x(self, g, cc):
        to = (self.f + g) % self.groups
        return pltpu.make_async_remote_copy(
            src_ref=self.rows(to, cc),
            dst_ref=self.got.at[g - 1, cc],
            send_sem=self.x_sems.at[g - 1, cc, 0],
            recv_sem=self.x_sems.at[g - 1, cc, 1],
            device_id={"fsdp": to},
            device_id_type=MESH,
        )

    def load(self, cc):
        return pltpu.make_async_copy(self.rows(self.f, cc), self.mine.at[cc], self.l_sems.at[cc])

    def z(self, cc, source):
        return pltpu.make_async_remote_copy(
            src_ref=self.ready.at[cc],
            dst_ref=self.out.at[self.c],
            send_sem=self.z_sems.at[cc, 0],
            recv_sem=self.z_sems.at[source, 1],
            device_id={"ctx": cc},
            device_id_type=MESH,
        )

    def keep(self):
        return pltpu.make_async_copy(
            self.ready.at[self.c], self.out.at[self.c], self.l_sems.at[self.size]
        )

    def each(self, body):
        def one(i, carry):
            body(i)
            return carry

        lax.fori_loop(0, self.size, one, 0)

    def start(self, cc):
        for g in range(1, self.groups):
            self.x(g, cc).start()
        self.load(cc).start()

    def step(self, cc):
        self.load(cc).wait()
        for g in range(1, self.groups):
            self.x(g, cc).wait_recv()

        def add(i, carry):
            r = pl.ds(pl.multiple_of(i * 16, 16), 16)
            value = self.mine[cc, r, :].astype(jnp.float32)
            for g in range(1, self.groups):
                value = value + self.got[g - 1, cc, r, :].astype(jnp.float32)
            self.ready[cc, r, :] = value.astype(jnp.bfloat16)
            return carry

        lax.fori_loop(0, self.d // 16, add, 0)

        @pl.when(cc != self.c)
        def _():
            self.z(cc, self.c).start()

        @pl.when(cc == self.c)
        def _():
            self.keep().start()

    def finish(self):
        def one(cc):
            for g in range(1, self.groups):
                self.x(g, cc).wait_send()

            @pl.when(cc != self.c)
            def _():
                self.z(cc, self.c).wait_send()
                self.z(cc, cc).wait_recv()

        self.each(one)
        self.keep().wait()


def gather_kernel(size, groups, plan, n_move, part, n_in, n_out, compute, *refs):
    x_ref = refs[0]
    hbm_ins = refs[1 : 1 + n_in]
    sent = refs[1 + n_in : 1 + n_in + n_move]
    refs = refs[1 + n_in + n_move :]
    full_ref = refs[0]
    outs = refs[1 : 1 + n_out]
    moved = refs[1 + n_out : 1 + n_out + n_move]
    refs = refs[1 + n_out + n_move :]
    ins = refs[:n_in]
    buf, recv, zs, ys, ks, local, load, in_sems, *move_sems = refs[n_in:]
    moves = Moves(size, groups, sent, moved, *move_sems) if n_move else None
    c, y, k = places()
    sub = part // SUBS

    def slot(cc, yy, kk, s):
        return buf.at[cc * 2 + yy, pl.ds(pl.multiple_of(kk * part + s * sub, sub), sub)]

    def copy(cc, yy, kk, s, sem, dev):
        return pltpu.make_async_remote_copy(
            src_ref=slot(cc, yy, kk, s),
            dst_ref=slot(cc, yy, kk, s),
            send_sem=sem,
            recv_sem=recv.at[cc * 2 + yy, kk, s],
            device_id=dev,
            device_id_type=MESH,
        )

    up, down = {"ctx": c + 1}, {"ctx": c - 1}
    ydev, kdev = {"tp": (1 - y) * 2 + k}, {"tp": y * 2 + 1 - k}

    def z_up(cc, s):
        return copy(cc, y, k, s, zs.at[0, cc, s], up)

    def z_down(cc, s):
        return copy(cc, y, k, s, zs.at[1, cc, s], down)

    def y_send(cc, s):
        return copy(cc, y, k, s, ys.at[cc, s], ydev)

    def k_send(cc, yy, s):
        return copy(cc, yy, k, s, ks.at[cc * 2 + yy, s], kdev)

    def pair_out(cc, yy):
        pair = cc * 2 + yy
        return pltpu.make_async_copy(
            buf.at[pair],
            full_ref.at[pl.ds(pl.multiple_of(pair * 2 * part, 2 * part), 2 * part)],
            local.at[pair],
        )

    def got(cc, yy, kk, s):
        copy(cc, yy, kk, s, ys.at[0, 0], ydev).wait_recv()

    mine = buf.at[c * 2 + y, pl.ds(pl.multiple_of(k * part, part), part)]
    first = pltpu.make_async_copy(x_ref, mine, load)
    first.start()
    for i in range(n_in):
        pltpu.make_async_copy(hbm_ins[i], ins[i], in_sems.at[i]).start()
    if moves:
        greet_all(c, y, k, size, groups)
    else:
        greet(c, y, k, size)
    first.wait()

    def z_stage(cc, s):
        @pl.when((cc <= c) & (c < size - 1))
        def _():
            z_up(cc, s).start()

        @pl.when((cc >= c) & (c > 0))
        def _():
            z_down(cc, s).start()

        y_send(cc, s).start()
        k_send(cc, y, s).start()

    for s in range(SUBS):
        z_stage(c, s)

    def move_on(step):
        for kind, w, s in plan.get(step, ()):
            (moves.start_z if kind == "z" else moves.start_x)(w, s)

    move_on(-1)
    for i in range(n_in):
        pltpu.make_async_copy(hbm_ins[i], ins[i], in_sems.at[i]).wait()

    def finish(cc, yy):
        for s in range(SUBS):
            got(cc, yy, 1 - k, s)
        pair_out(cc, yy).start()
        compute(cc * 2 + yy, buf, ins, outs)

    def step(r, carry):
        for s in range(SUBS):
            for sign in (-1, 1):
                nxt = c + sign * (r + 1)

                @pl.when((nxt >= 0) & (nxt < size))
                def _():
                    got(nxt, y, k, s)
                    z_stage(nxt, s)

            for sign in (-1, 1):
                cc = c + sign * r

                @pl.when((cc >= 0) & (cc < size) & ((r > 0) | (sign > 0)))
                def _():
                    if s == SUBS - 1:
                        finish(cc, y)
                    got(cc, 1 - y, k, s)
                    k_send(cc, 1 - y, s).start()
                    if s == SUBS - 1:
                        finish(cc, 1 - y)

        for at in sorted(plan):
            if at >= 0:

                @pl.when(r == at)
                def _():
                    move_on(at)

        return carry

    lax.fori_loop(0, size, step, 0)

    def drain(cc, carry):
        for s in range(SUBS):
            @pl.when((cc <= c) & (c < size - 1))
            def _():
                z_up(cc, s).wait_send()

            @pl.when((cc >= c) & (c > 0))
            def _():
                z_down(cc, s).wait_send()

            y_send(cc, s).wait_send()
            for yy in range(2):
                k_send(cc, yy, s).wait_send()
        for yy in range(2):
            pair_out(cc, yy).wait()
        return carry

    lax.fori_loop(0, size, drain, 0)
    if moves:
        moves.finish()


def gather_call(x, ins, out_shapes, compute, cid, size, sent=(), plan=None):
    part, width = x.shape
    groups = lax.axis_size("fsdp")
    dma = pltpu.SemaphoreType.DMA
    any_spec = pl.BlockSpec(memory_space=pl.ANY)
    vmem = pl.BlockSpec(memory_space=pltpu.VMEM)
    full = jax.ShapeDtypeStruct((size * 4 * part, width), x.dtype)
    return pl.pallas_call(
        functools.partial(
            gather_kernel,
            size,
            groups,
            plan or {},
            len(sent),
            part,
            len(ins),
            len(out_shapes),
            compute,
        ),
        out_shape=(
            full,
            *out_shapes,
            *(
                jax.ShapeDtypeStruct((groups * size, *one.shape[1:]), one.dtype)
                for one in sent
            ),
        ),
        in_specs=[any_spec] * (1 + len(ins) + len(sent)),
        out_specs=(any_spec, *([vmem] * len(out_shapes)), *([any_spec] * len(sent))),
        scratch_shapes=[
            *(pltpu.VMEM(one.shape, one.dtype) for one in ins),
            pltpu.VMEM((size * 2, 2 * part, width), x.dtype),
            pltpu.SemaphoreType.DMA((size * 2, 2, SUBS)),
            pltpu.SemaphoreType.DMA((2, size, SUBS)),
            pltpu.SemaphoreType.DMA((size, SUBS)),
            pltpu.SemaphoreType.DMA((size * 2, SUBS)),
            pltpu.SemaphoreType.DMA((size * 2,)),
            pltpu.SemaphoreType.DMA,
            pltpu.SemaphoreType.DMA((max(len(ins), 1),)),
            *(
                [dma((len(sent), size - 1, 2)), dma((len(sent), max(groups - 1, 1), size, 2))]
                if sent
                else []
            ),
        ],
        compiler_params=pltpu.CompilerParams(
            collective_id=cid, has_side_effects=True, vmem_limit_bytes=VLIM
        ),
        cost_estimate=cost(75),
    )(x, *ins, *sent)


def reduce_kernel(size, groups, last, plan, n_move, part, n_in, n_out, final, *refs):
    a_ref, w_ref = refs[:2]
    ins = refs[2 : 2 + n_in]
    sent = refs[2 + n_in : 2 + n_in + n_move]
    refs = refs[n_move:]
    outs = refs[2 + n_in : 2 + n_in + n_out]
    moved = refs[2 + n_in + n_out : 2 + n_in + n_out + n_move]
    refs = refs[n_move:]
    (
        own,
        ksend,
        krecv,
        ysend,
        yrecv,
        qown,
        zsend,
        zrecv,
        total,
        prod,
        k_sems,
        y_sems,
        z_sems,
        *extra,
    ) = refs[2 + n_in + n_out :]
    moves = Moves(size, groups, sent, moved, *extra) if n_move else None
    hand = HandOut(size, groups, ins[-1], outs[2], *extra[9:]) if last else None
    c, y, k = places()
    depth = a_ref.shape[1]
    chunk = 16
    tile = 512
    width = total.shape[1]

    sub = part // SUBS

    def remote(src, dst, sems, dev):
        return pltpu.make_async_remote_copy(
            src_ref=src,
            dst_ref=dst,
            send_sem=sems.at[0],
            recv_sem=sems.at[1],
            device_id=dev,
            device_id_type=MESH,
        )

    ydev, kdev = {"tp": (1 - y) * 2 + k}, {"tp": y * 2 + 1 - k}

    def k_copy(cc, yy):
        pair = cc * 2 + yy
        return remote(ksend.at[pair], krecv.at[pair], k_sems.at[pair], kdev)

    def y_copy(cc, s):
        r = pl.ds(s * sub, sub)
        return remote(ysend.at[cc, r], yrecv.at[cc, r], y_sems.at[cc, s], ydev)

    def z_up(cc, s):
        r = pl.ds(s * sub, sub)
        return remote(zsend.at[cc, r], zrecv.at[0, cc, r], z_sems.at[0, cc, s], {"ctx": c + 1})

    def z_down(cc, s):
        r = pl.ds(s * sub, sub)
        return remote(zsend.at[cc, r], zrecv.at[1, cc, r], z_sems.at[1, cc, s], {"ctx": c - 1})

    if last or moves:
        greet_all(c, y, k, size, groups)
    else:
        greet(c, y, k, size)

    def move_on(step):
        for kind, w, s in plan.get(step, ()):
            (moves.start_z if kind == "z" else moves.start_x)(w, s)

    move_on(-1)

    def rows(i):
        return pl.ds(pl.multiple_of(i * chunk, chunk), chunk)

    def sweep(body, s=None):
        steps = part // chunk
        lo, hi = (0, steps) if s is None else (s * steps // SUBS, (s + 1) * steps // SUBS)

        def one(i, carry):
            body(rows(i))
            return carry

        lax.fori_loop(lo, hi, one, 0)

    def produce(cc, yy, keep):
        pair = cc * 2 + yy
        both = pl.ds(pl.multiple_of(pair * 2 * part, 2 * part), 2 * part)
        mine = pl.ds(pl.multiple_of(k * part, part), part)
        other = pl.ds(pl.multiple_of((1 - k) * part, part), part)

        def one(i, carry):
            lanes = pl.ds(pl.multiple_of(i * tile, tile), tile)
            prod[...] = jnp.dot(
                a_ref[both, :], w_ref[0:depth, lanes], preferred_element_type=jnp.float32
            )
            ksend[pair, :, lanes] = prod[other, :].astype(jnp.bfloat16)
            own[keep, :, lanes] = prod[mine, :]
            return carry

        lax.fori_loop(0, width // tile, one, 0)
        k_copy(cc, yy).start()

    def first(j):
        cc = near_order(c, size - 1 - j, size)
        if last:
            hand.start(cc)
        produce(cc, 1 - y, 0)
        k_copy(cc, 1 - y).wait_recv()

        def add_y(r):
            got = krecv[cc * 2 + 1 - y, r, :].astype(jnp.float32)
            ysend[cc, r, :] = (own[0, r, :] + got).astype(jnp.bfloat16)

        for s in range(SUBS):
            sweep(add_y, s)
            y_copy(cc, s).start()
        produce(cc, y, 1)
        k_copy(cc, y).wait_recv()

        def add_k(r):
            qown[cc, r, :] = own[1, r, :] + krecv[cc * 2 + y, r, :].astype(jnp.float32)

        sweep(add_k)

    def pass_on(cc, s, into, edge, send):
        @pl.when(jnp.logical_not(edge))
        def _():
            send(cc, s).wait_recv()

            def add(r):
                part_sum = qown[cc, r, :] + yrecv[cc, r, :].astype(jnp.float32)
                zsend[cc, r, :] = (part_sum + zrecv[into, cc, r, :].astype(jnp.float32)).astype(
                    jnp.bfloat16
                )

            sweep(add, s)

        @pl.when(edge)
        def _():
            def add(r):
                part_sum = qown[cc, r, :] + yrecv[cc, r, :].astype(jnp.float32)
                zsend[cc, r, :] = part_sum.astype(jnp.bfloat16)

            sweep(add, s)

        send(cc, s).start()

    def second(j):
        cc = near_order(c, size - 1 - j, size)
        for s in range(SUBS):

            @pl.when(cc > c)
            def _():
                y_copy(cc, s).wait_recv()
                pass_on(cc, s, 0, c == 0, z_up)

            @pl.when(cc < c)
            def _():
                y_copy(cc, s).wait_recv()
                pass_on(cc, s, 1, c == size - 1, z_down)

        if last:
            hand.step(cc)

        for at in sorted(plan):
            if at >= 0:

                @pl.when(j == at)
                def _():
                    move_on(at)

    lag = jnp.where((c == 0) | (c == size - 1), 1, 2)

    def both(i, carry):
        @pl.when(i < size)
        def _():
            first(i)

        @pl.when((i >= lag) & (i - lag < size))
        def _():
            second(i - lag)

        return carry

    lax.fori_loop(0, size + 2, both, 0)

    def sum_up(r):
        own_sum = qown[c, r, :] + yrecv[c, r, :].astype(jnp.float32)

        @pl.when(c == 0)
        def _():
            total[r, :] = own_sum + zrecv[1, c, r, :].astype(jnp.float32)

        @pl.when(c == size - 1)
        def _():
            total[r, :] = own_sum + zrecv[0, c, r, :].astype(jnp.float32)

        @pl.when((c > 0) & (c < size - 1))
        def _():
            below = own_sum + zrecv[0, c, r, :].astype(jnp.float32)
            total[r, :] = below + zrecv[1, c, r, :].astype(jnp.float32)

    begin, one_chunk, end = final(total, ins, outs, extra)
    begin()
    for s in range(SUBS):
        y_copy(c, s).wait_recv()

        @pl.when(c > 0)
        def _():
            z_up(c, s).wait_recv()

        @pl.when(c < size - 1)
        def _():
            z_down(c, s).wait_recv()

        def close(r):
            sum_up(r)
            one_chunk(r)

        sweep(close, s)
    end()
    if last:
        spread_out(size, groups, c, y, k, ydev, kdev, outs, extra)

    def drain(cc, carry):
        for yy in range(2):
            k_copy(cc, yy).wait_send()
        for s in range(SUBS):
            y_copy(cc, s).wait_send()

            @pl.when(cc > c)
            def _():
                z_up(cc, s).wait_send()

            @pl.when(cc < c)
            def _():
                z_down(cc, s).wait_send()

        return carry

    lax.fori_loop(0, size, drain, 0)
    if moves:
        moves.finish()
    if last:
        hand.finish()


def spread_out(size, groups, c, y, k, ydev, kdev, outs, extra):
    rows_all, sums, got, row_sems, k_sem, y_sem, f_sems, z_sems, out_sem = extra[:9]
    f = lax.axis_index("fsdp")

    def copy(src, dst, sems, dev):
        return pltpu.make_async_remote_copy(
            src_ref=src,
            dst_ref=dst,
            send_sem=sems.at[0],
            recv_sem=sems.at[1],
            device_id=dev,
            device_id_type=MESH,
        )

    def row_copy(yy, kk, n, dev):
        slot = rows_all.at[yy * 2 + kk]
        return copy(slot, slot, row_sems.at[n], dev)

    to_y, to_k, on_k = row_copy(y, k, 0, ydev), row_copy(y, k, 1, kdev), row_copy(1 - y, k, 2, kdev)
    to_y.start()
    to_k.start()

    def add(n, first, count):
        value = sums[n]
        for i in range(first, first + count):
            value = value + got[i]
        sums[n + 1] = value

    swap_k = copy(sums.at[0], got.at[0], k_sem, kdev)
    swap_k.start()
    swap_k.wait()
    add(0, 0, 1)
    swap_y = copy(sums.at[1], got.at[1], y_sem, ydev)
    swap_y.start()
    swap_y.wait()
    add(1, 1, 1)
    swaps = [
        copy(sums.at[2], got.at[1 + g], f_sems.at[g - 1], {"fsdp": (f + g) % groups})
        for g in range(1, groups)
    ]
    for one in swaps:
        one.start()
    for one in swaps:
        one.wait()
    add(2, 2, groups - 1)
    swaps = [
        copy(sums.at[3], got.at[groups + s], z_sems.at[s - 1], {"ctx": (c + s) % size})
        for s in range(1, size)
    ]
    for one in swaps:
        one.start()
    row_copy(1 - y, k, 0, ydev).wait_recv()
    on_k.start()
    for one in swaps:
        one.wait()
    add(3, groups + 1, size - 1)
    outs[1][...] = sums[4]
    row_copy(y, 1 - k, 1, kdev).wait_recv()
    row_copy(1 - y, 1 - k, 2, kdev).wait_recv()
    to_y.wait_send()
    to_k.wait_send()
    on_k.wait_send()
    out = pltpu.make_async_copy(rows_all, outs[0], out_sem)
    out.start()
    out.wait()


def reduce_call(a, w, ins, out_shapes, final, cid, size, last=False, sent=(), plan=None):
    width = w.shape[1]
    part = a.shape[0] // (size * 4)
    vmem = pl.BlockSpec(memory_space=pltpu.VMEM)
    low, full = jnp.bfloat16, jnp.float32
    groups = lax.axis_size("fsdp")
    any_spec = pl.BlockSpec(memory_space=pl.ANY)
    dma = pltpu.SemaphoreType.DMA
    out_specs, extra = [vmem] * len(out_shapes), []
    if sent:
        extra = [dma((len(sent), size - 1, 2)), dma((len(sent), max(groups - 1, 1), size, 2))]
    if last:
        out_specs[0] = out_specs[2] = any_spec
        extra = [
            pltpu.VMEM((4, part, width), low),
            pltpu.VMEM((5, 8, width), full),
            pltpu.VMEM((groups + size, 8, width), full),
            dma((3, 2)),
            dma((2,)),
            dma((2,)),
            dma((max(groups - 1, 1), 2)),
            dma((size - 1, 2)),
            dma,
            pltpu.VMEM((max(groups - 1, 1), *out_shapes[2].shape), low),
            pltpu.VMEM(out_shapes[2].shape, low),
            pltpu.VMEM(out_shapes[2].shape, low),
            dma((max(groups - 1, 1), size, 2)),
            dma((size, 2)),
            dma((size + 1,)),
        ]
    return pl.pallas_call(
        functools.partial(
            reduce_kernel,
            size,
            groups,
            last,
            plan or {},
            len(sent),
            part,
            len(ins),
            len(out_shapes),
            final,
        ),
        out_shape=(
            *out_shapes,
            *(
                jax.ShapeDtypeStruct((groups * size, *one.shape[1:]), one.dtype)
                for one in sent
            ),
        ),
        in_specs=[vmem] * (1 + len(ins))
        + [any_spec if last else vmem]
        + [any_spec] * len(sent),
        out_specs=(*out_specs, *([any_spec] * len(sent))),
        scratch_shapes=[
            pltpu.VMEM((2, part, width), full),
            pltpu.VMEM((size * 2, part, width), low),
            pltpu.VMEM((size * 2, part, width), low),
            pltpu.VMEM((size, part, width), low),
            pltpu.VMEM((size, part, width), low),
            pltpu.VMEM((size, part, width), full),
            pltpu.VMEM((size, part, width), low),
            pltpu.VMEM((2, size, part, width), low),
            pltpu.VMEM((part, width), full),
            pltpu.VMEM((2 * part, 512), full),
            pltpu.SemaphoreType.DMA((size * 2, 2)),
            pltpu.SemaphoreType.DMA((size, SUBS, 2)),
            pltpu.SemaphoreType.DMA((2, size, SUBS, 2)),
            *extra,
        ],
        compiler_params=pltpu.CompilerParams(
            collective_id=cid, has_side_effects=True, vmem_limit_bytes=VLIM
        ),
        cost_estimate=cost(85),
    )(a, w, *ins, *sent)


def doc_positions(segment_row):
    places_in = jnp.arange(segment_row.shape[0], dtype=jnp.int32)
    starts = jnp.concatenate([jnp.ones((1,), dtype=jnp.bool_), segment_row[1:] != segment_row[:-1]])
    first = lax.cummax(jnp.where(starts, places_in, jnp.zeros_like(places_in)), axis=0)
    return places_in - first


def rope_tables(positions):
    freqs = ROPE_BASE ** (-(jnp.arange(HALF, dtype=jnp.float32) * 2.0 / HD))
    angles = positions.astype(jnp.float32)[:, None] * freqs
    gap = jnp.zeros((positions.shape[0], LANES // 2 - HALF), jnp.float32)
    cosine, sine = jnp.cos(angles), jnp.sin(angles)
    return (
        jnp.concatenate([cosine, gap, cosine, gap], axis=1),
        jnp.concatenate([-sine, gap, sine, gap], axis=1),
    )


def spread(array, axis):
    shape = array.shape
    halves = array.reshape(*shape[:axis], shape[axis] // HALF, HALF, *shape[axis + 1 :])
    pads = [(0, 0)] * halves.ndim
    pads[axis + 1] = (0, LANES // 2 - HALF)
    wide = jnp.pad(halves, pads)
    return wide.reshape(*shape[:axis], -1, *shape[axis + 1 :])


def unspread(array, axis):
    shape = array.shape
    half = LANES // 2
    halves = array.reshape(*shape[:axis], shape[axis] // half, half, *shape[axis + 1 :])
    kept = lax.slice_in_dim(halves, 0, HALF, axis=axis + 1)
    return kept.reshape(*shape[:axis], -1, *shape[axis + 1 :])


def nt(left, right):
    return lax.dot_general(left, right, (((1,), (1,)), ((), ())), preferred_element_type=jnp.float32)


def nn(left, right):
    return jnp.dot(left, right, preferred_element_type=jnp.float32)


def tn(left, right):
    return lax.dot_general(left, right, (((0,), (0,)), ((), ())), preferred_element_type=jnp.float32)


def qkv_kernel(heads, x_ref, w_ref, gain_ref, cos_ref, sin_ref, out_ref, normed_ref):
    for i in range(BLK // 16):
        at = slice(i * 16, (i + 1) * 16)
        x = x_ref[at, :].astype(jnp.float32)
        scale = lax.rsqrt(jnp.mean(x * x, axis=1, keepdims=True) + EPSILON)
        normed_ref[at, :] = (x * scale * gain_ref[...]).astype(jnp.bfloat16)
    proj = nt(normed_ref[...], w_ref[...])
    for i in range(3 * heads):
        cut = slice(i * LANES, (i + 1) * LANES)
        one = proj[:, cut]
        if i < 2 * heads:
            one = one * cos_ref[...] + pltpu.roll(one, LANES // 2, 1) * sin_ref[...]
        out_ref[:, cut] = one.astype(jnp.bfloat16)


def qkv_call(x, w, gain, cosine, sine, heads):
    rows, width = x.shape
    tall = 3 * heads * LANES
    return pl.pallas_call(
        functools.partial(qkv_kernel, heads),
        out_shape=(
            jax.ShapeDtypeStruct((rows, tall), jnp.bfloat16),
            jax.ShapeDtypeStruct((rows, width), jnp.bfloat16),
        ),
        grid=(rows // BLK,),
        in_specs=[
            pl.BlockSpec((BLK, width), lambda i: (i, 0)),
            pl.BlockSpec((tall, width), lambda i: (0, 0)),
            pl.BlockSpec((1, width), lambda i: (0, 0)),
            pl.BlockSpec((BLK, LANES), lambda i: (i, 0)),
            pl.BlockSpec((BLK, LANES), lambda i: (i, 0)),
        ],
        out_specs=(
            pl.BlockSpec((BLK, tall), lambda i: (i, 0)),
            pl.BlockSpec((BLK, width), lambda i: (i, 0)),
        ),
        compiler_params=pltpu.CompilerParams(vmem_limit_bytes=VLIM),
        cost_estimate=cost(18),
        name="qkv",
    )(x, w, gain, cosine, sine)


def block(ref, i, head):
    return ref[pl.ds(pl.multiple_of(i * BLK, BLK), BLK), head * LANES : (head + 1) * LANES]


def masked_scores(keys, query, seg_col, seg_row, kb, qb, scale):
    scores = nt(keys, query) * scale
    key_pos = kb * BLK + lax.broadcasted_iota(jnp.int32, scores.shape, 0)
    query_pos = qb * BLK + lax.broadcasted_iota(jnp.int32, scores.shape, 1)
    return jnp.where((key_pos <= query_pos) & (seg_col == seg_row), scores, MASK_FILL)


def attend_kernel(heads, scale, low_ref, qkv_ref, col_ref, row_ref, out_ref, lse_ref):
    blocks = qkv_ref.shape[0] // BLK

    def one(i, carry):
        cut = pl.ds(pl.multiple_of(i * BLK, BLK), BLK)
        seg_row = row_ref[:, cut]
        for h in range(heads):
            query = block(qkv_ref, i, h)

            def inner(kb, state):
                peak, total, acc = state
                keys = block(qkv_ref, kb, heads + h)
                seg_col = col_ref[pl.ds(pl.multiple_of(kb * BLK, BLK), BLK), :]
                scores = masked_scores(keys, query, seg_col, seg_row, kb, i, scale)
                new = jnp.maximum(peak, jnp.max(scores, axis=0, keepdims=True))
                fade = jnp.exp(peak - new)
                expo = jnp.exp(scores - new)
                total = total * fade + jnp.sum(expo, axis=0, keepdims=True)
                mixed = tn(block(qkv_ref, kb, 2 * heads + h), expo.astype(jnp.bfloat16))
                return new, total, acc * fade + mixed

            peak, total, acc = lax.fori_loop(
                low_ref[i],
                i + 1,
                inner,
                (
                    jnp.full((1, BLK), MASK_FILL, jnp.float32),
                    jnp.zeros((1, BLK), jnp.float32),
                    jnp.zeros((LANES, BLK), jnp.float32),
                ),
            )
            out_ref[cut, h * LANES : (h + 1) * LANES] = (acc / total).T.astype(jnp.bfloat16)
            lse_ref[h : h + 1, cut] = peak + jnp.log(total)
        return carry

    lax.fori_loop(0, blocks, one, 0)


def attend_call(qkv, seg, low, heads, scale):
    rows = qkv.shape[0]
    vmem = pl.BlockSpec(memory_space=pltpu.VMEM)
    return pl.pallas_call(
        functools.partial(attend_kernel, heads, scale),
        out_shape=(
            jax.ShapeDtypeStruct((rows, heads * LANES), jnp.bfloat16),
            jax.ShapeDtypeStruct((heads, rows), jnp.float32),
        ),
        in_specs=[pl.BlockSpec(memory_space=pltpu.SMEM), vmem, vmem, vmem],
        out_specs=(vmem, vmem),
        compiler_params=pltpu.CompilerParams(vmem_limit_bytes=VLIM),
        cost_estimate=cost(20),
        name="attend",
    )(low, qkv, seg[:, None], seg[None, :])


def attend_back_kernel(
    heads,
    scale,
    high_ref,
    qkv_ref,
    out_ref,
    grad_ref,
    lse_ref,
    col_ref,
    row_ref,
    cos_ref,
    sin_ref,
    res_ref,
    delta_ref,
    gq_ref,
):
    blocks = qkv_ref.shape[0] // BLK
    gq_ref[...] = jnp.zeros_like(gq_ref)

    def dots(i, carry):
        cut = pl.ds(pl.multiple_of(i * BLK, BLK), BLK)
        for h in range(heads):
            prod = block(out_ref, i, h).astype(jnp.float32) * block(grad_ref, i, h).astype(
                jnp.float32
            )
            delta_ref[h : h + 1, cut] = jnp.sum(prod.T, axis=0, keepdims=True)
        return carry

    lax.fori_loop(0, blocks, dots, 0)

    def turn_back(value, cut):
        low = value.astype(jnp.bfloat16).astype(jnp.float32)
        turned = low * cos_ref[cut, :] - pltpu.roll(low, LANES // 2, 1) * sin_ref[cut, :]
        return turned.astype(jnp.bfloat16)

    def one(kb, carry):
        cut = pl.ds(pl.multiple_of(kb * BLK, BLK), BLK)
        seg_col = col_ref[cut, :]
        for h in range(heads):
            keys = block(qkv_ref, kb, heads + h)
            values = block(qkv_ref, kb, 2 * heads + h)

            def inner(i, state):
                gk, gv = state
                at = pl.ds(pl.multiple_of(i * BLK, BLK), BLK)
                query = block(qkv_ref, i, h)
                grad = block(grad_ref, i, h)
                scores = masked_scores(keys, query, seg_col, row_ref[:, at], kb, i, scale)
                probs = jnp.exp(scores - lse_ref[h : h + 1, at])
                gv = gv + nn(probs.astype(jnp.bfloat16), grad)
                g_probs = nt(values, grad)
                g_scores = (probs * (g_probs - delta_ref[h : h + 1, at])).astype(jnp.bfloat16)
                gk = gk + nn(g_scores, query)
                lanes = slice(h * LANES, (h + 1) * LANES)
                gq_ref[at, lanes] += tn(g_scores, keys)
                return gk, gv

            zero = jnp.zeros((BLK, LANES), jnp.float32)
            gk, gv = lax.fori_loop(kb, high_ref[kb] + 1, inner, (zero, zero))
            at_k = slice((heads + h) * LANES, (heads + h + 1) * LANES)
            at_v = slice((2 * heads + h) * LANES, (2 * heads + h + 1) * LANES)
            res_ref[cut, at_k] = turn_back(gk * scale, cut)
            res_ref[cut, at_v] = gv.astype(jnp.bfloat16)
        return carry

    lax.fori_loop(0, blocks, one, 0)

    def close(i, carry):
        cut = pl.ds(pl.multiple_of(i * BLK, BLK), BLK)
        for h in range(heads):
            lanes = slice(h * LANES, (h + 1) * LANES)
            res_ref[cut, lanes] = turn_back(gq_ref[cut, lanes] * scale, cut)
        return carry

    lax.fori_loop(0, blocks, close, 0)


def attend_back_call(qkv, out, grad, lse, seg, high, cosine, sine, heads, scale):
    rows = qkv.shape[0]
    vmem = pl.BlockSpec(memory_space=pltpu.VMEM)
    return pl.pallas_call(
        functools.partial(attend_back_kernel, heads, scale),
        out_shape=jax.ShapeDtypeStruct(qkv.shape, jnp.bfloat16),
        in_specs=[pl.BlockSpec(memory_space=pltpu.SMEM)] + [vmem] * 8,
        out_specs=vmem,
        scratch_shapes=[
            pltpu.VMEM((heads, rows), jnp.float32),
            pltpu.VMEM((rows, heads * LANES), jnp.float32),
        ],
        compiler_params=pltpu.CompilerParams(vmem_limit_bytes=VLIM),
        cost_estimate=cost(32),
        name="attend_back",
    )(high, qkv, out, grad, lse, seg[:, None], seg[None, :], cosine, sine)


def join_kernel(cuts, groups, size, d, *refs):
    *pieces, out, sems = refs
    c, f = lax.axis_index("ctx"), lax.axis_index("fsdp")

    def copies(go):
        for i in range(groups * size):
            g, s = i // size, i % size
            place = ((f + groups - g) % groups) * size + (c + size - s) % size
            lanes = pl.ds(pl.multiple_of(place * d, d), d)
            for q, (src, dst, rows) in enumerate(cuts):
                if len(pieces) > 2:
                    piece = pieces[i]
                else:
                    piece = pieces[1].at[place] if i else pieces[0].at[c]
                go(
                    pltpu.make_async_copy(
                        piece.at[pl.ds(src, rows)], out.at[pl.ds(dst, rows), lanes], sems.at[i, q]
                    )
                )

    copies(lambda one: one.start())
    for q, (_, dst, rows) in enumerate(cuts):
        stop = cuts[q + 1][1] if q + 1 < len(cuts) else out.shape[0]
        if dst + rows < stop:
            gap = stop - dst - rows
            out[pl.ds(dst + rows, gap), :] = jnp.zeros((gap, out.shape[1]), out.dtype)
    copies(lambda one: one.wait())


def join(sent, pieces, spaced, tail=0):
    size, groups = lax.axis_size("ctx"), lax.axis_size("fsdp")
    c, f = lax.axis_index("ctx"), lax.axis_index("fsdp")
    count, (n, d) = size * groups, sent.shape[1:]
    n = n - tail
    width = count * d
    if d % LANES:
        own = lax.dynamic_slice_in_dim(sent, c, 1, 0)
        if isinstance(pieces, list):
            buf = jnp.zeros((count, n + tail, d), sent.dtype)
            for i, one in enumerate(pieces):
                g, s = i // size, i % size
                place = ((f + groups - g) % groups) * size + (c + size - s) % size
                buf = lax.dynamic_update_slice(buf, one[None], (place, 0, 0))
        else:
            buf = lax.dynamic_update_slice(pieces, own, (f * size + c, 0, 0))
        flat = buf.transpose(1, 0, 2).reshape(n + tail, width)
        return jnp.concatenate([spread(flat[:n], 0), flat[n:]]) if spaced else flat
    cuts = [(0, 0, n)]
    if spaced:
        cuts = [(i * HALF, i * LANES // 2, HALF) for i in range(n // HALF)]
    tall = n * LANES // HD if spaced else n
    if tail:
        cuts.append((n, tall, tail))
        tall += tail
    refs = pieces if isinstance(pieces, list) else [sent, pieces]
    return pl.pallas_call(
        functools.partial(join_kernel, cuts, groups, size, d),
        out_shape=jax.ShapeDtypeStruct((tall, width), sent.dtype),
        in_specs=[pl.BlockSpec(memory_space=pl.ANY)] * len(refs),
        out_specs=pl.BlockSpec(memory_space=pltpu.VMEM),
        scratch_shapes=[pltpu.SemaphoreType.DMA((count, len(cuts)))],
        compiler_params=pltpu.CompilerParams(vmem_limit_bytes=VLIM),
        cost_estimate=cost(4),
    )(*refs)


def cross(sent):
    size, groups = lax.axis_size("ctx"), lax.axis_size("fsdp")
    c = lax.axis_index("ctx")
    pieces = []
    for s in range(size):
        piece = lax.dynamic_index_in_dim(sent, (c + s) % size, 0, False)
        if s:
            piece = lax.ppermute(piece, "ctx", [(i, (i + s) % size) for i in range(size)])
        pieces.append(piece)
    for g in range(1, groups):
        for s in range(size):
            pieces.append(
                lax.ppermute(
                    pieces[s], "fsdp", [(i, (i + g) % groups) for i in range(groups)]
                )
            )
    return pieces


def hand_out(grad, beside=None):
    size, groups = lax.axis_size("ctx"), lax.axis_size("fsdp")
    c, f = lax.axis_index("ctx"), lax.axis_index("fsdp")
    rows = grad.shape[0] // groups
    d = rows // size
    total = lax.dynamic_slice_in_dim(grad, f * rows, rows, 0)
    for g in range(1, groups):
        sent = lax.dynamic_slice_in_dim(grad, ((f + g) % groups) * rows, rows, 0)
        got = lax.ppermute(sent, "fsdp", [(i, (i + g) % groups) for i in range(groups)])
        total = total.astype(jnp.float32) + got.astype(jnp.float32)
    total = total.astype(jnp.bfloat16)
    if beside is not None:
        total, beside = lax.optimization_barrier((total, beside))
    out = jnp.zeros((size, d, grad.shape[1]), jnp.bfloat16)
    for s in range(size):
        piece = lax.dynamic_slice_in_dim(total, ((c + s) % size) * d, d, 0)
        if s:
            piece = lax.ppermute(piece, "ctx", [(i, (i + s) % size) for i in range(size)])
        out = lax.dynamic_update_slice(out, piece[None], ((c - s) % size, 0, 0))
    return out if beside is None else (out, beside)


def wide_gather(part):
    full = lax.all_gather(part, GROUP, axis=0, tiled=True)
    return full


def mlp_block(half, pair, buf, ins, outs):
    w, wd, cot = ins
    act, g_gate, g_up = outs
    rows = buf.shape[1]
    tile = 256
    at = pl.ds(pl.multiple_of(pair * rows, rows), rows)

    def one(i, carry):
        lanes = pl.ds(pl.multiple_of(i * tile, tile), tile)
        gate = nt(buf[pair], w[lanes, :])
        up = nt(buf[pair], w[pl.ds(pl.multiple_of(half + i * tile, tile), tile), :])
        grad = nt(cot[at, :], wd[lanes, :])
        sigma = 1.0 / (1.0 + jnp.exp(-gate))
        silu = gate * sigma
        act[at, lanes] = (silu * up).astype(jnp.bfloat16)
        g_up[at, lanes] = (grad * silu).astype(jnp.bfloat16)
        g_gate[at, lanes] = (grad * up * sigma * (1.0 + gate * (1.0 - sigma))).astype(jnp.bfloat16)
        return carry

    lax.fori_loop(0, half // tile, one, 0)


def attn_block(pair, buf, ins, outs):
    rows = buf.shape[1]
    at = pl.ds(pl.multiple_of(pair * rows, rows), rows)
    outs[0][at, :] = nt(buf[pair], ins[0][...]).astype(jnp.bfloat16)


def no_block(pair, buf, ins, outs):
    pass


def nothing():
    pass


def after_out(total, ins, outs, extra):
    tokens, gain = ins
    hidden, normed = outs

    def one(r):
        value = tokens[r, :].astype(jnp.float32) + total[r, :]
        scale = lax.rsqrt(jnp.mean(value * value, axis=1, keepdims=True) + EPSILON)
        hidden[r, :] = value
        normed[r, :] = (value * scale * gain[...]).astype(jnp.bfloat16)

    return nothing, one, nothing


def norm_back(grad, value, gain, top):
    scale = lax.rsqrt(jnp.mean(value * value, axis=1, keepdims=True) + EPSILON)
    unit = value * scale
    g_unit = grad * gain
    inner = jnp.mean(g_unit * unit, axis=1, keepdims=True)
    return top + scale * (g_unit - unit * inner), grad * unit


def after_mlp(total, ins, outs, extra):
    hidden, cot, gain = ins
    g_hidden, g_branch, g_gain = outs

    def begin():
        g_gain[...] = jnp.zeros_like(g_gain)

    def one(r):
        grad, part = norm_back(
            total[r, :], hidden[r, :], gain[...], cot[r, :].astype(jnp.float32)
        )
        g_hidden[r, :] = grad
        g_branch[r, :] = grad.astype(jnp.bfloat16)
        g_gain[...] += part

    return begin, one, nothing


def after_qkv(total, ins, outs, extra):
    tokens, g_hidden, gain, g_gain_mlp, _ = ins
    rows_all, sums = extra[:2]
    place = lax.axis_index("tp")

    def begin():
        sums[4] = jnp.zeros(sums.shape[1:], jnp.float32)

    def one(r):
        grad, part = norm_back(
            total[r, :], tokens[r, :].astype(jnp.float32), gain[...], g_hidden[r, :]
        )
        rows_all[place, r, :] = grad.astype(jnp.bfloat16)
        sums[4] += part[0:8] + part[8:16]

    def end():
        sums[0] = jnp.concatenate(
            [
                jnp.sum(sums[4], axis=0, keepdims=True),
                jnp.sum(g_gain_mlp[...], axis=0, keepdims=True),
                jnp.zeros((6, total.shape[1]), jnp.float32),
            ],
            axis=0,
        )

    return begin, one, end


PLAN = {
    -1: [("z", 0, 1), ("z", 0, 2), ("z", 0, 3), ("x", 0, 0), ("x", 1, 0)],
    0: [("z", 1, 1), ("z", 1, 2), ("z", 1, 3), ("x", 0, 1)],
    1: [("x", 0, 2), ("x", 0, 3), ("x", 1, 1)],
    2: [("x", 1, 2), ("x", 1, 3)],
}
PLAN_OUT = {
    -1: [("z", 0, 1), ("z", 0, 2), ("z", 0, 3), ("x", 0, 0)],
    1: [("x", 0, 1)],
    2: [("x", 0, 2)],
    3: [("x", 0, 3)],
}


def shards(tokens, segments, w_qkv, w_out, w_gate_up, w_down, norm_attn, norm_mlp, cotangent):
    seqs, rows, width = tokens.shape
    size, tp_size = lax.axis_size("ctx"), lax.axis_size("tp")
    length = segments.shape[1]
    assert seqs == 1 and tp_size == 4
    part = rows // tp_size
    begin = lax.axis_index("tp") * part
    scale = 1.0 / math.sqrt(HD)
    low, full = jnp.bfloat16, jnp.float32
    heads = w_qkv.shape[2] // HD // size
    seg = segments[0]

    tokens_own = lax.dynamic_slice_in_dim(tokens[0], begin, part, 0)
    cot_own = lax.dynamic_slice_in_dim(cotangent[0], begin, part, 0)

    d = w_qkv.shape[1]
    gain_rows = jnp.concatenate(
        [norm_attn[None], norm_mlp[None], jnp.zeros((GAIN_ROWS - 2, d), low)], axis=0
    )
    sent_q = w_qkv.transpose(0, 2, 1).reshape(3, size, -1, d).transpose(1, 0, 2, 3)
    sent_q = jnp.concatenate(
        [sent_q.reshape(size, -1, d), jnp.broadcast_to(gain_rows, (size, GAIN_ROWS, d))], axis=1
    )
    sent_o = w_out.reshape(size, -1, d)
    sent_g = w_gate_up.transpose(0, 2, 1).reshape(2, size, -1, d).transpose(1, 0, 2, 3)
    sent_g = sent_g.reshape(size, -1, d)
    sent_d = w_down.reshape(size, -1, d)
    tokens_full, moved_q, moved_o = gather_call(
        tokens_own, [], [], no_block, 1, size, [sent_q, sent_o], PLAN
    )
    wq = join(sent_q, moved_q, True, GAIN_ROWS)
    wo = join(sent_o, moved_o, True)
    wg = join(sent_g, cross(sent_g), False)
    half = sent_d.shape[1]
    tall = 3 * heads * LANES
    gains = wq[tall : tall + 2].astype(full)
    gain_attn, gain_mlp = gains[0:1], gains[1:2]
    cot_gate, tokens_full = lax.optimization_barrier((cot_own, tokens_full))
    cot_full = wide_gather(cot_gate)

    positions = doc_positions(seg)
    cosine, sine = rope_tables(positions)
    starts = (jnp.arange(length, dtype=jnp.int32) - positions)[::BLK] // BLK
    marks = jnp.arange(length // BLK, dtype=jnp.int32)
    ends = jnp.sum((starts[None, :] <= marks[:, None]).astype(jnp.int32), axis=1) - 1

    qkv, normed1 = qkv_call(tokens_full, wq, gain_attn, cosine, sine, heads)
    attn, lse = attend_call(qkv, seg, starts, heads, scale)

    row_shape = jax.ShapeDtypeStruct((part, width), full)
    row_low = jax.ShapeDtypeStruct((part, width), low)
    gain_shape = jax.ShapeDtypeStruct((16, width), full)
    hidden1, normed2_own, moved_d = reduce_call(
        attn,
        wo,
        [tokens_own, gain_mlp],
        [row_shape, row_low],
        after_out,
        2,
        size,
        sent=[sent_d],
        plan=PLAN_OUT,
    )
    wd = join(sent_d, moved_d, False)
    half_shape = jax.ShapeDtypeStruct((length, half), low)
    normed2, act, g_gate, g_up = gather_call(
        normed2_own,
        [wg, wd, cot_full],
        [half_shape] * 3,
        functools.partial(mlp_block, half),
        3,
        size,
    )
    g_gu = jnp.concatenate([g_gate, g_up], axis=1)
    down_part = nn(act, wd).astype(low)
    down = lax.psum_scatter(down_part, GROUP, scatter_dimension=0, tiled=True)
    output = (hidden1 + down.astype(full)).astype(low)
    output = lax.all_gather(output, "tp", axis=0, tiled=True)[None]

    part_down, part_gu = tn(cot_full, act).astype(low), tn(normed2, g_gu).astype(low)
    g_gu, part_down, part_gu = lax.optimization_barrier((g_gu, part_down, part_gu))
    g_hidden1, g_branch_own, g_gain_mlp = reduce_call(
        g_gu, wg, [hidden1, cot_own, gain_mlp], [row_shape, row_low, gain_shape], after_mlp, 4, size
    )
    g_branch, g_attn = gather_call(
        g_branch_own,
        [wo],
        [jax.ShapeDtypeStruct((length, heads * LANES), low)],
        attn_block,
        5,
        size,
    )
    out_down = hand_out(part_down)
    out_gu = hand_out(part_gu)
    part_out = unspread(tn(g_branch, attn), 1).astype(low)
    g_attn, part_out = lax.optimization_barrier((g_attn, part_out))
    g_proj = attend_back_call(qkv, attn, g_attn, lse, seg, ends, cosine, sine, heads, scale)
    out_out = hand_out(part_out)
    part_qkv = unspread(tn(normed1, g_proj), 1).astype(low)
    g_proj, part_qkv = lax.optimization_barrier((g_proj, part_qkv))
    g_tokens, gain_sums, out_qkv = reduce_call(
        g_proj,
        wq,
        [tokens_own, g_hidden1, gain_attn, g_gain_mlp, part_qkv],
        [
            jax.ShapeDtypeStruct((tp_size, part, width), low),
            jax.ShapeDtypeStruct((8, width), full),
            jax.ShapeDtypeStruct((size, d, part_qkv.shape[1]), low),
        ],
        after_qkv,
        6,
        size,
        True,
    )
    g_tokens = g_tokens.reshape(1, rows, width)

    def natural(grad, count):
        wide = grad.astype(full).reshape(size, d, count, -1).transpose(2, 1, 0, 3)
        return wide.reshape(count, d, -1)

    grad_gu = natural(out_gu, 2)
    grad_out = out_out.astype(full).transpose(0, 2, 1).reshape(-1, d)
    grad_down = out_down.astype(full).transpose(0, 2, 1).reshape(-1, d)
    grad_qkv = natural(out_qkv, 3)

    mine = lax.axis_index("fsdp") * size + lax.axis_index("ctx")
    gain_grads = lax.dynamic_slice_in_dim(gain_sums, mine * d, d, 1)
    return (
        output,
        g_tokens,
        grad_qkv,
        grad_out,
        grad_gu,
        grad_down,
        gain_grads[0],
        gain_grads[1],
    )


def solution(mesh):
    in_specs = (
        P("fsdp", "ctx", None),
        P("fsdp", None),
        P(None, ("fsdp", "ctx"), "tp"),
        P("tp", ("fsdp", "ctx")),
        P(None, ("fsdp", "ctx"), "tp"),
        P("tp", ("fsdp", "ctx")),
        P(("fsdp", "ctx")),
        P(("fsdp", "ctx")),
        P("fsdp", "ctx", None),
    )
    out_specs = (
        P("fsdp", "ctx", None),
        P("fsdp", "ctx", None),
        P(None, ("fsdp", "ctx"), "tp"),
        P("tp", ("fsdp", "ctx")),
        P(None, ("fsdp", "ctx"), "tp"),
        P("tp", ("fsdp", "ctx")),
        P(("fsdp", "ctx")),
        P(("fsdp", "ctx")),
    )
    return jax.shard_map(shards, mesh=mesh, in_specs=in_specs, out_specs=out_specs, check_vma=False)
```

```python
import functools
import math

import jax
import jax.numpy as jnp
from jax import lax
from jax.experimental import pallas as pl
from jax.experimental.pallas import tpu as pltpu
from jax.sharding import PartitionSpec as P


HD = 96
HALF = HD // 2
LANES = 128
EPSILON = 1e-05
MASK_FILL = -1e30
ROPE_BASE = 10000.0
GROUP = ("ctx", "tp")
BLK = 256
GAIN_ROWS = 16
MESH = pl.DeviceIdType.MESH
SUBS = 2
PARTS = 4
VLIM = 64 * 1024 * 1024 - 65536


def cost(us):
    return pl.CostEstimate(flops=0, bytes_accessed=us * 3_000_000, transcendentals=0)


def near_order(c, j, size):
    low = c < size // 2
    base = jnp.where(low, c, size - 1 - c)
    zig = jnp.where(j % 2 == 1, base - (j + 1) // 2, base + j // 2)
    place = jnp.where(j <= 2 * base, zig, j)
    return jnp.where(low, place, size - 1 - place)


def places():
    c, t = lax.axis_index("ctx"), lax.axis_index("tp")
    return c, t // 2, t % 2


def greet(c, y, k, size):
    barrier = pltpu.get_barrier_semaphore()

    @pl.when(c < size - 1)
    def _():
        pl.semaphore_signal(barrier, inc=1, device_id={"ctx": c + 1}, device_id_type=MESH)

    @pl.when(c > 0)
    def _():
        pl.semaphore_signal(barrier, inc=1, device_id={"ctx": c - 1}, device_id_type=MESH)

    pl.semaphore_signal(barrier, inc=1, device_id={"tp": (1 - y) * 2 + k}, device_id_type=MESH)
    pl.semaphore_signal(barrier, inc=1, device_id={"tp": y * 2 + 1 - k}, device_id_type=MESH)
    pl.semaphore_wait(barrier, jnp.where((c > 0) & (c < size - 1), 4, 3))


def greet_all(c, y, k, size, groups):
    barrier = pltpu.get_barrier_semaphore()
    f = lax.axis_index("fsdp")

    def hello(dev):
        pl.semaphore_signal(barrier, inc=1, device_id=dev, device_id_type=MESH)

    for s in range(1, size):
        hello({"ctx": (c + s) % size})
    for g in range(1, groups):
        hello({"fsdp": (f + g) % groups})
    hello({"tp": (1 - y) * 2 + k})
    hello({"tp": y * 2 + 1 - k})
    pl.semaphore_wait(barrier, size + groups)


class Moves:
    def __init__(self, size, groups, sent, pieces, z_sems, x_sems):
        self.size, self.groups, self.sent, self.pieces = size, groups, sent, pieces
        self.z_sems, self.x_sems = z_sems, x_sems
        self.c, self.f = lax.axis_index("ctx"), lax.axis_index("fsdp")

    def z(self, w, s):
        to = (self.c + s) % self.size
        return pltpu.make_async_remote_copy(
            src_ref=self.sent[w].at[to],
            dst_ref=self.pieces[w].at[self.f * self.size + self.c],
            send_sem=self.z_sems.at[w, s - 1, 0],
            recv_sem=self.z_sems.at[w, s - 1, 1],
            device_id={"ctx": to},
            device_id_type=MESH,
        )

    def x(self, w, g, s):
        slot = self.pieces[w].at[self.f * self.size + (self.c + self.size - s) % self.size]
        return pltpu.make_async_remote_copy(
            src_ref=slot if s else self.sent[w].at[self.c],
            dst_ref=slot,
            send_sem=self.x_sems.at[w, g - 1, s, 0],
            recv_sem=self.x_sems.at[w, g - 1, s, 1],
            device_id={"fsdp": (self.f + g) % self.groups},
            device_id_type=MESH,
        )

    def start_z(self, w, s):
        self.z(w, s).start()

    def start_x(self, w, s):
        if s:
            self.z(w, s).wait_recv()
        for g in range(1, self.groups):
            self.x(w, g, s).start()

    def finish(self):
        for w in range(len(self.sent)):
            for s in range(self.size):
                if s:
                    self.z(w, s).wait_send()
                for g in range(1, self.groups):
                    self.x(w, g, s).wait()


class HandOut:
    def __init__(self, size, groups, part, out, got, mine, ready, x_sems, z_sems, l_sems):
        self.size, self.groups, self.part, self.out = size, groups, part, out
        self.got, self.mine, self.ready = got, mine, ready
        self.x_sems, self.z_sems, self.l_sems = x_sems, z_sems, l_sems
        self.c, self.f = lax.axis_index("ctx"), lax.axis_index("fsdp")
        self.d = mine.shape[1]

    def rows(self, f, c):
        return self.part.at[pl.ds(pl.multiple_of((f * self.size + c) * self.d, self.d), self.d)]

    def x(self, g, cc):
        to = (self.f + g) % self.groups
        return pltpu.make_async_remote_copy(
            src_ref=self.rows(to, cc),
            dst_ref=self.got.at[g - 1, cc],
            send_sem=self.x_sems.at[g - 1, cc, 0],
            recv_sem=self.x_sems.at[g - 1, cc, 1],
            device_id={"fsdp": to},
            device_id_type=MESH,
        )

    def load(self, cc):
        return pltpu.make_async_copy(self.rows(self.f, cc), self.mine.at[cc], self.l_sems.at[cc])

    def z(self, cc, source):
        return pltpu.make_async_remote_copy(
            src_ref=self.ready.at[cc],
            dst_ref=self.out.at[self.c],
            send_sem=self.z_sems.at[cc, 0],
            recv_sem=self.z_sems.at[source, 1],
            device_id={"ctx": cc},
            device_id_type=MESH,
        )

    def keep(self):
        return pltpu.make_async_copy(
            self.ready.at[self.c], self.out.at[self.c], self.l_sems.at[self.size]
        )

    def each(self, body):
        def one(i, carry):
            body(i)
            return carry

        lax.fori_loop(0, self.size, one, 0)

    def start(self, cc):
        for g in range(1, self.groups):
            self.x(g, cc).start()
        self.load(cc).start()

    def step(self, cc):
        self.load(cc).wait()
        for g in range(1, self.groups):
            self.x(g, cc).wait_recv()

        def add(i, carry):
            r = pl.ds(pl.multiple_of(i * 16, 16), 16)
            value = self.mine[cc, r, :].astype(jnp.float32)
            for g in range(1, self.groups):
                value = value + self.got[g - 1, cc, r, :].astype(jnp.float32)
            self.ready[cc, r, :] = value.astype(jnp.bfloat16)
            return carry

        lax.fori_loop(0, self.d // 16, add, 0)

        @pl.when(cc != self.c)
        def _():
            self.z(cc, self.c).start()

        @pl.when(cc == self.c)
        def _():
            self.keep().start()

    def finish(self):
        def one(cc):
            for g in range(1, self.groups):
                self.x(g, cc).wait_send()

            @pl.when(cc != self.c)
            def _():
                self.z(cc, self.c).wait_send()
                self.z(cc, cc).wait_recv()

        self.each(one)
        self.keep().wait()


def gather_kernel(size, groups, plan, n_move, part, n_in, n_out, compute, *refs):
    x_ref = refs[0]
    hbm_ins = refs[1 : 1 + n_in]
    sent = refs[1 + n_in : 1 + n_in + n_move]
    refs = refs[1 + n_in + n_move :]
    full_ref = refs[0]
    outs = refs[1 : 1 + n_out]
    moved = refs[1 + n_out : 1 + n_out + n_move]
    refs = refs[1 + n_out + n_move :]
    ins = refs[:n_in]
    buf, recv, zs, ys, ks, local, load, in_sems, *move_sems = refs[n_in:]
    moves = Moves(size, groups, sent, moved, *move_sems) if n_move else None
    c, y, k = places()
    sub = part // SUBS

    def slot(cc, yy, kk, s):
        return buf.at[cc * 2 + yy, pl.ds(pl.multiple_of(kk * part + s * sub, sub), sub)]

    def copy(cc, yy, kk, s, sem, dev):
        return pltpu.make_async_remote_copy(
            src_ref=slot(cc, yy, kk, s),
            dst_ref=slot(cc, yy, kk, s),
            send_sem=sem,
            recv_sem=recv.at[cc * 2 + yy, kk, s],
            device_id=dev,
            device_id_type=MESH,
        )

    up, down = {"ctx": c + 1}, {"ctx": c - 1}
    ydev, kdev = {"tp": (1 - y) * 2 + k}, {"tp": y * 2 + 1 - k}

    def z_up(cc, s):
        return copy(cc, y, k, s, zs.at[0, cc, s], up)

    def z_down(cc, s):
        return copy(cc, y, k, s, zs.at[1, cc, s], down)

    def y_send(cc, s):
        return copy(cc, y, k, s, ys.at[cc, s], ydev)

    def k_send(cc, yy, s):
        return copy(cc, yy, k, s, ks.at[cc * 2 + yy, s], kdev)

    def pair_out(cc, yy):
        pair = cc * 2 + yy
        return pltpu.make_async_copy(
            buf.at[pair],
            full_ref.at[pl.ds(pl.multiple_of(pair * 2 * part, 2 * part), 2 * part)],
            local.at[pair],
        )

    def got(cc, yy, kk, s):
        copy(cc, yy, kk, s, ys.at[0, 0], ydev).wait_recv()

    mine = buf.at[c * 2 + y, pl.ds(pl.multiple_of(k * part, part), part)]
    first = pltpu.make_async_copy(x_ref, mine, load)
    first.start()
    for i in range(n_in):
        pltpu.make_async_copy(hbm_ins[i], ins[i], in_sems.at[i]).start()
    if moves:
        greet_all(c, y, k, size, groups)
    else:
        greet(c, y, k, size)
    first.wait()

    def z_stage(cc, s):
        @pl.when((cc <= c) & (c < size - 1))
        def _():
            z_up(cc, s).start()

        @pl.when((cc >= c) & (c > 0))
        def _():
            z_down(cc, s).start()

        y_send(cc, s).start()
        k_send(cc, y, s).start()

    for s in range(SUBS):
        z_stage(c, s)

    def move_on(step):
        for kind, w, s in plan.get(step, ()):
            (moves.start_z if kind == "z" else moves.start_x)(w, s)

    move_on(-1)
    for i in range(n_in):
        pltpu.make_async_copy(hbm_ins[i], ins[i], in_sems.at[i]).wait()

    def finish(cc, yy):
        for s in range(SUBS):
            got(cc, yy, 1 - k, s)
        pair_out(cc, yy).start()
        compute(cc * 2 + yy, buf, ins, outs)

    def step(r, carry):
        for s in range(SUBS):
            for sign in (-1, 1):
                nxt = c + sign * (r + 1)

                @pl.when((nxt >= 0) & (nxt < size))
                def _():
                    got(nxt, y, k, s)
                    z_stage(nxt, s)

            for sign in (-1, 1):
                cc = c + sign * r

                @pl.when((cc >= 0) & (cc < size) & ((r > 0) | (sign > 0)))
                def _():
                    if s == SUBS - 1:
                        finish(cc, y)
                    got(cc, 1 - y, k, s)
                    k_send(cc, 1 - y, s).start()
                    if s == SUBS - 1:
                        finish(cc, 1 - y)

        for at in sorted(plan):
            if at >= 0:

                @pl.when(r == at)
                def _():
                    move_on(at)

        return carry

    lax.fori_loop(0, size, step, 0)

    def drain(cc, carry):
        for s in range(SUBS):
            @pl.when((cc <= c) & (c < size - 1))
            def _():
                z_up(cc, s).wait_send()

            @pl.when((cc >= c) & (c > 0))
            def _():
                z_down(cc, s).wait_send()

            y_send(cc, s).wait_send()
            for yy in range(2):
                k_send(cc, yy, s).wait_send()
        for yy in range(2):
            pair_out(cc, yy).wait()
        return carry

    lax.fori_loop(0, size, drain, 0)
    if moves:
        moves.finish()


def gather_call(x, ins, out_shapes, compute, cid, size, sent=(), plan=None):
    part, width = x.shape
    groups = lax.axis_size("fsdp")
    dma = pltpu.SemaphoreType.DMA
    any_spec = pl.BlockSpec(memory_space=pl.ANY)
    vmem = pl.BlockSpec(memory_space=pltpu.VMEM)
    full = jax.ShapeDtypeStruct((size * 4 * part, width), x.dtype)
    return pl.pallas_call(
        functools.partial(
            gather_kernel,
            size,
            groups,
            plan or {},
            len(sent),
            part,
            len(ins),
            len(out_shapes),
            compute,
        ),
        out_shape=(
            full,
            *out_shapes,
            *(
                jax.ShapeDtypeStruct((groups * size, *one.shape[1:]), one.dtype)
                for one in sent
            ),
        ),
        in_specs=[any_spec] * (1 + len(ins) + len(sent)),
        out_specs=(any_spec, *([vmem] * len(out_shapes)), *([any_spec] * len(sent))),
        scratch_shapes=[
            *(pltpu.VMEM(one.shape, one.dtype) for one in ins),
            pltpu.VMEM((size * 2, 2 * part, width), x.dtype),
            pltpu.SemaphoreType.DMA((size * 2, 2, SUBS)),
            pltpu.SemaphoreType.DMA((2, size, SUBS)),
            pltpu.SemaphoreType.DMA((size, SUBS)),
            pltpu.SemaphoreType.DMA((size * 2, SUBS)),
            pltpu.SemaphoreType.DMA((size * 2,)),
            pltpu.SemaphoreType.DMA,
            pltpu.SemaphoreType.DMA((max(len(ins), 1),)),
            *(
                [dma((len(sent), size - 1, 2)), dma((len(sent), max(groups - 1, 1), size, 2))]
                if sent
                else []
            ),
        ],
        compiler_params=pltpu.CompilerParams(
            collective_id=cid, has_side_effects=True, vmem_limit_bytes=VLIM
        ),
        cost_estimate=cost(75),
    )(x, *ins, *sent)


def reduce_kernel(size, groups, last, plan, n_move, part, n_in, n_out, final, *refs):
    a_ref, w_ref = refs[:2]
    ins = refs[2 : 2 + n_in]
    sent = refs[2 + n_in : 2 + n_in + n_move]
    refs = refs[n_move:]
    outs = refs[2 + n_in : 2 + n_in + n_out]
    moved = refs[2 + n_in + n_out : 2 + n_in + n_out + n_move]
    refs = refs[n_move:]
    (
        own,
        ksend,
        krecv,
        ysend,
        yrecv,
        qown,
        zsend,
        zrecv,
        total,
        prod,
        k_sems,
        y_sems,
        z_sems,
        *extra,
    ) = refs[2 + n_in + n_out :]
    moves = Moves(size, groups, sent, moved, *extra) if n_move else None
    hand = HandOut(size, groups, ins[-1], outs[2], *extra[9:]) if last else None
    c, y, k = places()
    depth = a_ref.shape[1]
    chunk = 16
    tile = 512
    width = total.shape[1]

    sub = part // PARTS

    def remote(src, dst, sems, dev):
        return pltpu.make_async_remote_copy(
            src_ref=src,
            dst_ref=dst,
            send_sem=sems.at[0],
            recv_sem=sems.at[1],
            device_id=dev,
            device_id_type=MESH,
        )

    ydev, kdev = {"tp": (1 - y) * 2 + k}, {"tp": y * 2 + 1 - k}

    def k_copy(cc, yy):
        pair = cc * 2 + yy
        return remote(ksend.at[pair], krecv.at[pair], k_sems.at[pair], kdev)

    def y_copy(cc, s):
        r = pl.ds(s * sub, sub)
        return remote(ysend.at[cc, r], yrecv.at[cc, r], y_sems.at[cc, s], ydev)

    def z_up(cc, s):
        r = pl.ds(s * sub, sub)
        return remote(zsend.at[cc, r], zrecv.at[0, cc, r], z_sems.at[0, cc, s], {"ctx": c + 1})

    def z_down(cc, s):
        r = pl.ds(s * sub, sub)
        return remote(zsend.at[cc, r], zrecv.at[1, cc, r], z_sems.at[1, cc, s], {"ctx": c - 1})

    if last or moves:
        greet_all(c, y, k, size, groups)
    else:
        greet(c, y, k, size)

    def move_on(step):
        for kind, w, s in plan.get(step, ()):
            (moves.start_z if kind == "z" else moves.start_x)(w, s)

    move_on(-1)

    def rows(i):
        return pl.ds(pl.multiple_of(i * chunk, chunk), chunk)

    def sweep(body, s=None):
        steps = part // chunk
        lo, hi = (0, steps) if s is None else (s * steps // PARTS, (s + 1) * steps // PARTS)

        def one(i, carry):
            body(rows(i))
            return carry

        lax.fori_loop(lo, hi, one, 0)

    def produce(cc, yy, keep):
        pair = cc * 2 + yy
        both = pl.ds(pl.multiple_of(pair * 2 * part, 2 * part), 2 * part)
        mine = pl.ds(pl.multiple_of(k * part, part), part)
        other = pl.ds(pl.multiple_of((1 - k) * part, part), part)

        def one(i, carry):
            lanes = pl.ds(pl.multiple_of(i * tile, tile), tile)
            prod[...] = jnp.dot(
                a_ref[both, :], w_ref[0:depth, lanes], preferred_element_type=jnp.float32
            )
            ksend[pair, :, lanes] = prod[other, :].astype(jnp.bfloat16)
            own[keep, :, lanes] = prod[mine, :]
            return carry

        lax.fori_loop(0, width // tile, one, 0)
        k_copy(cc, yy).start()

    def first(j):
        cc = near_order(c, size - 1 - j, size)
        if last:
            hand.start(cc)
        produce(cc, 1 - y, 0)
        k_copy(cc, 1 - y).wait_recv()

        def add_y(r):
            got = krecv[cc * 2 + 1 - y, r, :].astype(jnp.float32)
            ysend[cc, r, :] = (own[0, r, :] + got).astype(jnp.bfloat16)

        for s in range(PARTS):
            sweep(add_y, s)
            y_copy(cc, s).start()
        produce(cc, y, 1)
        k_copy(cc, y).wait_recv()

        def add_k(r):
            qown[cc, r, :] = own[1, r, :] + krecv[cc * 2 + y, r, :].astype(jnp.float32)

        sweep(add_k)

    def pass_on(cc, s, into, edge, send):
        @pl.when(jnp.logical_not(edge))
        def _():
            send(cc, s).wait_recv()

            def add(r):
                part_sum = qown[cc, r, :] + yrecv[cc, r, :].astype(jnp.float32)
                zsend[cc, r, :] = (part_sum + zrecv[into, cc, r, :].astype(jnp.float32)).astype(
                    jnp.bfloat16
                )

            sweep(add, s)

        @pl.when(edge)
        def _():
            def add(r):
                part_sum = qown[cc, r, :] + yrecv[cc, r, :].astype(jnp.float32)
                zsend[cc, r, :] = part_sum.astype(jnp.bfloat16)

            sweep(add, s)

        send(cc, s).start()

    def second(j):
        cc = near_order(c, size - 1 - j, size)
        for s in range(PARTS):

            @pl.when(cc > c)
            def _():
                y_copy(cc, s).wait_recv()
                pass_on(cc, s, 0, c == 0, z_up)

            @pl.when(cc < c)
            def _():
                y_copy(cc, s).wait_recv()
                pass_on(cc, s, 1, c == size - 1, z_down)

        if last:
            hand.step(cc)

        for at in sorted(plan):
            if at >= 0:

                @pl.when(j == at)
                def _():
                    move_on(at)

    lag = jnp.where((c == 0) | (c == size - 1), 1, 2)

    def both(i, carry):
        @pl.when(i < size)
        def _():
            first(i)

        @pl.when((i >= lag) & (i - lag < size))
        def _():
            second(i - lag)

        return carry

    lax.fori_loop(0, size + 2, both, 0)

    def sum_up(r):
        own_sum = qown[c, r, :] + yrecv[c, r, :].astype(jnp.float32)

        @pl.when(c == 0)
        def _():
            total[r, :] = own_sum + zrecv[1, c, r, :].astype(jnp.float32)

        @pl.when(c == size - 1)
        def _():
            total[r, :] = own_sum + zrecv[0, c, r, :].astype(jnp.float32)

        @pl.when((c > 0) & (c < size - 1))
        def _():
            below = own_sum + zrecv[0, c, r, :].astype(jnp.float32)
            total[r, :] = below + zrecv[1, c, r, :].astype(jnp.float32)

    begin, one_chunk, end = final(total, ins, outs, extra)
    begin()
    for s in range(PARTS):
        y_copy(c, s).wait_recv()

        @pl.when(c > 0)
        def _():
            z_up(c, s).wait_recv()

        @pl.when(c < size - 1)
        def _():
            z_down(c, s).wait_recv()

        def close(r):
            sum_up(r)
            one_chunk(r)

        sweep(close, s)
    end()
    if last:
        spread_out(size, groups, c, y, k, ydev, kdev, outs, extra)

    def drain(cc, carry):
        for yy in range(2):
            k_copy(cc, yy).wait_send()
        for s in range(PARTS):
            y_copy(cc, s).wait_send()

            @pl.when(cc > c)
            def _():
                z_up(cc, s).wait_send()

            @pl.when(cc < c)
            def _():
                z_down(cc, s).wait_send()

        return carry

    lax.fori_loop(0, size, drain, 0)
    if moves:
        moves.finish()
    if last:
        hand.finish()


def spread_out(size, groups, c, y, k, ydev, kdev, outs, extra):
    rows_all, sums, got, row_sems, k_sem, y_sem, f_sems, z_sems, out_sem = extra[:9]
    f = lax.axis_index("fsdp")

    def copy(src, dst, sems, dev):
        return pltpu.make_async_remote_copy(
            src_ref=src,
            dst_ref=dst,
            send_sem=sems.at[0],
            recv_sem=sems.at[1],
            device_id=dev,
            device_id_type=MESH,
        )

    def row_copy(yy, kk, n, dev):
        slot = rows_all.at[yy * 2 + kk]
        return copy(slot, slot, row_sems.at[n], dev)

    to_y, to_k, on_k = row_copy(y, k, 0, ydev), row_copy(y, k, 1, kdev), row_copy(1 - y, k, 2, kdev)
    to_y.start()
    to_k.start()

    def add(n, first, count):
        value = sums[n]
        for i in range(first, first + count):
            value = value + got[i]
        sums[n + 1] = value

    swap_k = copy(sums.at[0], got.at[0], k_sem, kdev)
    swap_k.start()
    swap_k.wait()
    add(0, 0, 1)
    swap_y = copy(sums.at[1], got.at[1], y_sem, ydev)
    swap_y.start()
    swap_y.wait()
    add(1, 1, 1)
    swaps = [
        copy(sums.at[2], got.at[1 + g], f_sems.at[g - 1], {"fsdp": (f + g) % groups})
        for g in range(1, groups)
    ]
    for one in swaps:
        one.start()
    for one in swaps:
        one.wait()
    add(2, 2, groups - 1)
    swaps = [
        copy(sums.at[3], got.at[groups + s], z_sems.at[s - 1], {"ctx": (c + s) % size})
        for s in range(1, size)
    ]
    for one in swaps:
        one.start()
    row_copy(1 - y, k, 0, ydev).wait_recv()
    on_k.start()
    for one in swaps:
        one.wait()
    add(3, groups + 1, size - 1)
    outs[1][...] = sums[4]
    row_copy(y, 1 - k, 1, kdev).wait_recv()
    row_copy(1 - y, 1 - k, 2, kdev).wait_recv()
    to_y.wait_send()
    to_k.wait_send()
    on_k.wait_send()
    out = pltpu.make_async_copy(rows_all, outs[0], out_sem)
    out.start()
    out.wait()


def reduce_call(a, w, ins, out_shapes, final, cid, size, last=False, sent=(), plan=None):
    width = w.shape[1]
    part = a.shape[0] // (size * 4)
    vmem = pl.BlockSpec(memory_space=pltpu.VMEM)
    low, full = jnp.bfloat16, jnp.float32
    groups = lax.axis_size("fsdp")
    any_spec = pl.BlockSpec(memory_space=pl.ANY)
    dma = pltpu.SemaphoreType.DMA
    out_specs, extra = [vmem] * len(out_shapes), []
    if sent:
        extra = [dma((len(sent), size - 1, 2)), dma((len(sent), max(groups - 1, 1), size, 2))]
    if last:
        out_specs[0] = out_specs[2] = any_spec
        extra = [
            pltpu.VMEM((4, part, width), low),
            pltpu.VMEM((5, 8, width), full),
            pltpu.VMEM((groups + size, 8, width), full),
            dma((3, 2)),
            dma((2,)),
            dma((2,)),
            dma((max(groups - 1, 1), 2)),
            dma((size - 1, 2)),
            dma,
            pltpu.VMEM((max(groups - 1, 1), *out_shapes[2].shape), low),
            pltpu.VMEM(out_shapes[2].shape, low),
            pltpu.VMEM(out_shapes[2].shape, low),
            dma((max(groups - 1, 1), size, 2)),
            dma((size, 2)),
            dma((size + 1,)),
        ]
    return pl.pallas_call(
        functools.partial(
            reduce_kernel,
            size,
            groups,
            last,
            plan or {},
            len(sent),
            part,
            len(ins),
            len(out_shapes),
            final,
        ),
        out_shape=(
            *out_shapes,
            *(
                jax.ShapeDtypeStruct((groups * size, *one.shape[1:]), one.dtype)
                for one in sent
            ),
        ),
        in_specs=[vmem] * (1 + len(ins))
        + [any_spec if last else vmem]
        + [any_spec] * len(sent),
        out_specs=(*out_specs, *([any_spec] * len(sent))),
        scratch_shapes=[
            pltpu.VMEM((2, part, width), full),
            pltpu.VMEM((size * 2, part, width), low),
            pltpu.VMEM((size * 2, part, width), low),
            pltpu.VMEM((size, part, width), low),
            pltpu.VMEM((size, part, width), low),
            pltpu.VMEM((size, part, width), full),
            pltpu.VMEM((size, part, width), low),
            pltpu.VMEM((2, size, part, width), low),
            pltpu.VMEM((part, width), full),
            pltpu.VMEM((2 * part, 512), full),
            pltpu.SemaphoreType.DMA((size * 2, 2)),
            pltpu.SemaphoreType.DMA((size, PARTS, 2)),
            pltpu.SemaphoreType.DMA((2, size, PARTS, 2)),
            *extra,
        ],
        compiler_params=pltpu.CompilerParams(
            collective_id=cid, has_side_effects=True, vmem_limit_bytes=VLIM
        ),
        cost_estimate=cost(85),
    )(a, w, *ins, *sent)


def doc_positions(segment_row):
    places_in = jnp.arange(segment_row.shape[0], dtype=jnp.int32)
    starts = jnp.concatenate([jnp.ones((1,), dtype=jnp.bool_), segment_row[1:] != segment_row[:-1]])
    first = lax.cummax(jnp.where(starts, places_in, jnp.zeros_like(places_in)), axis=0)
    return places_in - first


def rope_tables(positions):
    freqs = ROPE_BASE ** (-(jnp.arange(HALF, dtype=jnp.float32) * 2.0 / HD))
    angles = positions.astype(jnp.float32)[:, None] * freqs
    gap = jnp.zeros((positions.shape[0], LANES // 2 - HALF), jnp.float32)
    cosine, sine = jnp.cos(angles), jnp.sin(angles)
    return (
        jnp.concatenate([cosine, gap, cosine, gap], axis=1),
        jnp.concatenate([-sine, gap, sine, gap], axis=1),
    )


def spread(array, axis):
    shape = array.shape
    halves = array.reshape(*shape[:axis], shape[axis] // HALF, HALF, *shape[axis + 1 :])
    pads = [(0, 0)] * halves.ndim
    pads[axis + 1] = (0, LANES // 2 - HALF)
    wide = jnp.pad(halves, pads)
    return wide.reshape(*shape[:axis], -1, *shape[axis + 1 :])


def unspread(array, axis):
    shape = array.shape
    half = LANES // 2
    halves = array.reshape(*shape[:axis], shape[axis] // half, half, *shape[axis + 1 :])
    kept = lax.slice_in_dim(halves, 0, HALF, axis=axis + 1)
    return kept.reshape(*shape[:axis], -1, *shape[axis + 1 :])


def nt(left, right):
    return lax.dot_general(left, right, (((1,), (1,)), ((), ())), preferred_element_type=jnp.float32)


def nn(left, right):
    return jnp.dot(left, right, preferred_element_type=jnp.float32)


def tn(left, right):
    return lax.dot_general(left, right, (((0,), (0,)), ((), ())), preferred_element_type=jnp.float32)


def qkv_kernel(heads, x_ref, w_ref, gain_ref, cos_ref, sin_ref, out_ref, normed_ref):
    for i in range(BLK // 16):
        at = slice(i * 16, (i + 1) * 16)
        x = x_ref[at, :].astype(jnp.float32)
        scale = lax.rsqrt(jnp.mean(x * x, axis=1, keepdims=True) + EPSILON)
        normed_ref[at, :] = (x * scale * gain_ref[...]).astype(jnp.bfloat16)
    proj = nt(normed_ref[...], w_ref[...])
    for i in range(3 * heads):
        cut = slice(i * LANES, (i + 1) * LANES)
        one = proj[:, cut]
        if i < 2 * heads:
            one = one * cos_ref[...] + pltpu.roll(one, LANES // 2, 1) * sin_ref[...]
        out_ref[:, cut] = one.astype(jnp.bfloat16)


def qkv_call(x, w, gain, cosine, sine, heads):
    rows, width = x.shape
    tall = 3 * heads * LANES
    return pl.pallas_call(
        functools.partial(qkv_kernel, heads),
        out_shape=(
            jax.ShapeDtypeStruct((rows, tall), jnp.bfloat16),
            jax.ShapeDtypeStruct((rows, width), jnp.bfloat16),
        ),
        grid=(rows // BLK,),
        in_specs=[
            pl.BlockSpec((BLK, width), lambda i: (i, 0)),
            pl.BlockSpec((tall, width), lambda i: (0, 0)),
            pl.BlockSpec((1, width), lambda i: (0, 0)),
            pl.BlockSpec((BLK, LANES), lambda i: (i, 0)),
            pl.BlockSpec((BLK, LANES), lambda i: (i, 0)),
        ],
        out_specs=(
            pl.BlockSpec((BLK, tall), lambda i: (i, 0)),
            pl.BlockSpec((BLK, width), lambda i: (i, 0)),
        ),
        compiler_params=pltpu.CompilerParams(vmem_limit_bytes=VLIM),
        cost_estimate=cost(18),
        name="qkv",
    )(x, w, gain, cosine, sine)


def block(ref, i, head):
    return ref[pl.ds(pl.multiple_of(i * BLK, BLK), BLK), head * LANES : (head + 1) * LANES]


def masked_scores(keys, query, seg_col, seg_row, kb, qb, scale):
    scores = nt(keys, query) * scale
    key_pos = kb * BLK + lax.broadcasted_iota(jnp.int32, scores.shape, 0)
    query_pos = qb * BLK + lax.broadcasted_iota(jnp.int32, scores.shape, 1)
    return jnp.where((key_pos <= query_pos) & (seg_col == seg_row), scores, MASK_FILL)


def attend_kernel(heads, scale, low_ref, qkv_ref, col_ref, row_ref, out_ref, lse_ref):
    blocks = qkv_ref.shape[0] // BLK

    def one(i, carry):
        cut = pl.ds(pl.multiple_of(i * BLK, BLK), BLK)
        seg_row = row_ref[:, cut]
        for h in range(heads):
            query = block(qkv_ref, i, h)

            def inner(kb, state):
                peak, total, acc = state
                keys = block(qkv_ref, kb, heads + h)
                seg_col = col_ref[pl.ds(pl.multiple_of(kb * BLK, BLK), BLK), :]
                scores = masked_scores(keys, query, seg_col, seg_row, kb, i, scale)
                new = jnp.maximum(peak, jnp.max(scores, axis=0, keepdims=True))
                fade = jnp.exp(peak - new)
                expo = jnp.exp(scores - new)
                total = total * fade + jnp.sum(expo, axis=0, keepdims=True)
                mixed = tn(block(qkv_ref, kb, 2 * heads + h), expo.astype(jnp.bfloat16))
                return new, total, acc * fade + mixed

            peak, total, acc = lax.fori_loop(
                low_ref[i],
                i + 1,
                inner,
                (
                    jnp.full((1, BLK), MASK_FILL, jnp.float32),
                    jnp.zeros((1, BLK), jnp.float32),
                    jnp.zeros((LANES, BLK), jnp.float32),
                ),
            )
            out_ref[cut, h * LANES : (h + 1) * LANES] = (acc / total).T.astype(jnp.bfloat16)
            lse_ref[h : h + 1, cut] = peak + jnp.log(total)
        return carry

    lax.fori_loop(0, blocks, one, 0)


def attend_call(qkv, seg, low, heads, scale):
    rows = qkv.shape[0]
    vmem = pl.BlockSpec(memory_space=pltpu.VMEM)
    return pl.pallas_call(
        functools.partial(attend_kernel, heads, scale),
        out_shape=(
            jax.ShapeDtypeStruct((rows, heads * LANES), jnp.bfloat16),
            jax.ShapeDtypeStruct((heads, rows), jnp.float32),
        ),
        in_specs=[pl.BlockSpec(memory_space=pltpu.SMEM), vmem, vmem, vmem],
        out_specs=(vmem, vmem),
        compiler_params=pltpu.CompilerParams(vmem_limit_bytes=VLIM),
        cost_estimate=cost(20),
        name="attend",
    )(low, qkv, seg[:, None], seg[None, :])


def attend_back_kernel(
    heads,
    scale,
    high_ref,
    qkv_ref,
    out_ref,
    grad_ref,
    lse_ref,
    col_ref,
    row_ref,
    cos_ref,
    sin_ref,
    res_ref,
    delta_ref,
    gq_ref,
):
    blocks = qkv_ref.shape[0] // BLK
    gq_ref[...] = jnp.zeros_like(gq_ref)

    def dots(i, carry):
        cut = pl.ds(pl.multiple_of(i * BLK, BLK), BLK)
        for h in range(heads):
            prod = block(out_ref, i, h).astype(jnp.float32) * block(grad_ref, i, h).astype(
                jnp.float32
            )
            delta_ref[h : h + 1, cut] = jnp.sum(prod.T, axis=0, keepdims=True)
        return carry

    lax.fori_loop(0, blocks, dots, 0)

    def turn_back(value, cut):
        low = value.astype(jnp.bfloat16).astype(jnp.float32)
        turned = low * cos_ref[cut, :] - pltpu.roll(low, LANES // 2, 1) * sin_ref[cut, :]
        return turned.astype(jnp.bfloat16)

    def one(kb, carry):
        cut = pl.ds(pl.multiple_of(kb * BLK, BLK), BLK)
        seg_col = col_ref[cut, :]
        for h in range(heads):
            keys = block(qkv_ref, kb, heads + h)
            values = block(qkv_ref, kb, 2 * heads + h)

            def inner(i, state):
                gk, gv = state
                at = pl.ds(pl.multiple_of(i * BLK, BLK), BLK)
                query = block(qkv_ref, i, h)
                grad = block(grad_ref, i, h)
                scores = masked_scores(keys, query, seg_col, row_ref[:, at], kb, i, scale)
                probs = jnp.exp(scores - lse_ref[h : h + 1, at])
                gv = gv + nn(probs.astype(jnp.bfloat16), grad)
                g_probs = nt(values, grad)
                g_scores = (probs * (g_probs - delta_ref[h : h + 1, at])).astype(jnp.bfloat16)
                gk = gk + nn(g_scores, query)
                lanes = slice(h * LANES, (h + 1) * LANES)
                gq_ref[at, lanes] += tn(g_scores, keys)
                return gk, gv

            zero = jnp.zeros((BLK, LANES), jnp.float32)
            gk, gv = lax.fori_loop(kb, high_ref[kb] + 1, inner, (zero, zero))
            at_k = slice((heads + h) * LANES, (heads + h + 1) * LANES)
            at_v = slice((2 * heads + h) * LANES, (2 * heads + h + 1) * LANES)
            res_ref[cut, at_k] = turn_back(gk * scale, cut)
            res_ref[cut, at_v] = gv.astype(jnp.bfloat16)
        return carry

    lax.fori_loop(0, blocks, one, 0)

    def close(i, carry):
        cut = pl.ds(pl.multiple_of(i * BLK, BLK), BLK)
        for h in range(heads):
            lanes = slice(h * LANES, (h + 1) * LANES)
            res_ref[cut, lanes] = turn_back(gq_ref[cut, lanes] * scale, cut)
        return carry

    lax.fori_loop(0, blocks, close, 0)


def attend_back_call(qkv, out, grad, lse, seg, high, cosine, sine, heads, scale):
    rows = qkv.shape[0]
    vmem = pl.BlockSpec(memory_space=pltpu.VMEM)
    return pl.pallas_call(
        functools.partial(attend_back_kernel, heads, scale),
        out_shape=jax.ShapeDtypeStruct(qkv.shape, jnp.bfloat16),
        in_specs=[pl.BlockSpec(memory_space=pltpu.SMEM)] + [vmem] * 8,
        out_specs=vmem,
        scratch_shapes=[
            pltpu.VMEM((heads, rows), jnp.float32),
            pltpu.VMEM((rows, heads * LANES), jnp.float32),
        ],
        compiler_params=pltpu.CompilerParams(vmem_limit_bytes=VLIM),
        cost_estimate=cost(32),
        name="attend_back",
    )(high, qkv, out, grad, lse, seg[:, None], seg[None, :], cosine, sine)


def join_kernel(cuts, groups, size, d, *refs):
    *pieces, out, sems = refs
    c, f = lax.axis_index("ctx"), lax.axis_index("fsdp")

    def copies(go):
        for i in range(groups * size):
            g, s = i // size, i % size
            place = ((f + groups - g) % groups) * size + (c + size - s) % size
            lanes = pl.ds(pl.multiple_of(place * d, d), d)
            for q, (src, dst, rows) in enumerate(cuts):
                if len(pieces) > 2:
                    piece = pieces[i]
                else:
                    piece = pieces[1].at[place] if i else pieces[0].at[c]
                go(
                    pltpu.make_async_copy(
                        piece.at[pl.ds(src, rows)], out.at[pl.ds(dst, rows), lanes], sems.at[i, q]
                    )
                )

    copies(lambda one: one.start())
    for q, (_, dst, rows) in enumerate(cuts):
        stop = cuts[q + 1][1] if q + 1 < len(cuts) else out.shape[0]
        if dst + rows < stop:
            gap = stop - dst - rows
            out[pl.ds(dst + rows, gap), :] = jnp.zeros((gap, out.shape[1]), out.dtype)
    copies(lambda one: one.wait())


def join(sent, pieces, spaced, tail=0):
    size, groups = lax.axis_size("ctx"), lax.axis_size("fsdp")
    c, f = lax.axis_index("ctx"), lax.axis_index("fsdp")
    count, (n, d) = size * groups, sent.shape[1:]
    n = n - tail
    width = count * d
    if d % LANES:
        own = lax.dynamic_slice_in_dim(sent, c, 1, 0)
        if isinstance(pieces, list):
            buf = jnp.zeros((count, n + tail, d), sent.dtype)
            for i, one in enumerate(pieces):
                g, s = i // size, i % size
                place = ((f + groups - g) % groups) * size + (c + size - s) % size
                buf = lax.dynamic_update_slice(buf, one[None], (place, 0, 0))
        else:
            buf = lax.dynamic_update_slice(pieces, own, (f * size + c, 0, 0))
        flat = buf.transpose(1, 0, 2).reshape(n + tail, width)
        return jnp.concatenate([spread(flat[:n], 0), flat[n:]]) if spaced else flat
    cuts = [(0, 0, n)]
    if spaced:
        cuts = [(i * HALF, i * LANES // 2, HALF) for i in range(n // HALF)]
    tall = n * LANES // HD if spaced else n
    if tail:
        cuts.append((n, tall, tail))
        tall += tail
    refs = pieces if isinstance(pieces, list) else [sent, pieces]
    return pl.pallas_call(
        functools.partial(join_kernel, cuts, groups, size, d),
        out_shape=jax.ShapeDtypeStruct((tall, width), sent.dtype),
        in_specs=[pl.BlockSpec(memory_space=pl.ANY)] * len(refs),
        out_specs=pl.BlockSpec(memory_space=pltpu.VMEM),
        scratch_shapes=[pltpu.SemaphoreType.DMA((count, len(cuts)))],
        compiler_params=pltpu.CompilerParams(vmem_limit_bytes=VLIM),
        cost_estimate=cost(4),
    )(*refs)


def cross(sent):
    size, groups = lax.axis_size("ctx"), lax.axis_size("fsdp")
    c = lax.axis_index("ctx")
    pieces = []
    for s in range(size):
        piece = lax.dynamic_index_in_dim(sent, (c + s) % size, 0, False)
        if s:
            piece = lax.ppermute(piece, "ctx", [(i, (i + s) % size) for i in range(size)])
        pieces.append(piece)
    for g in range(1, groups):
        for s in range(size):
            pieces.append(
                lax.ppermute(
                    pieces[s], "fsdp", [(i, (i + g) % groups) for i in range(groups)]
                )
            )
    return pieces


def hand_out(grad):
    size, groups = lax.axis_size("ctx"), lax.axis_size("fsdp")
    c, f = lax.axis_index("ctx"), lax.axis_index("fsdp")
    rows = grad.shape[0] // groups
    d = rows // size
    total = lax.dynamic_slice_in_dim(grad, f * rows, rows, 0)
    for g in range(1, groups):
        sent = lax.dynamic_slice_in_dim(grad, ((f + g) % groups) * rows, rows, 0)
        got = lax.ppermute(sent, "fsdp", [(i, (i + g) % groups) for i in range(groups)])
        total = total.astype(jnp.float32) + got.astype(jnp.float32)
    total = total.astype(jnp.bfloat16)
    pieces = []
    for s in range(size):
        piece = lax.dynamic_slice_in_dim(total, ((c + s) % size) * d, d, 0)
        if s:
            piece = lax.ppermute(piece, "ctx", [(i, (i + s) % size) for i in range(size)])
        pieces.append(piece)
    return pieces


def finish_kernel(size, *refs):
    gu, down, out = refs[:size], refs[size : 2 * size], refs[2 * size : 3 * size]
    rows, gu_ref, down_ref, out_ref, rows_ref = refs[3 * size :]
    c = lax.axis_index("ctx")
    half, narrow = down[0].shape[1], out[0].shape[1]
    for s in range(size):
        source = (c + size - s) % size
        lanes = pl.ds(pl.multiple_of(source * half, half), half)
        for j in range(2):
            gu_ref[j, :, lanes] = gu[s][:, j * half : (j + 1) * half].astype(jnp.float32)
        down_ref[lanes, :] = down[s][...].astype(jnp.float32).T
        at = pl.ds(pl.multiple_of(source * narrow, narrow), narrow)
        out_ref[at, :] = out[s][...].astype(jnp.float32).T
    rows_ref[...] = rows[...]


def finish_call(gu, down, out, rows, size):
    d, full = gu[0].shape[0], jnp.float32
    vmem = pl.BlockSpec(memory_space=pltpu.VMEM)
    return pl.pallas_call(
        functools.partial(finish_kernel, size),
        out_shape=(
            jax.ShapeDtypeStruct((2, d, size * down[0].shape[1]), full),
            jax.ShapeDtypeStruct((size * down[0].shape[1], d), full),
            jax.ShapeDtypeStruct((size * out[0].shape[1], d), full),
            jax.ShapeDtypeStruct(rows.shape, rows.dtype),
        ),
        in_specs=[vmem] * (3 * size + 1),
        out_specs=(vmem,) * 4,
        compiler_params=pltpu.CompilerParams(vmem_limit_bytes=VLIM),
        cost_estimate=cost(8),
        name="finish",
    )(*gu, *down, *out, rows)


def wide_gather(part):
    full = lax.all_gather(part, GROUP, axis=0, tiled=True)
    return full


def mlp_block(half, pair, buf, ins, outs):
    w, wd, cot = ins
    act, g_gate, g_up = outs
    rows = buf.shape[1]
    tile = 256
    at = pl.ds(pl.multiple_of(pair * rows, rows), rows)

    def one(i, carry):
        lanes = pl.ds(pl.multiple_of(i * tile, tile), tile)
        gate = nt(buf[pair], w[lanes, :])
        up = nt(buf[pair], w[pl.ds(pl.multiple_of(half + i * tile, tile), tile), :])
        grad = nt(cot[at, :], wd[lanes, :])
        sigma = 1.0 / (1.0 + jnp.exp(-gate))
        silu = gate * sigma
        act[at, lanes] = (silu * up).astype(jnp.bfloat16)
        g_up[at, lanes] = (grad * silu).astype(jnp.bfloat16)
        g_gate[at, lanes] = (grad * up * sigma * (1.0 + gate * (1.0 - sigma))).astype(jnp.bfloat16)
        return carry

    lax.fori_loop(0, half // tile, one, 0)


def attn_block(pair, buf, ins, outs):
    rows = buf.shape[1]
    at = pl.ds(pl.multiple_of(pair * rows, rows), rows)
    outs[0][at, :] = nt(buf[pair], ins[0][...]).astype(jnp.bfloat16)


def no_block(pair, buf, ins, outs):
    pass


def nothing():
    pass


def after_out(total, ins, outs, extra):
    tokens, gain = ins
    hidden, normed = outs

    def one(r):
        value = tokens[r, :].astype(jnp.float32) + total[r, :]
        scale = lax.rsqrt(jnp.mean(value * value, axis=1, keepdims=True) + EPSILON)
        hidden[r, :] = value
        normed[r, :] = (value * scale * gain[...]).astype(jnp.bfloat16)

    return nothing, one, nothing


def norm_back(grad, value, gain, top):
    scale = lax.rsqrt(jnp.mean(value * value, axis=1, keepdims=True) + EPSILON)
    unit = value * scale
    g_unit = grad * gain
    inner = jnp.mean(g_unit * unit, axis=1, keepdims=True)
    return top + scale * (g_unit - unit * inner), grad * unit


def after_mlp(total, ins, outs, extra):
    hidden, cot, gain = ins
    g_hidden, g_branch, g_gain = outs

    def begin():
        g_gain[...] = jnp.zeros_like(g_gain)

    def one(r):
        grad, part = norm_back(
            total[r, :], hidden[r, :], gain[...], cot[r, :].astype(jnp.float32)
        )
        g_hidden[r, :] = grad
        g_branch[r, :] = grad.astype(jnp.bfloat16)
        g_gain[...] += part

    return begin, one, nothing


def after_qkv(total, ins, outs, extra):
    tokens, g_hidden, gain, g_gain_mlp, _ = ins
    rows_all, sums = extra[:2]
    place = lax.axis_index("tp")

    def begin():
        sums[4] = jnp.zeros(sums.shape[1:], jnp.float32)

    def one(r):
        grad, part = norm_back(
            total[r, :], tokens[r, :].astype(jnp.float32), gain[...], g_hidden[r, :]
        )
        rows_all[place, r, :] = grad.astype(jnp.bfloat16)
        sums[4] += part[0:8] + part[8:16]

    def end():
        sums[0] = jnp.concatenate(
            [
                jnp.sum(sums[4], axis=0, keepdims=True),
                jnp.sum(g_gain_mlp[...], axis=0, keepdims=True),
                jnp.zeros((6, total.shape[1]), jnp.float32),
            ],
            axis=0,
        )

    return begin, one, end


PLAN = {
    -1: [("z", 0, 1), ("z", 0, 2), ("z", 0, 3), ("x", 0, 0), ("x", 1, 0)],
    0: [("z", 1, 1), ("z", 1, 2), ("z", 1, 3), ("x", 0, 1)],
    1: [("x", 0, 2), ("x", 0, 3), ("x", 1, 1)],
    2: [("x", 1, 2), ("x", 1, 3)],
}
PLAN_OUT = {
    -1: [("z", 0, 1), ("z", 0, 2), ("z", 0, 3), ("x", 0, 0)],
    1: [("x", 0, 1)],
    2: [("x", 0, 2)],
    3: [("x", 0, 3)],
}


def shards(tokens, segments, w_qkv, w_out, w_gate_up, w_down, norm_attn, norm_mlp, cotangent):
    seqs, rows, width = tokens.shape
    size, tp_size = lax.axis_size("ctx"), lax.axis_size("tp")
    length = segments.shape[1]
    assert seqs == 1 and tp_size == 4
    part = rows // tp_size
    begin = lax.axis_index("tp") * part
    scale = 1.0 / math.sqrt(HD)
    low, full = jnp.bfloat16, jnp.float32
    heads = w_qkv.shape[2] // HD // size
    seg = segments[0]

    tokens_own = lax.dynamic_slice_in_dim(tokens[0], begin, part, 0)
    cot_own = lax.dynamic_slice_in_dim(cotangent[0], begin, part, 0)

    d = w_qkv.shape[1]
    gain_rows = jnp.concatenate(
        [norm_attn[None], norm_mlp[None], jnp.zeros((GAIN_ROWS - 2, d), low)], axis=0
    )
    sent_q = w_qkv.reshape(3, d, size, -1).transpose(2, 0, 3, 1)
    sent_q = jnp.concatenate(
        [sent_q.reshape(size, -1, d), jnp.broadcast_to(gain_rows, (size, GAIN_ROWS, d))], axis=1
    )
    sent_o = w_out.reshape(size, -1, d)
    sent_g = w_gate_up.reshape(2, d, size, -1).transpose(2, 0, 3, 1).reshape(size, -1, d)
    sent_d = w_down.reshape(size, -1, d)
    tokens_full, moved_q, moved_o = gather_call(
        tokens_own, [], [], no_block, 1, size, [sent_q, sent_o], PLAN
    )
    wq = join(sent_q, moved_q, True, GAIN_ROWS)
    wo = join(sent_o, moved_o, True)
    wg = join(sent_g, cross(sent_g), False)
    half = sent_d.shape[1]
    tall = 3 * heads * LANES
    gains = wq[tall : tall + 2].astype(full)
    gain_attn, gain_mlp = gains[0:1], gains[1:2]
    cot_gate, tokens_full = lax.optimization_barrier((cot_own, tokens_full))
    cot_full = wide_gather(cot_gate)

    positions = doc_positions(seg)
    cosine, sine = rope_tables(positions)
    starts = (jnp.arange(length, dtype=jnp.int32) - positions)[::BLK] // BLK
    marks = jnp.arange(length // BLK, dtype=jnp.int32)
    ends = jnp.sum((starts[None, :] <= marks[:, None]).astype(jnp.int32), axis=1) - 1

    qkv, normed1 = qkv_call(tokens_full, wq, gain_attn, cosine, sine, heads)
    attn, lse = attend_call(qkv, seg, starts, heads, scale)

    row_shape = jax.ShapeDtypeStruct((part, width), full)
    row_low = jax.ShapeDtypeStruct((part, width), low)
    gain_shape = jax.ShapeDtypeStruct((16, width), full)
    hidden1, normed2_own, moved_d = reduce_call(
        attn,
        wo,
        [tokens_own, gain_mlp],
        [row_shape, row_low],
        after_out,
        2,
        size,
        sent=[sent_d],
        plan=PLAN_OUT,
    )
    wd = join(sent_d, moved_d, False)
    half_shape = jax.ShapeDtypeStruct((length, half), low)
    normed2, act, g_gate, g_up = gather_call(
        normed2_own,
        [wg, wd, cot_full],
        [half_shape] * 3,
        functools.partial(mlp_block, half),
        3,
        size,
    )
    g_gu = jnp.concatenate([g_gate, g_up], axis=1)
    down_part = nn(act, wd).astype(low)
    down = lax.psum_scatter(down_part, GROUP, scatter_dimension=0, tiled=True)
    output = (hidden1 + down.astype(full)).astype(low)
    output = lax.all_gather(output, "tp", axis=0, tiled=True)[None]

    part_down, part_gu = tn(cot_full, act).astype(low), tn(normed2, g_gu).astype(low)
    g_gu, part_down, part_gu = lax.optimization_barrier((g_gu, part_down, part_gu))
    g_hidden1, g_branch_own, g_gain_mlp = reduce_call(
        g_gu, wg, [hidden1, cot_own, gain_mlp], [row_shape, row_low, gain_shape], after_mlp, 4, size
    )
    g_branch, g_attn = gather_call(
        g_branch_own,
        [wo],
        [jax.ShapeDtypeStruct((length, heads * LANES), low)],
        attn_block,
        5,
        size,
    )
    out_down = hand_out(part_down)
    out_gu = hand_out(part_gu)
    part_out = unspread(tn(g_branch, attn), 1).astype(low)
    g_attn, part_out = lax.optimization_barrier((g_attn, part_out))
    g_proj = attend_back_call(qkv, attn, g_attn, lse, seg, ends, cosine, sine, heads, scale)
    out_out = hand_out(part_out)
    part_qkv = unspread(tn(normed1, g_proj), 1).astype(low)
    g_proj, part_qkv = lax.optimization_barrier((g_proj, part_qkv))
    g_tokens, gain_sums, out_qkv = reduce_call(
        g_proj,
        wq,
        [tokens_own, g_hidden1, gain_attn, g_gain_mlp, part_qkv],
        [
            jax.ShapeDtypeStruct((tp_size, part, width), low),
            jax.ShapeDtypeStruct((8, width), full),
            jax.ShapeDtypeStruct((size, d, part_qkv.shape[1]), low),
        ],
        after_qkv,
        6,
        size,
        True,
    )
    g_tokens = g_tokens.reshape(1, rows, width)

    def natural(grad, count):
        wide = grad.astype(full).reshape(size, d, count, -1).transpose(2, 1, 0, 3)
        return wide.reshape(count, d, -1)

    grad_gu, grad_down, grad_out, g_tokens = finish_call(out_gu, out_down, out_out, g_tokens, size)
    grad_qkv = natural(out_qkv, 3)

    mine = lax.axis_index("fsdp") * size + lax.axis_index("ctx")
    gain_grads = lax.dynamic_slice_in_dim(gain_sums, mine * d, d, 1)
    return (
        output,
        g_tokens,
        grad_qkv,
        grad_out,
        grad_gu,
        grad_down,
        gain_grads[0],
        gain_grads[1],
    )


def solution(mesh):
    in_specs = (
        P("fsdp", "ctx", None),
        P("fsdp", None),
        P(None, ("fsdp", "ctx"), "tp"),
        P("tp", ("fsdp", "ctx")),
        P(None, ("fsdp", "ctx"), "tp"),
        P("tp", ("fsdp", "ctx")),
        P(("fsdp", "ctx")),
        P(("fsdp", "ctx")),
        P("fsdp", "ctx", None),
    )
    out_specs = (
        P("fsdp", "ctx", None),
        P("fsdp", "ctx", None),
        P(None, ("fsdp", "ctx"), "tp"),
        P("tp", ("fsdp", "ctx")),
        P(None, ("fsdp", "ctx"), "tp"),
        P("tp", ("fsdp", "ctx")),
        P(("fsdp", "ctx")),
        P(("fsdp", "ctx")),
    )
    return jax.shard_map(shards, mesh=mesh, in_specs=in_specs, out_specs=out_specs, check_vma=False)
```

```python
import functools
import math

import jax
import jax.numpy as jnp
from jax import lax
from jax.experimental import pallas as pl
from jax.experimental.pallas import tpu as pltpu
from jax.sharding import PartitionSpec as P


HD = 96
HALF = HD // 2
LANES = 128
EPSILON = 1e-05
MASK_FILL = -1e30
ROPE_BASE = 10000.0
GROUP = ("ctx", "tp")
BLK = 256
GAIN_ROWS = 16
MESH = pl.DeviceIdType.MESH
SUBS = 2
PARTS = 4
VLIM = 64 * 1024 * 1024 - 65536


def cost(us):
    return pl.CostEstimate(flops=0, bytes_accessed=us * 3_000_000, transcendentals=0)


def near_order(c, j, size):
    low = c < size // 2
    base = jnp.where(low, c, size - 1 - c)
    zig = jnp.where(j % 2 == 1, base - (j + 1) // 2, base + j // 2)
    place = jnp.where(j <= 2 * base, zig, j)
    return jnp.where(low, place, size - 1 - place)


def places():
    c, t = lax.axis_index("ctx"), lax.axis_index("tp")
    return c, t // 2, t % 2


def greet(c, y, k, size):
    barrier = pltpu.get_barrier_semaphore()

    @pl.when(c < size - 1)
    def _():
        pl.semaphore_signal(barrier, inc=1, device_id={"ctx": c + 1}, device_id_type=MESH)

    @pl.when(c > 0)
    def _():
        pl.semaphore_signal(barrier, inc=1, device_id={"ctx": c - 1}, device_id_type=MESH)

    pl.semaphore_signal(barrier, inc=1, device_id={"tp": (1 - y) * 2 + k}, device_id_type=MESH)
    pl.semaphore_signal(barrier, inc=1, device_id={"tp": y * 2 + 1 - k}, device_id_type=MESH)
    pl.semaphore_wait(barrier, jnp.where((c > 0) & (c < size - 1), 4, 3))


def greet_all(c, y, k, size, groups):
    barrier = pltpu.get_barrier_semaphore()
    f = lax.axis_index("fsdp")

    def hello(dev):
        pl.semaphore_signal(barrier, inc=1, device_id=dev, device_id_type=MESH)

    for s in range(1, size):
        hello({"ctx": (c + s) % size})
    for g in range(1, groups):
        hello({"fsdp": (f + g) % groups})
    hello({"tp": (1 - y) * 2 + k})
    hello({"tp": y * 2 + 1 - k})
    pl.semaphore_wait(barrier, size + groups)


class Moves:
    def __init__(self, size, groups, sent, pieces, z_sems, x_sems):
        self.size, self.groups, self.sent, self.pieces = size, groups, sent, pieces
        self.z_sems, self.x_sems = z_sems, x_sems
        self.c, self.f = lax.axis_index("ctx"), lax.axis_index("fsdp")

    def z(self, w, s):
        to = (self.c + s) % self.size
        return pltpu.make_async_remote_copy(
            src_ref=self.sent[w].at[to],
            dst_ref=self.pieces[w].at[self.f * self.size + self.c],
            send_sem=self.z_sems.at[w, s - 1, 0],
            recv_sem=self.z_sems.at[w, s - 1, 1],
            device_id={"ctx": to},
            device_id_type=MESH,
        )

    def x(self, w, g, s):
        slot = self.pieces[w].at[self.f * self.size + (self.c + self.size - s) % self.size]
        return pltpu.make_async_remote_copy(
            src_ref=slot if s else self.sent[w].at[self.c],
            dst_ref=slot,
            send_sem=self.x_sems.at[w, g - 1, s, 0],
            recv_sem=self.x_sems.at[w, g - 1, s, 1],
            device_id={"fsdp": (self.f + g) % self.groups},
            device_id_type=MESH,
        )

    def start_z(self, w, s):
        self.z(w, s).start()

    def start_x(self, w, s):
        if s:
            self.z(w, s).wait_recv()
        for g in range(1, self.groups):
            self.x(w, g, s).start()

    def finish(self):
        for w in range(len(self.sent)):
            for s in range(self.size):
                if s:
                    self.z(w, s).wait_send()
                for g in range(1, self.groups):
                    self.x(w, g, s).wait()


class HandOut:
    def __init__(self, size, groups, part, out, got, mine, ready, x_sems, z_sems, l_sems):
        self.size, self.groups, self.part, self.out = size, groups, part, out
        self.got, self.mine, self.ready = got, mine, ready
        self.x_sems, self.z_sems, self.l_sems = x_sems, z_sems, l_sems
        self.c, self.f = lax.axis_index("ctx"), lax.axis_index("fsdp")
        self.d = mine.shape[1]

    def rows(self, f, c):
        return self.part.at[pl.ds(pl.multiple_of((f * self.size + c) * self.d, self.d), self.d)]

    def x(self, g, cc):
        to = (self.f + g) % self.groups
        return pltpu.make_async_remote_copy(
            src_ref=self.rows(to, cc),
            dst_ref=self.got.at[g - 1, cc],
            send_sem=self.x_sems.at[g - 1, cc, 0],
            recv_sem=self.x_sems.at[g - 1, cc, 1],
            device_id={"fsdp": to},
            device_id_type=MESH,
        )

    def load(self, cc):
        return pltpu.make_async_copy(self.rows(self.f, cc), self.mine.at[cc], self.l_sems.at[cc])

    def z(self, cc, source):
        return pltpu.make_async_remote_copy(
            src_ref=self.ready.at[cc],
            dst_ref=self.out.at[self.c],
            send_sem=self.z_sems.at[cc, 0],
            recv_sem=self.z_sems.at[source, 1],
            device_id={"ctx": cc},
            device_id_type=MESH,
        )

    def keep(self):
        return pltpu.make_async_copy(
            self.ready.at[self.c], self.out.at[self.c], self.l_sems.at[self.size]
        )

    def each(self, body):
        def one(i, carry):
            body(i)
            return carry

        lax.fori_loop(0, self.size, one, 0)

    def start(self, cc):
        for g in range(1, self.groups):
            self.x(g, cc).start()
        self.load(cc).start()

    def step(self, cc):
        self.load(cc).wait()
        for g in range(1, self.groups):
            self.x(g, cc).wait_recv()

        def add(i, carry):
            r = pl.ds(pl.multiple_of(i * 16, 16), 16)
            value = self.mine[cc, r, :].astype(jnp.float32)
            for g in range(1, self.groups):
                value = value + self.got[g - 1, cc, r, :].astype(jnp.float32)
            self.ready[cc, r, :] = value.astype(jnp.bfloat16)
            return carry

        lax.fori_loop(0, self.d // 16, add, 0)

        @pl.when(cc != self.c)
        def _():
            self.z(cc, self.c).start()

        @pl.when(cc == self.c)
        def _():
            self.keep().start()

    def finish(self):
        def one(cc):
            for g in range(1, self.groups):
                self.x(g, cc).wait_send()

            @pl.when(cc != self.c)
            def _():
                self.z(cc, self.c).wait_send()
                self.z(cc, cc).wait_recv()

        self.each(one)
        self.keep().wait()


def gather_kernel(size, groups, plan, n_move, part, n_in, n_out, compute, *refs):
    x_ref = refs[0]
    hbm_ins = refs[1 : 1 + n_in]
    sent = refs[1 + n_in : 1 + n_in + n_move]
    refs = refs[1 + n_in + n_move :]
    full_ref = refs[0]
    outs = refs[1 : 1 + n_out]
    moved = refs[1 + n_out : 1 + n_out + n_move]
    refs = refs[1 + n_out + n_move :]
    ins = refs[:n_in]
    buf, recv, zs, ys, ks, local, load, in_sems, *move_sems = refs[n_in:]
    moves = Moves(size, groups, sent, moved, *move_sems) if n_move else None
    c, y, k = places()
    sub = part // SUBS

    def slot(cc, yy, kk, s):
        return buf.at[cc * 2 + yy, pl.ds(pl.multiple_of(kk * part + s * sub, sub), sub)]

    def copy(cc, yy, kk, s, sem, dev):
        return pltpu.make_async_remote_copy(
            src_ref=slot(cc, yy, kk, s),
            dst_ref=slot(cc, yy, kk, s),
            send_sem=sem,
            recv_sem=recv.at[cc * 2 + yy, kk, s],
            device_id=dev,
            device_id_type=MESH,
        )

    up, down = {"ctx": c + 1}, {"ctx": c - 1}
    ydev, kdev = {"tp": (1 - y) * 2 + k}, {"tp": y * 2 + 1 - k}

    def z_up(cc, s):
        return copy(cc, y, k, s, zs.at[0, cc, s], up)

    def z_down(cc, s):
        return copy(cc, y, k, s, zs.at[1, cc, s], down)

    def y_send(cc, s):
        return copy(cc, y, k, s, ys.at[cc, s], ydev)

    def k_send(cc, yy, s):
        return copy(cc, yy, k, s, ks.at[cc * 2 + yy, s], kdev)

    def pair_out(cc, yy):
        pair = cc * 2 + yy
        return pltpu.make_async_copy(
            buf.at[pair],
            full_ref.at[pl.ds(pl.multiple_of(pair * 2 * part, 2 * part), 2 * part)],
            local.at[pair],
        )

    def got(cc, yy, kk, s):
        copy(cc, yy, kk, s, ys.at[0, 0], ydev).wait_recv()

    mine = buf.at[c * 2 + y, pl.ds(pl.multiple_of(k * part, part), part)]
    first = pltpu.make_async_copy(x_ref, mine, load)
    first.start()
    for i in range(n_in):
        pltpu.make_async_copy(hbm_ins[i], ins[i], in_sems.at[i]).start()
    if moves:
        greet_all(c, y, k, size, groups)
    else:
        greet(c, y, k, size)
    first.wait()

    def z_stage(cc, s):
        @pl.when((cc <= c) & (c < size - 1))
        def _():
            z_up(cc, s).start()

        @pl.when((cc >= c) & (c > 0))
        def _():
            z_down(cc, s).start()

        y_send(cc, s).start()
        k_send(cc, y, s).start()

    for s in range(SUBS):
        z_stage(c, s)

    def move_on(step):
        for kind, w, s in plan.get(step, ()):
            (moves.start_z if kind == "z" else moves.start_x)(w, s)

    move_on(-1)
    for i in range(n_in):
        pltpu.make_async_copy(hbm_ins[i], ins[i], in_sems.at[i]).wait()

    def finish(cc, yy):
        for s in range(SUBS):
            got(cc, yy, 1 - k, s)
        pair_out(cc, yy).start()
        compute(cc * 2 + yy, buf, ins, outs)

    def step(r, carry):
        for s in range(SUBS):
            for sign in (-1, 1):
                nxt = c + sign * (r + 1)

                @pl.when((nxt >= 0) & (nxt < size))
                def _():
                    got(nxt, y, k, s)
                    z_stage(nxt, s)

            for sign in (-1, 1):
                cc = c + sign * r

                @pl.when((cc >= 0) & (cc < size) & ((r > 0) | (sign > 0)))
                def _():
                    if s == SUBS - 1:
                        finish(cc, y)
                    got(cc, 1 - y, k, s)
                    k_send(cc, 1 - y, s).start()
                    if s == SUBS - 1:
                        finish(cc, 1 - y)

        for at in sorted(plan):
            if at >= 0:

                @pl.when(r == at)
                def _():
                    move_on(at)

        return carry

    lax.fori_loop(0, size, step, 0)

    def drain(cc, carry):
        for s in range(SUBS):
            @pl.when((cc <= c) & (c < size - 1))
            def _():
                z_up(cc, s).wait_send()

            @pl.when((cc >= c) & (c > 0))
            def _():
                z_down(cc, s).wait_send()

            y_send(cc, s).wait_send()
            for yy in range(2):
                k_send(cc, yy, s).wait_send()
        for yy in range(2):
            pair_out(cc, yy).wait()
        return carry

    lax.fori_loop(0, size, drain, 0)
    if moves:
        moves.finish()


def gather_call(x, ins, out_shapes, compute, cid, size, sent=(), plan=None):
    part, width = x.shape
    groups = lax.axis_size("fsdp")
    dma = pltpu.SemaphoreType.DMA
    any_spec = pl.BlockSpec(memory_space=pl.ANY)
    vmem = pl.BlockSpec(memory_space=pltpu.VMEM)
    full = jax.ShapeDtypeStruct((size * 4 * part, width), x.dtype)
    return pl.pallas_call(
        functools.partial(
            gather_kernel,
            size,
            groups,
            plan or {},
            len(sent),
            part,
            len(ins),
            len(out_shapes),
            compute,
        ),
        out_shape=(
            full,
            *out_shapes,
            *(
                jax.ShapeDtypeStruct((groups * size, *one.shape[1:]), one.dtype)
                for one in sent
            ),
        ),
        in_specs=[any_spec] * (1 + len(ins) + len(sent)),
        out_specs=(any_spec, *([vmem] * len(out_shapes)), *([any_spec] * len(sent))),
        scratch_shapes=[
            *(pltpu.VMEM(one.shape, one.dtype) for one in ins),
            pltpu.VMEM((size * 2, 2 * part, width), x.dtype),
            pltpu.SemaphoreType.DMA((size * 2, 2, SUBS)),
            pltpu.SemaphoreType.DMA((2, size, SUBS)),
            pltpu.SemaphoreType.DMA((size, SUBS)),
            pltpu.SemaphoreType.DMA((size * 2, SUBS)),
            pltpu.SemaphoreType.DMA((size * 2,)),
            pltpu.SemaphoreType.DMA,
            pltpu.SemaphoreType.DMA((max(len(ins), 1),)),
            *(
                [dma((len(sent), size - 1, 2)), dma((len(sent), max(groups - 1, 1), size, 2))]
                if sent
                else []
            ),
        ],
        compiler_params=pltpu.CompilerParams(
            collective_id=cid, has_side_effects=True, vmem_limit_bytes=VLIM
        ),
        cost_estimate=cost(75),
    )(x, *ins, *sent)


def reduce_kernel(size, groups, last, plan, n_move, part, n_in, n_out, final, *refs):
    a_ref, w_ref = refs[:2]
    ins = refs[2 : 2 + n_in]
    sent = refs[2 + n_in : 2 + n_in + n_move]
    refs = refs[n_move:]
    outs = refs[2 + n_in : 2 + n_in + n_out]
    moved = refs[2 + n_in + n_out : 2 + n_in + n_out + n_move]
    refs = refs[n_move:]
    (
        own,
        ksend,
        krecv,
        ysend,
        yrecv,
        qown,
        zsend,
        zrecv,
        total,
        prod,
        k_sems,
        y_sems,
        z_sems,
        *extra,
    ) = refs[2 + n_in + n_out :]
    moves = Moves(size, groups, sent, moved, *extra) if n_move else None
    hand = HandOut(size, groups, ins[-1], outs[2], *extra[9:]) if last else None
    c, y, k = places()
    depth = a_ref.shape[1]
    chunk = 16
    tile = 512
    width = total.shape[1]

    sub = part // PARTS

    def remote(src, dst, sems, dev):
        return pltpu.make_async_remote_copy(
            src_ref=src,
            dst_ref=dst,
            send_sem=sems.at[0],
            recv_sem=sems.at[1],
            device_id=dev,
            device_id_type=MESH,
        )

    ydev, kdev = {"tp": (1 - y) * 2 + k}, {"tp": y * 2 + 1 - k}

    def k_copy(cc, yy):
        pair = cc * 2 + yy
        return remote(ksend.at[pair], krecv.at[pair], k_sems.at[pair], kdev)

    def y_copy(cc, s):
        r = pl.ds(s * sub, sub)
        return remote(ysend.at[cc, r], yrecv.at[cc, r], y_sems.at[cc, s], ydev)

    def z_up(cc, s):
        r = pl.ds(s * sub, sub)
        return remote(zsend.at[cc, r], zrecv.at[0, cc, r], z_sems.at[0, cc, s], {"ctx": c + 1})

    def z_down(cc, s):
        r = pl.ds(s * sub, sub)
        return remote(zsend.at[cc, r], zrecv.at[1, cc, r], z_sems.at[1, cc, s], {"ctx": c - 1})

    def z_got(into, cc, s):
        r = pl.ds(s * sub, sub)
        remote(zsend.at[cc, r], zrecv.at[into, cc, r], z_sems.at[into, cc, s], ydev).wait_recv()

    if last or moves:
        greet_all(c, y, k, size, groups)
    else:
        greet(c, y, k, size)

    def move_on(step):
        for kind, w, s in plan.get(step, ()):
            (moves.start_z if kind == "z" else moves.start_x)(w, s)

    move_on(-1)

    def rows(i):
        return pl.ds(pl.multiple_of(i * chunk, chunk), chunk)

    def sweep(body, s=None):
        steps = part // chunk
        lo, hi = (0, steps) if s is None else (s * steps // PARTS, (s + 1) * steps // PARTS)

        def one(i, carry):
            body(rows(i))
            return carry

        lax.fori_loop(lo, hi, one, 0)

    def produce(cc, yy, keep):
        pair = cc * 2 + yy
        both = pl.ds(pl.multiple_of(pair * 2 * part, 2 * part), 2 * part)
        mine = pl.ds(pl.multiple_of(k * part, part), part)
        other = pl.ds(pl.multiple_of((1 - k) * part, part), part)

        def one(i, carry):
            lanes = pl.ds(pl.multiple_of(i * tile, tile), tile)
            prod[...] = jnp.dot(
                a_ref[both, :], w_ref[0:depth, lanes], preferred_element_type=jnp.float32
            )
            ksend[pair, :, lanes] = prod[other, :].astype(jnp.bfloat16)
            own[keep, :, lanes] = prod[mine, :]
            return carry

        lax.fori_loop(0, width // tile, one, 0)
        k_copy(cc, yy).start()

    def first(j):
        cc = near_order(c, size - 1 - j, size)
        if last:
            hand.start(cc)
        produce(cc, 1 - y, 0)
        k_copy(cc, 1 - y).wait_recv()

        def add_y(r):
            got = krecv[cc * 2 + 1 - y, r, :].astype(jnp.float32)
            ysend[cc, r, :] = (own[0, r, :] + got).astype(jnp.bfloat16)

        for s in range(PARTS):
            sweep(add_y, s)
            y_copy(cc, s).start()
        produce(cc, y, 1)
        k_copy(cc, y).wait_recv()

        def add_k(r):
            qown[cc, r, :] = own[1, r, :] + krecv[cc * 2 + y, r, :].astype(jnp.float32)

        sweep(add_k)

    def pass_on(cc, s, into, edge, send):
        @pl.when(jnp.logical_not(edge))
        def _():
            z_got(into, cc, s)

            def add(r):
                part_sum = qown[cc, r, :] + yrecv[cc, r, :].astype(jnp.float32)
                zsend[cc, r, :] = (part_sum + zrecv[into, cc, r, :].astype(jnp.float32)).astype(
                    jnp.bfloat16
                )

            sweep(add, s)

        @pl.when(edge)
        def _():
            def add(r):
                part_sum = qown[cc, r, :] + yrecv[cc, r, :].astype(jnp.float32)
                zsend[cc, r, :] = part_sum.astype(jnp.bfloat16)

            sweep(add, s)

        send(cc, s).start()

    def second(j):
        cc = near_order(c, size - 1 - j, size)
        for s in range(PARTS):

            @pl.when(cc > c)
            def _():
                y_copy(cc, s).wait_recv()
                pass_on(cc, s, 0, c == 0, z_up)

            @pl.when(cc < c)
            def _():
                y_copy(cc, s).wait_recv()
                pass_on(cc, s, 1, c == size - 1, z_down)

        if last:
            hand.step(cc)

        for at in sorted(plan):
            if at >= 0:

                @pl.when(j == at)
                def _():
                    move_on(at)

    lag = jnp.where((c == 0) | (c == size - 1), 1, 2)

    def both(i, carry):
        @pl.when(i < size)
        def _():
            first(i)

        @pl.when((i >= lag) & (i - lag < size))
        def _():
            second(i - lag)

        return carry

    lax.fori_loop(0, size + 2, both, 0)

    def sum_up(r):
        own_sum = qown[c, r, :] + yrecv[c, r, :].astype(jnp.float32)

        @pl.when(c == 0)
        def _():
            total[r, :] = own_sum + zrecv[1, c, r, :].astype(jnp.float32)

        @pl.when(c == size - 1)
        def _():
            total[r, :] = own_sum + zrecv[0, c, r, :].astype(jnp.float32)

        @pl.when((c > 0) & (c < size - 1))
        def _():
            below = own_sum + zrecv[0, c, r, :].astype(jnp.float32)
            total[r, :] = below + zrecv[1, c, r, :].astype(jnp.float32)

    begin, one_chunk, end = final(total, ins, outs, extra)
    begin()
    for s in range(PARTS):
        y_copy(c, s).wait_recv()

        @pl.when(c > 0)
        def _():
            z_got(0, c, s)

        @pl.when(c < size - 1)
        def _():
            z_got(1, c, s)

        def close(r):
            sum_up(r)
            one_chunk(r)

        sweep(close, s)
    end()
    if last:
        spread_out(size, groups, c, y, k, ydev, kdev, outs, extra)

    def drain(cc, carry):
        for yy in range(2):
            k_copy(cc, yy).wait_send()
        for s in range(PARTS):
            y_copy(cc, s).wait_send()

            @pl.when(cc > c)
            def _():
                z_up(cc, s).wait_send()

            @pl.when(cc < c)
            def _():
                z_down(cc, s).wait_send()

        return carry

    lax.fori_loop(0, size, drain, 0)
    if moves:
        moves.finish()
    if last:
        hand.finish()


def spread_out(size, groups, c, y, k, ydev, kdev, outs, extra):
    rows_all, sums, got, row_sems, k_sem, y_sem, f_sems, z_sems, out_sem = extra[:9]
    f = lax.axis_index("fsdp")

    def copy(src, dst, sems, dev):
        return pltpu.make_async_remote_copy(
            src_ref=src,
            dst_ref=dst,
            send_sem=sems.at[0],
            recv_sem=sems.at[1],
            device_id=dev,
            device_id_type=MESH,
        )

    def row_copy(yy, kk, n, dev):
        slot = rows_all.at[yy * 2 + kk]
        return copy(slot, slot, row_sems.at[n], dev)

    to_y, to_k, on_k = row_copy(y, k, 0, ydev), row_copy(y, k, 1, kdev), row_copy(1 - y, k, 2, kdev)
    to_y.start()
    to_k.start()

    def add(n, first, count):
        value = sums[n]
        for i in range(first, first + count):
            value = value + got[i]
        sums[n + 1] = value

    swap_k = copy(sums.at[0], got.at[0], k_sem, kdev)
    swap_k.start()
    swap_k.wait()
    add(0, 0, 1)
    swap_y = copy(sums.at[1], got.at[1], y_sem, ydev)
    swap_y.start()
    swap_y.wait()
    add(1, 1, 1)
    swaps = [
        copy(sums.at[2], got.at[1 + g], f_sems.at[g - 1], {"fsdp": (f + g) % groups})
        for g in range(1, groups)
    ]
    for one in swaps:
        one.start()
    for one in swaps:
        one.wait()
    add(2, 2, groups - 1)
    swaps = [
        copy(sums.at[3], got.at[groups + s], z_sems.at[s - 1], {"ctx": (c + s) % size})
        for s in range(1, size)
    ]
    for one in swaps:
        one.start()
    row_copy(1 - y, k, 0, ydev).wait_recv()
    on_k.start()
    for one in swaps:
        one.wait()
    add(3, groups + 1, size - 1)
    outs[1][...] = sums[4]
    row_copy(y, 1 - k, 1, kdev).wait_recv()
    row_copy(1 - y, 1 - k, 2, kdev).wait_recv()
    to_y.wait_send()
    to_k.wait_send()
    on_k.wait_send()
    out = pltpu.make_async_copy(rows_all, outs[0], out_sem)
    out.start()
    out.wait()


def reduce_call(a, w, ins, out_shapes, final, cid, size, last=False, sent=(), plan=None):
    width = w.shape[1]
    part = a.shape[0] // (size * 4)
    vmem = pl.BlockSpec(memory_space=pltpu.VMEM)
    low, full = jnp.bfloat16, jnp.float32
    groups = lax.axis_size("fsdp")
    any_spec = pl.BlockSpec(memory_space=pl.ANY)
    dma = pltpu.SemaphoreType.DMA
    out_specs, extra = [vmem] * len(out_shapes), []
    if sent:
        extra = [dma((len(sent), size - 1, 2)), dma((len(sent), max(groups - 1, 1), size, 2))]
    if last:
        out_specs[0] = out_specs[2] = any_spec
        extra = [
            pltpu.VMEM((4, part, width), low),
            pltpu.VMEM((5, 8, width), full),
            pltpu.VMEM((groups + size, 8, width), full),
            dma((3, 2)),
            dma((2,)),
            dma((2,)),
            dma((max(groups - 1, 1), 2)),
            dma((size - 1, 2)),
            dma,
            pltpu.VMEM((max(groups - 1, 1), *out_shapes[2].shape), low),
            pltpu.VMEM(out_shapes[2].shape, low),
            pltpu.VMEM(out_shapes[2].shape, low),
            dma((max(groups - 1, 1), size, 2)),
            dma((size, 2)),
            dma((size + 1,)),
        ]
    return pl.pallas_call(
        functools.partial(
            reduce_kernel,
            size,
            groups,
            last,
            plan or {},
            len(sent),
            part,
            len(ins),
            len(out_shapes),
            final,
        ),
        out_shape=(
            *out_shapes,
            *(
                jax.ShapeDtypeStruct((groups * size, *one.shape[1:]), one.dtype)
                for one in sent
            ),
        ),
        in_specs=[vmem] * (1 + len(ins))
        + [any_spec if last else vmem]
        + [any_spec] * len(sent),
        out_specs=(*out_specs, *([any_spec] * len(sent))),
        scratch_shapes=[
            pltpu.VMEM((2, part, width), full),
            pltpu.VMEM((size * 2, part, width), low),
            pltpu.VMEM((size * 2, part, width), low),
            pltpu.VMEM((size, part, width), low),
            pltpu.VMEM((size, part, width), low),
            pltpu.VMEM((size, part, width), full),
            pltpu.VMEM((size, part, width), low),
            pltpu.VMEM((2, size, part, width), low),
            pltpu.VMEM((part, width), full),
            pltpu.VMEM((2 * part, 512), full),
            pltpu.SemaphoreType.DMA((size * 2, 2)),
            pltpu.SemaphoreType.DMA((size, PARTS, 2)),
            pltpu.SemaphoreType.DMA((2, size, PARTS, 2)),
            *extra,
        ],
        compiler_params=pltpu.CompilerParams(
            collective_id=cid, has_side_effects=True, vmem_limit_bytes=VLIM
        ),
        cost_estimate=cost(85),
    )(a, w, *ins, *sent)


def doc_positions(segment_row):
    places_in = jnp.arange(segment_row.shape[0], dtype=jnp.int32)
    starts = jnp.concatenate([jnp.ones((1,), dtype=jnp.bool_), segment_row[1:] != segment_row[:-1]])
    first = lax.cummax(jnp.where(starts, places_in, jnp.zeros_like(places_in)), axis=0)
    return places_in - first


def rope_tables(positions):
    freqs = ROPE_BASE ** (-(jnp.arange(HALF, dtype=jnp.float32) * 2.0 / HD))
    angles = positions.astype(jnp.float32)[:, None] * freqs
    gap = jnp.zeros((positions.shape[0], LANES // 2 - HALF), jnp.float32)
    cosine, sine = jnp.cos(angles), jnp.sin(angles)
    return (
        jnp.concatenate([cosine, gap, cosine, gap], axis=1),
        jnp.concatenate([-sine, gap, sine, gap], axis=1),
    )


def spread(array, axis):
    shape = array.shape
    halves = array.reshape(*shape[:axis], shape[axis] // HALF, HALF, *shape[axis + 1 :])
    pads = [(0, 0)] * halves.ndim
    pads[axis + 1] = (0, LANES // 2 - HALF)
    wide = jnp.pad(halves, pads)
    return wide.reshape(*shape[:axis], -1, *shape[axis + 1 :])


def unspread(array, axis):
    shape = array.shape
    half = LANES // 2
    halves = array.reshape(*shape[:axis], shape[axis] // half, half, *shape[axis + 1 :])
    kept = lax.slice_in_dim(halves, 0, HALF, axis=axis + 1)
    return kept.reshape(*shape[:axis], -1, *shape[axis + 1 :])


def nt(left, right):
    return lax.dot_general(left, right, (((1,), (1,)), ((), ())), preferred_element_type=jnp.float32)


def nn(left, right):
    return jnp.dot(left, right, preferred_element_type=jnp.float32)


def tn(left, right):
    return lax.dot_general(left, right, (((0,), (0,)), ((), ())), preferred_element_type=jnp.float32)


def qkv_kernel(heads, x_ref, w_ref, gain_ref, cos_ref, sin_ref, out_ref, normed_ref):
    for i in range(BLK // 16):
        at = slice(i * 16, (i + 1) * 16)
        x = x_ref[at, :].astype(jnp.float32)
        scale = lax.rsqrt(jnp.mean(x * x, axis=1, keepdims=True) + EPSILON)
        normed_ref[at, :] = (x * scale * gain_ref[...]).astype(jnp.bfloat16)
    proj = nt(normed_ref[...], w_ref[...])
    for i in range(3 * heads):
        cut = slice(i * LANES, (i + 1) * LANES)
        one = proj[:, cut]
        if i < 2 * heads:
            one = one * cos_ref[...] + pltpu.roll(one, LANES // 2, 1) * sin_ref[...]
        out_ref[:, cut] = one.astype(jnp.bfloat16)


def qkv_call(x, w, gain, cosine, sine, heads):
    rows, width = x.shape
    tall = 3 * heads * LANES
    return pl.pallas_call(
        functools.partial(qkv_kernel, heads),
        out_shape=(
            jax.ShapeDtypeStruct((rows, tall), jnp.bfloat16),
            jax.ShapeDtypeStruct((rows, width), jnp.bfloat16),
        ),
        grid=(rows // BLK,),
        in_specs=[
            pl.BlockSpec((BLK, width), lambda i: (i, 0)),
            pl.BlockSpec((tall, width), lambda i: (0, 0)),
            pl.BlockSpec((1, width), lambda i: (0, 0)),
            pl.BlockSpec((BLK, LANES), lambda i: (i, 0)),
            pl.BlockSpec((BLK, LANES), lambda i: (i, 0)),
        ],
        out_specs=(
            pl.BlockSpec((BLK, tall), lambda i: (i, 0)),
            pl.BlockSpec((BLK, width), lambda i: (i, 0)),
        ),
        compiler_params=pltpu.CompilerParams(vmem_limit_bytes=VLIM),
        cost_estimate=cost(18),
        name="qkv",
    )(x, w, gain, cosine, sine)


def block(ref, i, head):
    return ref[pl.ds(pl.multiple_of(i * BLK, BLK), BLK), head * LANES : (head + 1) * LANES]


def masked_scores(keys, query, seg_col, seg_row, kb, qb, scale):
    scores = nt(keys, query) * scale
    key_pos = kb * BLK + lax.broadcasted_iota(jnp.int32, scores.shape, 0)
    query_pos = qb * BLK + lax.broadcasted_iota(jnp.int32, scores.shape, 1)
    return jnp.where((key_pos <= query_pos) & (seg_col == seg_row), scores, MASK_FILL)


def attend_kernel(heads, scale, low_ref, qkv_ref, col_ref, row_ref, out_ref, lse_ref):
    blocks = qkv_ref.shape[0] // BLK

    def one(i, carry):
        cut = pl.ds(pl.multiple_of(i * BLK, BLK), BLK)
        seg_row = row_ref[:, cut]
        for h in range(heads):
            query = block(qkv_ref, i, h)

            def inner(kb, state):
                peak, total, acc = state
                keys = block(qkv_ref, kb, heads + h)
                seg_col = col_ref[pl.ds(pl.multiple_of(kb * BLK, BLK), BLK), :]
                scores = masked_scores(keys, query, seg_col, seg_row, kb, i, scale)
                new = jnp.maximum(peak, jnp.max(scores, axis=0, keepdims=True))
                fade = jnp.exp(peak - new)
                expo = jnp.exp(scores - new)
                total = total * fade + jnp.sum(expo, axis=0, keepdims=True)
                mixed = tn(block(qkv_ref, kb, 2 * heads + h), expo.astype(jnp.bfloat16))
                return new, total, acc * fade + mixed

            peak, total, acc = lax.fori_loop(
                low_ref[i],
                i + 1,
                inner,
                (
                    jnp.full((1, BLK), MASK_FILL, jnp.float32),
                    jnp.zeros((1, BLK), jnp.float32),
                    jnp.zeros((LANES, BLK), jnp.float32),
                ),
            )
            out_ref[cut, h * LANES : (h + 1) * LANES] = (acc / total).T.astype(jnp.bfloat16)
            lse_ref[h : h + 1, cut] = peak + jnp.log(total)
        return carry

    lax.fori_loop(0, blocks, one, 0)


def attend_call(qkv, seg, low, heads, scale):
    rows = qkv.shape[0]
    vmem = pl.BlockSpec(memory_space=pltpu.VMEM)
    return pl.pallas_call(
        functools.partial(attend_kernel, heads, scale),
        out_shape=(
            jax.ShapeDtypeStruct((rows, heads * LANES), jnp.bfloat16),
            jax.ShapeDtypeStruct((heads, rows), jnp.float32),
        ),
        in_specs=[pl.BlockSpec(memory_space=pltpu.SMEM), vmem, vmem, vmem],
        out_specs=(vmem, vmem),
        compiler_params=pltpu.CompilerParams(vmem_limit_bytes=VLIM),
        cost_estimate=cost(20),
        name="attend",
    )(low, qkv, seg[:, None], seg[None, :])


def attend_back_kernel(
    heads,
    scale,
    high_ref,
    qkv_ref,
    out_ref,
    grad_ref,
    lse_ref,
    col_ref,
    row_ref,
    cos_ref,
    sin_ref,
    res_ref,
    delta_ref,
    gq_ref,
):
    blocks = qkv_ref.shape[0] // BLK
    gq_ref[...] = jnp.zeros_like(gq_ref)

    def dots(i, carry):
        cut = pl.ds(pl.multiple_of(i * BLK, BLK), BLK)
        for h in range(heads):
            prod = block(out_ref, i, h).astype(jnp.float32) * block(grad_ref, i, h).astype(
                jnp.float32
            )
            delta_ref[h : h + 1, cut] = jnp.sum(prod.T, axis=0, keepdims=True)
        return carry

    lax.fori_loop(0, blocks, dots, 0)

    def turn_back(value, cut):
        low = value.astype(jnp.bfloat16).astype(jnp.float32)
        turned = low * cos_ref[cut, :] - pltpu.roll(low, LANES // 2, 1) * sin_ref[cut, :]
        return turned.astype(jnp.bfloat16)

    def one(kb, carry):
        cut = pl.ds(pl.multiple_of(kb * BLK, BLK), BLK)
        seg_col = col_ref[cut, :]
        for h in range(heads):
            keys = block(qkv_ref, kb, heads + h)
            values = block(qkv_ref, kb, 2 * heads + h)

            def inner(i, state):
                gk, gv = state
                at = pl.ds(pl.multiple_of(i * BLK, BLK), BLK)
                query = block(qkv_ref, i, h)
                grad = block(grad_ref, i, h)
                scores = masked_scores(keys, query, seg_col, row_ref[:, at], kb, i, scale)
                probs = jnp.exp(scores - lse_ref[h : h + 1, at])
                gv = gv + nn(probs.astype(jnp.bfloat16), grad)
                g_probs = nt(values, grad)
                g_scores = (probs * (g_probs - delta_ref[h : h + 1, at])).astype(jnp.bfloat16)
                gk = gk + nn(g_scores, query)
                lanes = slice(h * LANES, (h + 1) * LANES)
                gq_ref[at, lanes] += tn(g_scores, keys)
                return gk, gv

            zero = jnp.zeros((BLK, LANES), jnp.float32)
            gk, gv = lax.fori_loop(kb, high_ref[kb] + 1, inner, (zero, zero))
            at_k = slice((heads + h) * LANES, (heads + h + 1) * LANES)
            at_v = slice((2 * heads + h) * LANES, (2 * heads + h + 1) * LANES)
            res_ref[cut, at_k] = turn_back(gk * scale, cut)
            res_ref[cut, at_v] = gv.astype(jnp.bfloat16)
        return carry

    lax.fori_loop(0, blocks, one, 0)

    def close(i, carry):
        cut = pl.ds(pl.multiple_of(i * BLK, BLK), BLK)
        for h in range(heads):
            lanes = slice(h * LANES, (h + 1) * LANES)
            res_ref[cut, lanes] = turn_back(gq_ref[cut, lanes] * scale, cut)
        return carry

    lax.fori_loop(0, blocks, close, 0)


def attend_back_call(qkv, out, grad, lse, seg, high, cosine, sine, heads, scale):
    rows = qkv.shape[0]
    vmem = pl.BlockSpec(memory_space=pltpu.VMEM)
    return pl.pallas_call(
        functools.partial(attend_back_kernel, heads, scale),
        out_shape=jax.ShapeDtypeStruct(qkv.shape, jnp.bfloat16),
        in_specs=[pl.BlockSpec(memory_space=pltpu.SMEM)] + [vmem] * 8,
        out_specs=vmem,
        scratch_shapes=[
            pltpu.VMEM((heads, rows), jnp.float32),
            pltpu.VMEM((rows, heads * LANES), jnp.float32),
        ],
        compiler_params=pltpu.CompilerParams(vmem_limit_bytes=VLIM),
        cost_estimate=cost(32),
        name="attend_back",
    )(high, qkv, out, grad, lse, seg[:, None], seg[None, :], cosine, sine)


def join_kernel(cuts, groups, size, d, *refs):
    *pieces, out, sems = refs
    c, f = lax.axis_index("ctx"), lax.axis_index("fsdp")

    def copies(go):
        for i in range(groups * size):
            g, s = i // size, i % size
            place = ((f + groups - g) % groups) * size + (c + size - s) % size
            lanes = pl.ds(pl.multiple_of(place * d, d), d)
            for q, (src, dst, rows) in enumerate(cuts):
                if len(pieces) > 2:
                    piece = pieces[i]
                else:
                    piece = pieces[1].at[place] if i else pieces[0].at[c]
                go(
                    pltpu.make_async_copy(
                        piece.at[pl.ds(src, rows)], out.at[pl.ds(dst, rows), lanes], sems.at[i, q]
                    )
                )

    copies(lambda one: one.start())
    for q, (_, dst, rows) in enumerate(cuts):
        stop = cuts[q + 1][1] if q + 1 < len(cuts) else out.shape[0]
        if dst + rows < stop:
            gap = stop - dst - rows
            out[pl.ds(dst + rows, gap), :] = jnp.zeros((gap, out.shape[1]), out.dtype)
    copies(lambda one: one.wait())


def join(sent, pieces, spaced, tail=0):
    size, groups = lax.axis_size("ctx"), lax.axis_size("fsdp")
    c, f = lax.axis_index("ctx"), lax.axis_index("fsdp")
    count, (n, d) = size * groups, sent.shape[1:]
    n = n - tail
    width = count * d
    if d % LANES:
        own = lax.dynamic_slice_in_dim(sent, c, 1, 0)
        if isinstance(pieces, list):
            buf = jnp.zeros((count, n + tail, d), sent.dtype)
            for i, one in enumerate(pieces):
                g, s = i // size, i % size
                place = ((f + groups - g) % groups) * size + (c + size - s) % size
                buf = lax.dynamic_update_slice(buf, one[None], (place, 0, 0))
        else:
            buf = lax.dynamic_update_slice(pieces, own, (f * size + c, 0, 0))
        flat = buf.transpose(1, 0, 2).reshape(n + tail, width)
        return jnp.concatenate([spread(flat[:n], 0), flat[n:]]) if spaced else flat
    cuts = [(0, 0, n)]
    if spaced:
        cuts = [(i * HALF, i * LANES // 2, HALF) for i in range(n // HALF)]
    tall = n * LANES // HD if spaced else n
    if tail:
        cuts.append((n, tall, tail))
        tall += tail
    refs = pieces if isinstance(pieces, list) else [sent, pieces]
    return pl.pallas_call(
        functools.partial(join_kernel, cuts, groups, size, d),
        out_shape=jax.ShapeDtypeStruct((tall, width), sent.dtype),
        in_specs=[pl.BlockSpec(memory_space=pl.ANY)] * len(refs),
        out_specs=pl.BlockSpec(memory_space=pltpu.VMEM),
        scratch_shapes=[pltpu.SemaphoreType.DMA((count, len(cuts)))],
        compiler_params=pltpu.CompilerParams(vmem_limit_bytes=VLIM),
        cost_estimate=cost(4),
    )(*refs)


def cross(sent):
    size, groups = lax.axis_size("ctx"), lax.axis_size("fsdp")
    c = lax.axis_index("ctx")
    pieces = []
    for s in range(size):
        piece = lax.dynamic_index_in_dim(sent, (c + s) % size, 0, False)
        if s:
            piece = lax.ppermute(piece, "ctx", [(i, (i + s) % size) for i in range(size)])
        pieces.append(piece)
    for g in range(1, groups):
        for s in range(size):
            pieces.append(
                lax.ppermute(
                    pieces[s], "fsdp", [(i, (i + g) % groups) for i in range(groups)]
                )
            )
    return pieces


def hand_out(grad):
    size, groups = lax.axis_size("ctx"), lax.axis_size("fsdp")
    c, f = lax.axis_index("ctx"), lax.axis_index("fsdp")
    rows = grad.shape[0] // groups
    d = rows // size
    total = lax.dynamic_slice_in_dim(grad, f * rows, rows, 0)
    for g in range(1, groups):
        sent = lax.dynamic_slice_in_dim(grad, ((f + g) % groups) * rows, rows, 0)
        got = lax.ppermute(sent, "fsdp", [(i, (i + g) % groups) for i in range(groups)])
        total = total.astype(jnp.float32) + got.astype(jnp.float32)
    total = total.astype(jnp.bfloat16)
    pieces = []
    for s in range(size):
        piece = lax.dynamic_slice_in_dim(total, ((c + s) % size) * d, d, 0)
        if s:
            piece = lax.ppermute(piece, "ctx", [(i, (i + s) % size) for i in range(size)])
        pieces.append(piece)
    return pieces


def finish_kernel(size, *refs):
    gu, down, out = refs[:size], refs[size : 2 * size], refs[2 * size : 3 * size]
    rows, gu_ref, down_ref, out_ref, rows_ref = refs[3 * size :]
    c = lax.axis_index("ctx")
    half, narrow = down[0].shape[1], out[0].shape[1]
    for s in range(size):
        source = (c + size - s) % size
        lanes = pl.ds(pl.multiple_of(source * half, half), half)
        for j in range(2):
            gu_ref[j, :, lanes] = gu[s][:, j * half : (j + 1) * half].astype(jnp.float32)
        down_ref[lanes, :] = down[s][...].astype(jnp.float32).T
        at = pl.ds(pl.multiple_of(source * narrow, narrow), narrow)
        out_ref[at, :] = out[s][...].astype(jnp.float32).T
    rows_ref[...] = rows[...]


def finish_call(gu, down, out, rows, size):
    d, full = gu[0].shape[0], jnp.float32
    vmem = pl.BlockSpec(memory_space=pltpu.VMEM)
    return pl.pallas_call(
        functools.partial(finish_kernel, size),
        out_shape=(
            jax.ShapeDtypeStruct((2, d, size * down[0].shape[1]), full),
            jax.ShapeDtypeStruct((size * down[0].shape[1], d), full),
            jax.ShapeDtypeStruct((size * out[0].shape[1], d), full),
            jax.ShapeDtypeStruct(rows.shape, rows.dtype),
        ),
        in_specs=[vmem] * (3 * size + 1),
        out_specs=(vmem,) * 4,
        compiler_params=pltpu.CompilerParams(vmem_limit_bytes=VLIM),
        cost_estimate=cost(8),
        name="finish",
    )(*gu, *down, *out, rows)


def wide_gather(part):
    full = lax.all_gather(part, GROUP, axis=0, tiled=True)
    return full


def mlp_block(half, pair, buf, ins, outs):
    w, wd, cot = ins
    act, g_gate, g_up = outs
    rows = buf.shape[1]
    tile = 256
    at = pl.ds(pl.multiple_of(pair * rows, rows), rows)

    def one(i, carry):
        lanes = pl.ds(pl.multiple_of(i * tile, tile), tile)
        gate = nt(buf[pair], w[lanes, :])
        up = nt(buf[pair], w[pl.ds(pl.multiple_of(half + i * tile, tile), tile), :])
        grad = nt(cot[at, :], wd[lanes, :])
        sigma = 1.0 / (1.0 + jnp.exp(-gate))
        silu = gate * sigma
        act[at, lanes] = (silu * up).astype(jnp.bfloat16)
        g_up[at, lanes] = (grad * silu).astype(jnp.bfloat16)
        g_gate[at, lanes] = (grad * up * sigma * (1.0 + gate * (1.0 - sigma))).astype(jnp.bfloat16)
        return carry

    lax.fori_loop(0, half // tile, one, 0)


def attn_block(pair, buf, ins, outs):
    rows = buf.shape[1]
    at = pl.ds(pl.multiple_of(pair * rows, rows), rows)
    outs[0][at, :] = nt(buf[pair], ins[0][...]).astype(jnp.bfloat16)


def no_block(pair, buf, ins, outs):
    pass


def nothing():
    pass


def after_out(total, ins, outs, extra):
    tokens, gain = ins
    hidden, normed = outs

    def one(r):
        value = tokens[r, :].astype(jnp.float32) + total[r, :]
        scale = lax.rsqrt(jnp.mean(value * value, axis=1, keepdims=True) + EPSILON)
        hidden[r, :] = value
        normed[r, :] = (value * scale * gain[...]).astype(jnp.bfloat16)

    return nothing, one, nothing


def norm_back(grad, value, gain, top):
    scale = lax.rsqrt(jnp.mean(value * value, axis=1, keepdims=True) + EPSILON)
    unit = value * scale
    g_unit = grad * gain
    inner = jnp.mean(g_unit * unit, axis=1, keepdims=True)
    return top + scale * (g_unit - unit * inner), grad * unit


def after_mlp(total, ins, outs, extra):
    hidden, cot, gain = ins
    g_hidden, g_branch, g_gain = outs

    def begin():
        g_gain[...] = jnp.zeros_like(g_gain)

    def one(r):
        grad, part = norm_back(
            total[r, :], hidden[r, :], gain[...], cot[r, :].astype(jnp.float32)
        )
        g_hidden[r, :] = grad
        g_branch[r, :] = grad.astype(jnp.bfloat16)
        g_gain[...] += part

    return begin, one, nothing


def after_qkv(total, ins, outs, extra):
    tokens, g_hidden, gain, g_gain_mlp, _ = ins
    rows_all, sums = extra[:2]
    place = lax.axis_index("tp")

    def begin():
        sums[4] = jnp.zeros(sums.shape[1:], jnp.float32)

    def one(r):
        grad, part = norm_back(
            total[r, :], tokens[r, :].astype(jnp.float32), gain[...], g_hidden[r, :]
        )
        rows_all[place, r, :] = grad.astype(jnp.bfloat16)
        sums[4] += part[0:8] + part[8:16]

    def end():
        sums[0] = jnp.concatenate(
            [
                jnp.sum(sums[4], axis=0, keepdims=True),
                jnp.sum(g_gain_mlp[...], axis=0, keepdims=True),
                jnp.zeros((6, total.shape[1]), jnp.float32),
            ],
            axis=0,
        )

    return begin, one, end


PLAN = {
    -1: [("z", 0, 1), ("z", 0, 2), ("z", 0, 3), ("x", 0, 0), ("x", 1, 0)],
    0: [("z", 1, 1), ("z", 1, 2), ("z", 1, 3), ("x", 0, 1)],
    1: [("x", 0, 2), ("x", 0, 3), ("x", 1, 1)],
    2: [("x", 1, 2), ("x", 1, 3)],
}
PLAN_OUT = {
    -1: [("z", 0, 1), ("z", 0, 2), ("z", 0, 3), ("x", 0, 0)],
    1: [("x", 0, 1)],
    2: [("x", 0, 2)],
    3: [("x", 0, 3)],
}


def shards(tokens, segments, w_qkv, w_out, w_gate_up, w_down, norm_attn, norm_mlp, cotangent):
    seqs, rows, width = tokens.shape
    size, tp_size = lax.axis_size("ctx"), lax.axis_size("tp")
    length = segments.shape[1]
    assert seqs == 1 and tp_size == 4
    part = rows // tp_size
    begin = lax.axis_index("tp") * part
    scale = 1.0 / math.sqrt(HD)
    low, full = jnp.bfloat16, jnp.float32
    heads = w_qkv.shape[2] // HD // size
    seg = segments[0]

    tokens_own = lax.dynamic_slice_in_dim(tokens[0], begin, part, 0)
    cot_own = lax.dynamic_slice_in_dim(cotangent[0], begin, part, 0)

    d = w_qkv.shape[1]
    gain_rows = jnp.concatenate(
        [norm_attn[None], norm_mlp[None], jnp.zeros((GAIN_ROWS - 2, d), low)], axis=0
    )
    sent_q = w_qkv.reshape(3, d, size, -1).transpose(2, 0, 3, 1)
    sent_q = jnp.concatenate(
        [sent_q.reshape(size, -1, d), jnp.broadcast_to(gain_rows, (size, GAIN_ROWS, d))], axis=1
    )
    sent_o = w_out.reshape(size, -1, d)
    sent_g = w_gate_up.reshape(2, d, size, -1).transpose(2, 0, 3, 1).reshape(size, -1, d)
    sent_d = w_down.reshape(size, -1, d)
    tokens_full, moved_q, moved_o = gather_call(
        tokens_own, [], [], no_block, 1, size, [sent_q, sent_o], PLAN
    )
    wq = join(sent_q, moved_q, True, GAIN_ROWS)
    wo = join(sent_o, moved_o, True)
    wg = join(sent_g, cross(sent_g), False)
    half = sent_d.shape[1]
    tall = 3 * heads * LANES
    gains = wq[tall : tall + 2].astype(full)
    gain_attn, gain_mlp = gains[0:1], gains[1:2]
    cot_gate, tokens_full = lax.optimization_barrier((cot_own, tokens_full))
    cot_full = wide_gather(cot_gate)

    positions = doc_positions(seg)
    cosine, sine = rope_tables(positions)
    starts = (jnp.arange(length, dtype=jnp.int32) - positions)[::BLK] // BLK
    marks = jnp.arange(length // BLK, dtype=jnp.int32)
    ends = jnp.sum((starts[None, :] <= marks[:, None]).astype(jnp.int32), axis=1) - 1

    qkv, normed1 = qkv_call(tokens_full, wq, gain_attn, cosine, sine, heads)
    attn, lse = attend_call(qkv, seg, starts, heads, scale)

    row_shape = jax.ShapeDtypeStruct((part, width), full)
    row_low = jax.ShapeDtypeStruct((part, width), low)
    gain_shape = jax.ShapeDtypeStruct((16, width), full)
    hidden1, normed2_own, moved_d = reduce_call(
        attn,
        wo,
        [tokens_own, gain_mlp],
        [row_shape, row_low],
        after_out,
        2,
        size,
        sent=[sent_d],
        plan=PLAN_OUT,
    )
    wd = join(sent_d, moved_d, False)
    half_shape = jax.ShapeDtypeStruct((length, half), low)
    normed2, act, g_gate, g_up = gather_call(
        normed2_own,
        [wg, wd, cot_full],
        [half_shape] * 3,
        functools.partial(mlp_block, half),
        3,
        size,
    )
    g_gu = jnp.concatenate([g_gate, g_up], axis=1)
    down_part = nn(act, wd).astype(low)
    down = lax.psum_scatter(down_part, GROUP, scatter_dimension=0, tiled=True)
    output = (hidden1 + down.astype(full)).astype(low)
    output = lax.all_gather(output, "tp", axis=0, tiled=True)[None]

    part_down, part_gu = tn(cot_full, act).astype(low), tn(normed2, g_gu).astype(low)
    g_gu, part_down, part_gu = lax.optimization_barrier((g_gu, part_down, part_gu))
    g_hidden1, g_branch_own, g_gain_mlp = reduce_call(
        g_gu, wg, [hidden1, cot_own, gain_mlp], [row_shape, row_low, gain_shape], after_mlp, 4, size
    )
    g_branch, g_attn = gather_call(
        g_branch_own,
        [wo],
        [jax.ShapeDtypeStruct((length, heads * LANES), low)],
        attn_block,
        5,
        size,
    )
    out_down = hand_out(part_down)
    out_gu = hand_out(part_gu)
    part_out = unspread(tn(g_branch, attn), 1).astype(low)
    g_attn, part_out = lax.optimization_barrier((g_attn, part_out))
    g_proj = attend_back_call(qkv, attn, g_attn, lse, seg, ends, cosine, sine, heads, scale)
    out_out = hand_out(part_out)
    part_qkv = unspread(tn(normed1, g_proj), 1).astype(low)
    g_proj, part_qkv = lax.optimization_barrier((g_proj, part_qkv))
    g_tokens, gain_sums, out_qkv = reduce_call(
        g_proj,
        wq,
        [tokens_own, g_hidden1, gain_attn, g_gain_mlp, part_qkv],
        [
            jax.ShapeDtypeStruct((tp_size, part, width), low),
            jax.ShapeDtypeStruct((8, width), full),
            jax.ShapeDtypeStruct((size, d, part_qkv.shape[1]), low),
        ],
        after_qkv,
        6,
        size,
        True,
    )
    g_tokens = g_tokens.reshape(1, rows, width)

    def natural(grad, count):
        wide = grad.astype(full).reshape(size, d, count, -1).transpose(2, 1, 0, 3)
        return wide.reshape(count, d, -1)

    grad_gu, grad_down, grad_out, g_tokens = finish_call(out_gu, out_down, out_out, g_tokens, size)
    grad_qkv = natural(out_qkv, 3)

    mine = lax.axis_index("fsdp") * size + lax.axis_index("ctx")
    gain_grads = lax.dynamic_slice_in_dim(gain_sums, mine * d, d, 1)
    return (
        output,
        g_tokens,
        grad_qkv,
        grad_out,
        grad_gu,
        grad_down,
        gain_grads[0],
        gain_grads[1],
    )


def solution(mesh):
    in_specs = (
        P("fsdp", "ctx", None),
        P("fsdp", None),
        P(None, ("fsdp", "ctx"), "tp"),
        P("tp", ("fsdp", "ctx")),
        P(None, ("fsdp", "ctx"), "tp"),
        P("tp", ("fsdp", "ctx")),
        P(("fsdp", "ctx")),
        P(("fsdp", "ctx")),
        P("fsdp", "ctx", None),
    )
    out_specs = (
        P("fsdp", "ctx", None),
        P("fsdp", "ctx", None),
        P(None, ("fsdp", "ctx"), "tp"),
        P("tp", ("fsdp", "ctx")),
        P(None, ("fsdp", "ctx"), "tp"),
        P("tp", ("fsdp", "ctx")),
        P(("fsdp", "ctx")),
        P(("fsdp", "ctx")),
    )
    return jax.shard_map(shards, mesh=mesh, in_specs=in_specs, out_specs=out_specs, check_vma=False)
```
